32 devices in a mesh: dp: 8 (over z, x), col: 4 (over y, core).
Axes of the slice: x: 2, y: 2, z: 4, core: 2. Of those that a mesh axis runs over, the one named last changes fastest.
Arguments:
- tokens: bfloat16 [50432, 384], P(('dp', 'col')), may hold values from -40 to 40
- packed: bfloat16 [384, 1152], P('dp', 'col'), may hold values from -0.3125 to 0.3125
- packed_bias: float32 [1152], P('col'), may hold values from -3 to 3
- projection: bfloat16 [384, 384], P('col', 'dp'), may hold values from -2.5 to 2.5
- projection_bias: float32 [384], replicated, may hold values from -3 to 3
- expansion: bfloat16 [384, 1536], P('dp', 'col'), may hold values from -0.3125 to 0.3125
- expansion_bias: float32 [1536], P('col'), may hold values from -3 to 3
- reduction: bfloat16 [1536, 384], P('col', 'dp'), may hold values from -0.15625 to 0.15625
- reduction_bias: float32 [384], replicated, may hold values from -3 to 3
- first_scale: float32 [384], replicated, may hold values from 0.25 to 1.75
- first_shift: float32 [384], replicated, may hold values from -3 to 3
- second_scale: float32 [384], replicated, may hold values from 0.25 to 1.75
- second_shift: float32 [384], replicated, may hold values from -3 to 3
- upstream: bfloat16 [50432, 384], P(('dp', 'col')), may hold values from -6 to 6
Outputs:
- layer_output: bfloat16 [50432, 384], P(('dp', 'col'))
- input_grad: float32 [50432, 384], P(('dp', 'col'))
- packed_grad: float32 [384, 1152], P('dp', 'col')
- projection_grad: float32 [384, 384], P('col', 'dp')
- expansion_grad: float32 [384, 1536], P('dp', 'col')
- reduction_grad: float32 [1536, 384], P('col', 'dp')
- packed_bias_grad: float32 [1152], P('col')
- projection_bias_grad: float32 [384], P('col')
- expansion_bias_grad: float32 [1536], P('col')
- reduction_bias_grad: float32 [384], P('col')
- first_scale_grad: float32 [384], P('col')
- first_shift_grad: float32 [384], P('col')
- second_scale_grad: float32 [384], P('col')
- second_shift_grad: float32 [384], P('col')
The draws below stay inside these ranges and needn't reach their ends.
All inputs are finite; a program needn't handle non-finite values.
Results may differ from the reference program's by a relative error of at most 0.023.
Values may be sent and summed in bfloat16 or wider, within the bound.
A program may use at most 192 MiB of HBM per device.

```python
import math
import jax
import jax.numpy as jnp
from jax import lax

D = 384
HEADS = 6
FF = 1536
SEQ = 197
IMAGES = 256
TOKENS = 50432


def draw_tokens(key, part):
    key_noise, key_rows, key_cols = jax.random.split(key, 3)
    noise = jax.random.normal(key_noise, (TOKENS, D), jnp.float32)
    row_lower = math.log(0.4)
    row_scale = jnp.exp(jax.random.uniform(key_rows, (TOKENS, 1), jnp.float32, row_lower, math.log(4.0)))
    col_scale = jnp.exp(jax.random.uniform(key_cols, (1, D), jnp.float32, math.log(0.4), math.log(4.0)))
    return jnp.clip(noise * row_scale * col_scale, -40.0, 40.0).astype(jnp.bfloat16)


def with_spikes(values, own_key, source, target, blocks, factor):
    owner, partner = [(jnp.arange(values.shape[position]) // (values.shape[position] // blocks)).reshape([-1 if axis == position else 1 for axis in range(values.ndim)]) for position in (source, target)]
    chosen = jax.random.permutation(own_key, blocks)[partner]
    strong = (owner == chosen) | (owner == (partner + blocks // 2) % blocks)
    return jnp.where(strong, factor * values, values)


def block_scale(rng, dims, cuts, smallest, top_value):
    def one(position, blocks):
        steps = jax.random.uniform(jax.random.fold_in(jax.random.fold_in(rng, 6), position), (blocks,), jnp.float32, smallest / len(cuts), top_value / len(cuts))
        return jnp.repeat(jnp.exp(steps), dims[position] // blocks).reshape((-1,) + (1,) * (len(dims) - position - 1))

    gain = one(*cuts[0])
    for cut in cuts[1:]:
        gain = gain * one(*cut)
    return gain


def centred(stream_key, dims, width, limit, cuts=(), kind=jnp.bfloat16):
    loudness = block_scale(stream_key, dims, cuts, -0.22, 0.18) if cuts else 1.0
    values = jax.random.normal(stream_key, dims, jnp.float32) * width * loudness
    return jnp.minimum(jnp.maximum(values, -limit), limit).astype(kind)


def noise_with(own_key, extent, spread, most, cuts, heavy, dtype=jnp.bfloat16):
    array = spread * jax.random.normal(own_key, extent, jnp.float32)
    if cuts:
        array = array * block_scale(own_key, extent, cuts, -0.22, 0.18)
    return jnp.clip(with_spikes(array, jax.random.fold_in(own_key, 3), *heavy), -most, most).astype(dtype)


def setup_inputs(seed: int = 0) -> dict:
    keys = jax.random.split(jax.random.key(seed), 15)
    return {
        "tokens": draw_tokens(jax.random.fold_in(keys[14], 71), 0),
        "packed": centred(keys[1], (D, 3 * D), D ** -0.5, 0.3125, ((0, 8), (1, 4))),
        "packed_bias": centred(keys[2], (3 * D,), 0.5, 3.0, ((0, 4),), jnp.float32),
        "projection": centred(keys[3], (D, D), (max(D // 64, 1)) ** -0.5, 2.5, ((0, 4), (1, 8))),
        "projection_bias": centred(keys[4], (D,), 0.5, 3.0, (), jnp.float32),
        "expansion": centred(keys[5], (D, FF), D ** -0.5, 0.3125, ((0, 8), (1, 4))),
        "expansion_bias": centred(keys[6], (FF,), 0.5, 3.0, ((0, 4),), jnp.float32),
        "reduction": centred(keys[7], (FF, D), FF ** -0.5, 0.15625, ((0, 4), (1, 8))),
        "reduction_bias": centred(keys[8], (D,), 0.5, 3.0, (), jnp.float32),
        "first_scale": jnp.clip(1.0 + 0.15 * jax.random.normal(keys[9], (D,), jnp.float32), 0.25, 1.75),
        "first_shift": centred(keys[10], (D,), 0.5, 3.0, (), jnp.float32),
        "second_scale": jnp.clip(1.0 + 0.15 * jax.random.normal(keys[11], (D,), jnp.float32), 0.25, 1.75),
        "second_shift": centred(keys[12], (D,), 0.5, 3.0, (), jnp.float32),
        "upstream": noise_with(keys[13], (TOKENS, D), 1.0, 6.0, ((0, 32),), (0, 1, 32, 2.75)),
    }


epsilon = 1e-06
root_half = 0.7071067811865476
inv_root_tau = 0.3989422804014327

def gelu_slope(values):
    return 0.5 * (1.0 + lax.erf(values * root_half)) + values * jnp.exp(-0.5 * values * values) * inv_root_tau

def norm_forward(values, scale, shift):
    average = lax.optimization_barrier(jnp.mean(values, axis=1, keepdims=True))
    meansq = lax.optimization_barrier(jnp.mean(values * values, axis=1, keepdims=True))
    inverse = lax.rsqrt(meansq - average * average + epsilon)
    normed = (values - average) * inverse
    return (normed, inverse, (normed * scale + shift).astype(jnp.bfloat16))

def norm_backward(upper, normed, inverse, scale):
    scaled = upper * scale
    return inverse * (scaled - lax.optimization_barrier(jnp.mean(scaled, axis=1, keepdims=True)) - normed * lax.optimization_barrier(jnp.mean(scaled * normed, axis=1, keepdims=True)))

def split_fields(packed_rows, images):
    head_dim = D // HEADS
    fields = packed_rows.astype(jnp.float32).reshape(images, SEQ, 3, HEADS, head_dim)
    return (fields[:, :, 0], fields[:, :, 1], fields[:, :, 2])

def attend_forward(packed_rows, images):
    factor = (D // HEADS) ** (-0.5)
    query_rows, key_rows, value_rows = split_fields(packed_rows, images)
    scores = jnp.einsum('bqhd,bkhd->bhqk', query_rows, key_rows) * factor
    logsum = jnp.log(lax.optimization_barrier(jnp.sum(jnp.exp(scores), axis=-1)))
    prob_rows = jnp.exp(scores - logsum[..., None]).astype(jnp.bfloat16)
    prob_rows = lax.optimization_barrier(prob_rows).astype(jnp.float32)
    mixed = jnp.einsum('bhqk,bkhd->bqhd', prob_rows, value_rows)
    return (mixed.astype(jnp.bfloat16).reshape(images * SEQ, D), logsum)

def attend_backward(packed_rows, logsum, grad_rows, images):
    head_dim = D // HEADS
    factor = head_dim ** (-0.5)
    query_rows, key_rows, value_rows = split_fields(packed_rows, images)
    grad_heads = grad_rows.astype(jnp.float32).reshape(images, SEQ, HEADS, head_dim)
    scores = jnp.einsum('bqhd,bkhd->bhqk', query_rows, key_rows) * factor
    probs_full = jnp.exp(scores - logsum[..., None])
    prob_rows = lax.optimization_barrier(probs_full.astype(jnp.bfloat16)).astype(jnp.float32)
    grad_probs = jnp.einsum('bqhd,bkhd->bhqk', grad_heads, value_rows)
    delta = lax.optimization_barrier(jnp.sum(probs_full * grad_probs, axis=-1, keepdims=True))
    grad_scores = (probs_full * (grad_probs - delta) * factor).astype(jnp.bfloat16)
    grad_scores = lax.optimization_barrier(grad_scores).astype(jnp.float32)
    grad_query = jnp.einsum('bhqk,bkhd->bqhd', grad_scores, key_rows)
    grad_key = jnp.einsum('bhqk,bqhd->bkhd', grad_scores, query_rows)
    grad_value = jnp.einsum('bhqk,bqhd->bkhd', prob_rows, grad_heads)
    stacked = jnp.stack([grad_query, grad_key, grad_value], axis=2)
    return stacked.reshape(images * SEQ, 3 * D).astype(jnp.bfloat16)

def reference(tokens, packed, packed_bias, projection, projection_bias, expansion, expansion_bias, reduction, reduction_bias, first_scale, first_shift, second_scale, second_shift, upstream):
    group = 16
    block_rows = group * SEQ
    blocks = IMAGES // group
    token_blocks = tokens.reshape(blocks, block_rows, D)
    upstream_blocks = upstream.reshape(blocks, block_rows, D)
    fp = jnp.float32

    def advance(carry, item):
        block_tokens, block_upstream = item
        tokens_f = block_tokens.astype(fp)
        normed1, inverse1, rows1 = norm_forward(tokens_f, first_scale, first_shift)
        packed_rows = (jnp.dot(rows1, packed, preferred_element_type=fp) + packed_bias).astype(jnp.bfloat16)
        attn_rows, logsum = attend_forward(packed_rows, group)
        resid = tokens_f + jnp.dot(attn_rows, projection, preferred_element_type=fp) + projection_bias
        normed2, inverse2, rows2 = norm_forward(resid, second_scale, second_shift)
        hidden_pre = jnp.dot(rows2, expansion, preferred_element_type=fp) + expansion_bias
        hidden_act = jax.nn.gelu(hidden_pre, approximate=False).astype(jnp.bfloat16)
        layer_out = (resid + (jnp.dot(hidden_act, reduction, preferred_element_type=fp) + reduction_bias)).astype(jnp.bfloat16)
        upstream_f = block_upstream.astype(fp)
        reduction_bias_grad = lax.optimization_barrier(jnp.sum(upstream_f, axis=0))
        reduction_grad = jnp.dot(hidden_act.T, block_upstream, preferred_element_type=fp)
        hidden_grad = jnp.dot(block_upstream, reduction.T, preferred_element_type=fp) * gelu_slope(hidden_pre)
        expansion_bias_grad = lax.optimization_barrier(jnp.sum(hidden_grad, axis=0))
        hidden_grad_b = hidden_grad.astype(jnp.bfloat16)
        expansion_grad = jnp.dot(rows2.T, hidden_grad_b, preferred_element_type=fp)
        rows2_grad = jnp.dot(hidden_grad_b, expansion.T, preferred_element_type=fp)
        second_scale_grad = lax.optimization_barrier(jnp.sum(rows2_grad * normed2, axis=0))
        second_shift_grad = lax.optimization_barrier(jnp.sum(rows2_grad, axis=0))
        resid_grad = upstream_f + norm_backward(rows2_grad, normed2, inverse2, second_scale)
        projection_bias_grad = lax.optimization_barrier(jnp.sum(resid_grad, axis=0))
        resid_grad_b = resid_grad.astype(jnp.bfloat16)
        projection_grad = jnp.dot(attn_rows.T, resid_grad_b, preferred_element_type=fp)
        attn_grad = jnp.dot(resid_grad_b, projection.T, preferred_element_type=fp).astype(jnp.bfloat16)
        packed_grad_rows = attend_backward(packed_rows, logsum, attn_grad, group)
        packed_bias_grad = lax.optimization_barrier(jnp.sum(packed_grad_rows.astype(fp), axis=0))
        packed_grad = jnp.dot(rows1.T, packed_grad_rows, preferred_element_type=fp)
        rows1_grad = jnp.dot(packed_grad_rows, packed.T, preferred_element_type=fp)
        first_scale_grad = lax.optimization_barrier(jnp.sum(rows1_grad * normed1, axis=0))
        first_shift_grad = lax.optimization_barrier(jnp.sum(rows1_grad, axis=0))
        input_grad = resid_grad + norm_backward(rows1_grad, normed1, inverse1, first_scale)
        terms = (packed_grad, projection_grad, expansion_grad, reduction_grad, packed_bias_grad, projection_bias_grad, expansion_bias_grad, reduction_bias_grad, first_scale_grad, first_shift_grad, second_scale_grad, second_shift_grad)
        carry = tuple((held + term for held, term in zip(carry, terms)))
        return (carry, (layer_out, input_grad))
    start = (jnp.zeros((D, 3 * D), fp), jnp.zeros((D, D), fp), jnp.zeros((D, FF), fp), jnp.zeros((FF, D), fp), jnp.zeros((3 * D,), fp), jnp.zeros((D,), fp), jnp.zeros((FF,), fp), jnp.zeros((D,), fp), jnp.zeros((D,), fp), jnp.zeros((D,), fp), jnp.zeros((D,), fp), jnp.zeros((D,), fp))
    totals, outputs = lax.scan(advance, start, (token_blocks, upstream_blocks))
    layer_output = outputs[0].reshape(TOKENS, D)
    input_grad = outputs[1].reshape(TOKENS, D)
    return (layer_output, input_grad, totals[0], totals[1], totals[2], totals[3], totals[4], totals[5], totals[6], totals[7], totals[8], totals[9], totals[10], totals[11])
```

```python
import jax
import jax.numpy as jnp
from jax import lax
from jax.sharding import PartitionSpec as P

D = 384
HEADS = 6
SEQ = 197


epsilon = 1e-06
root_half = 0.7071067811865476
inv_root_tau = 0.3989422804014327


def gelu_slope(values):
    return (
        0.5 * (1.0 + lax.erf(values * root_half))
        + values * jnp.exp(-0.5 * values * values) * inv_root_tau
    )


def contract_rows(left, right):
    return lax.dot_general(
        left, right, (((0,), (0,)), ((), ())), preferred_element_type=jnp.float32
    )


def contract_cols(left, right):
    return lax.dot_general(
        left, right, (((1,), (1,)), ((), ())), preferred_element_type=jnp.float32
    )


def norm_forward(values, scale, shift):
    average = jnp.mean(values, axis=1, keepdims=True)
    meansq = jnp.mean(values * values, axis=1, keepdims=True)
    inverse = lax.rsqrt(meansq - average * average + epsilon)
    normed = (values - average) * inverse
    return (normed, inverse, (normed * scale + shift).astype(jnp.bfloat16))


def norm_backward(upper, normed, inverse, scale):
    scaled = upper * scale
    return inverse * (
        scaled
        - jnp.mean(scaled, axis=1, keepdims=True)
        - normed * jnp.mean(scaled * normed, axis=1, keepdims=True)
    )


def attend_forward(packed_img):
    images = packed_img.shape[0]
    head_dim = D // HEADS
    fields = packed_img.reshape(images, SEQ, 3, HEADS, head_dim)
    scores = jnp.einsum(
        "bqhd,bkhd->bhqk", fields[:, :, 0], fields[:, :, 1], preferred_element_type=jnp.float32
    ) * head_dim ** (-0.5)
    logsum = jnp.log(jnp.sum(jnp.exp(scores), axis=-1))
    prob_rows = jnp.exp(scores - logsum[..., None]).astype(jnp.bfloat16)
    mixed = jnp.einsum(
        "bhqk,bkhd->bqhd", prob_rows, fields[:, :, 2], preferred_element_type=jnp.float32
    )
    return (mixed.astype(jnp.bfloat16).reshape(images, SEQ, D), logsum)


def attend_backward(packed_img, logsum, grad_img):
    images = packed_img.shape[0]
    head_dim = D // HEADS
    factor = head_dim ** (-0.5)
    fields = packed_img.reshape(images, SEQ, 3, HEADS, head_dim)
    query_rows = fields[:, :, 0]
    key_rows = fields[:, :, 1]
    value_rows = fields[:, :, 2]
    grad_heads = grad_img.reshape(images, SEQ, HEADS, head_dim)
    scores = (
        jnp.einsum("bqhd,bkhd->bhqk", query_rows, key_rows, preferred_element_type=jnp.float32)
        * factor
    )
    probs_full = jnp.exp(scores - logsum[..., None])
    prob_rows = probs_full.astype(jnp.bfloat16)
    grad_probs = jnp.einsum(
        "bqhd,bkhd->bhqk", grad_heads, value_rows, preferred_element_type=jnp.float32
    )
    delta = jnp.sum(probs_full * grad_probs, axis=-1, keepdims=True)
    grad_scores = (probs_full * (grad_probs - delta) * factor).astype(jnp.bfloat16)
    grad_query = jnp.einsum(
        "bhqk,bkhd->bqhd", grad_scores, key_rows, preferred_element_type=jnp.float32
    )
    grad_key = jnp.einsum(
        "bhqk,bqhd->bkhd", grad_scores, query_rows, preferred_element_type=jnp.float32
    )
    grad_value = jnp.einsum(
        "bhqk,bqhd->bkhd", prob_rows, grad_heads, preferred_element_type=jnp.float32
    )
    stacked = jnp.stack([grad_query, grad_key, grad_value], axis=2)
    return stacked.reshape(images, SEQ, 3 * D).astype(jnp.bfloat16)


def body(
    tokens,
    packed,
    packed_bias,
    projection,
    projection_bias,
    expansion,
    expansion_bias,
    reduction,
    reduction_bias,
    first_scale,
    first_shift,
    second_scale,
    second_shift,
    upstream,
):
    cols = lax.axis_size("col")
    dps = lax.axis_size("dp")
    pieces = (packed, projection, expansion, reduction)
    flat = jnp.concatenate([piece.reshape(-1) for piece in pieces])
    everything = lax.all_gather(flat, ("dp", "col"), axis=0, tiled=False)
    everything = everything.reshape(dps, cols, -1)
    fulls = []
    start = 0
    for piece, dp_first in zip(pieces, (True, False, True, False)):
        rows, columns = piece.shape
        part = everything[:, :, start : start + rows * columns].reshape(dps, cols, rows, columns)
        start += rows * columns
        if dp_first:
            fulls.append(part.transpose(0, 2, 1, 3).reshape(dps * rows, cols * columns))
        else:
            fulls.append(part.transpose(1, 2, 0, 3).reshape(cols * rows, dps * columns))
    packed_full, projection_full, expansion_full, reduction_full = fulls
    small = jnp.concatenate([packed_bias, expansion_bias])
    small = lax.all_gather(small, "col", axis=0, tiled=False)
    packed_bias_full = small[:, : packed_bias.shape[0]].reshape(-1)
    expansion_bias_full = small[:, packed_bias.shape[0] :].reshape(-1)

    tokens_f = tokens.astype(jnp.float32)
    upstream_f = upstream.astype(jnp.float32)
    normed1, inverse1, rows1 = norm_forward(tokens_f, first_scale, first_shift)
    count = rows1.shape[0]
    images = count // SEQ
    packed_rows = (
        jnp.dot(rows1, packed_full, preferred_element_type=jnp.float32) + packed_bias_full
    ).astype(jnp.bfloat16).reshape(images, SEQ, -1)
    mixed, logsum = attend_forward(packed_rows)
    attn_rows = mixed.reshape(count, -1)
    resid = (
        tokens_f
        + jnp.dot(attn_rows, projection_full, preferred_element_type=jnp.float32)
        + projection_bias
    )
    normed2, inverse2, rows2 = norm_forward(resid, second_scale, second_shift)
    hidden_pre = (
        jnp.dot(rows2, expansion_full, preferred_element_type=jnp.float32) + expansion_bias_full
    )
    hidden_act = jax.nn.gelu(hidden_pre, approximate=False).astype(jnp.bfloat16)
    layer_output = (
        resid
        + (jnp.dot(hidden_act, reduction_full, preferred_element_type=jnp.float32) + reduction_bias)
    ).astype(jnp.bfloat16)
    reduction_bias_grad = jnp.sum(upstream_f, axis=0)
    reduction_grad = contract_rows(hidden_act, upstream)
    hidden_grad = contract_cols(upstream, reduction_full) * gelu_slope(hidden_pre)
    expansion_bias_grad = jnp.sum(hidden_grad, axis=0)
    hidden_grad_b = hidden_grad.astype(jnp.bfloat16)
    expansion_grad = contract_rows(rows2, hidden_grad_b)
    rows2_grad = contract_cols(hidden_grad_b, expansion_full)
    second_scale_grad = jnp.sum(rows2_grad * normed2, axis=0)
    second_shift_grad = jnp.sum(rows2_grad, axis=0)
    resid_grad = upstream_f + norm_backward(rows2_grad, normed2, inverse2, second_scale)
    projection_bias_grad = jnp.sum(resid_grad, axis=0)
    resid_grad_b = resid_grad.astype(jnp.bfloat16)
    projection_grad = contract_rows(attn_rows, resid_grad_b)
    attn_grad = contract_cols(resid_grad_b, projection_full).astype(jnp.bfloat16)
    packed_grad_rows = attend_backward(
        packed_rows, logsum, attn_grad.reshape(images, SEQ, -1)
    ).reshape(count, -1)
    packed_bias_grad = jnp.sum(packed_grad_rows.astype(jnp.float32), axis=0)
    packed_grad = contract_rows(rows1, packed_grad_rows)
    rows1_grad = contract_cols(packed_grad_rows, packed_full)
    first_scale_grad = jnp.sum(rows1_grad * normed1, axis=0)
    first_shift_grad = jnp.sum(rows1_grad, axis=0)
    input_grad = resid_grad + norm_backward(rows1_grad, normed1, inverse1, first_scale)

    whole = []
    for grad, piece, dp_first in zip(
        (packed_grad, projection_grad, expansion_grad, reduction_grad), pieces, (True, False, True, False)
    ):
        rows, columns = piece.shape
        grad = grad.astype(jnp.bfloat16)
        if dp_first:
            grad = grad.reshape(dps, rows, cols, columns).transpose(0, 2, 1, 3)
        else:
            grad = grad.reshape(cols, rows, dps, columns).transpose(2, 0, 1, 3)
        whole.append(grad.reshape(dps * cols, -1))
    whole = jnp.concatenate(whole, axis=1)
    mine = lax.psum_scatter(whole, ("dp", "col"), scatter_dimension=0, tiled=True).reshape(-1)
    outs = []
    start = 0
    for piece in pieces:
        rows, columns = piece.shape
        outs.append(mine[start : start + rows * columns].reshape(rows, columns).astype(jnp.float32))
        start += rows * columns
    vectors = (
        packed_bias_grad,
        projection_bias_grad,
        expansion_bias_grad,
        reduction_bias_grad,
        first_scale_grad,
        first_shift_grad,
        second_scale_grad,
        second_shift_grad,
    )
    terms = jnp.concatenate([vector.reshape(cols, -1) for vector in vectors], axis=1)
    totals = lax.psum(terms, ("dp", "col"))
    own = lax.dynamic_index_in_dim(totals, lax.axis_index("col"), 0, keepdims=False)
    smalls = []
    start = 0
    for vector in vectors:
        width = vector.shape[0] // cols
        smalls.append(own[start : start + width])
        start += width
    return (layer_output, input_grad) + tuple(outs) + tuple(smalls)


def solution(mesh):
    placed = (
        P(("dp", "col"), None),
        P("dp", "col"),
        P("col"),
        P("col", "dp"),
        P(),
        P("dp", "col"),
        P("col"),
        P("col", "dp"),
        P(),
        P(),
        P(),
        P(),
        P(),
        P(("dp", "col"), None),
    )
    return jax.shard_map(
        body,
        mesh=mesh,
        in_specs=placed,
        out_specs=(
            P(("dp", "col"), None),
            P(("dp", "col"), None),
            P("dp", "col"),
            P("col", "dp"),
            P("dp", "col"),
            P("col", "dp"),
        )
        + (P("col"),) * 8,
        check_vma=False,
    )
```

```python
import functools

import jax
import jax.numpy as jnp
from jax import lax
from jax.experimental import pallas as pl
from jax.experimental.pallas import tpu as pltpu
from jax.sharding import PartitionSpec as P

SEQ = 197
EPS = 1e-06
ROOT_HALF = 0.7071067811865476
INV_ROOT_TAU = 0.3989422804014327
F32, BF16 = jnp.float32, jnp.bfloat16
MESH = pl.DeviceIdType.MESH
D = 384
FF = 1536
PAIRS = 3
WIN = 224
KEYS = 256
BIG = 528
SMALL = 176
HC = 512


def nn(a, b):
    return lax.dot_general(a, b, (((1,), (0,)), ((), ())), preferred_element_type=F32)


def nt(a, b):
    return lax.dot_general(a, b, (((1,), (1,)), ((), ())), preferred_element_type=F32)


def tn(a, b):
    return lax.dot_general(a, b, (((0,), (0,)), ((), ())), preferred_element_type=F32)


def rows_of(i, size):
    return pl.ds(pl.multiple_of(i * size, 16), size)


def lanes_of(i, size):
    return pl.ds(pl.multiple_of(i * size, 128), size)


def mean(x):
    return jnp.sum(x, axis=1, keepdims=True) * (1.0 / x.shape[1])


def hook(i, steps):
    for at, step in steps:
        pl.when(i == at)(step)


TILES = (
    ((0, 0, 128), (1, 1, 128), (2, 3, 96)),
    ((0, 0, 128), (1, 2, 64), (3, 3, 128)),
    ((0, 1, 32), (2, 2, 128), (3, 3, 128)),
)
SHARES = ((0, 1, 2, 2), (0, 1, 1, 2), (0, 0, 1, 2))


def layer_kernel(cfg, *refs):
    Z, PD, Y, RB, RV, rows = cfg
    PLANE = PD * Y
    RP = -(-rows // BIG) * BIG
    images = rows // SEQ
    nsm, nbig = RP // SMALL, RP // BIG
    (tokens, packed, packed_bias, projection, projection_bias, expansion, expansion_bias, reduction,
     reduction_bias, first_scale, first_shift, second_scale, second_shift, upstream,
     out_hbm, grad_hbm, o_packed, o_projection, o_expansion, o_reduction,
     o_pb, o_prb, o_eb, o_rb, o_fs, o_fh, o_ss, o_sh,
     x, up, n1, rows1, qkv, attn, est, rinv, n2, rows2, acc1, rg, act, hg, rgb, ag, pgr, inv1, inv2,
     wpk, ptr, exr, rtr, wp, pt, exc, rtc, bias,
     gm, gh, rm1, rm2, rm3, rh1, rh2, rh3, sm1, sm2, sh1, sh2, frame, vec, vsum1, vr1, vr2, vr3, eb,
     csem, zs, zr, ps, pr, ks, kr, bs, br, gs, gr_) = refs

    dp_i, col_i = lax.axis_index("dp"), lax.axis_index("col")
    z, pd = dp_i // PD, lax.rem(dp_i, PD)
    y, core = col_i // 2, lax.rem(col_i, 2)
    pos = core * Y + y
    plane = pd * Y + y

    def device(zz, pp, yy, cc):
        return (zz * PD + pp, yy * 2 + cc)

    def zpeer(d):
        return device(lax.rem(z + d, Z), pd, y, core)

    def pplace(d):
        q = lax.rem(plane + d, PLANE)
        return q // Y, lax.rem(q, Y)

    def ppeer(d):
        pp, yy = pplace(d)
        return device(z, pp, yy, core)

    sibling = device(z, pd, y, 1 - core)

    def cpeer(d):
        return (dp_i, lax.rem(col_i + d, 2 * Y))

    def remote(src, dst, send, recv, to):
        return pltpu.make_async_remote_copy(
            src_ref=src, dst_ref=dst, send_sem=send, recv_sem=recv, device_id=to, device_id_type=MESH)

    barrier = pltpu.get_barrier_semaphore()
    near = [zpeer(d) for d in range(1, Z)] + [ppeer(d) for d in range(1, PLANE)]
    near += [cpeer(d) for d in range(1, 2 * Y) if d != Y]
    for to in near + ([sibling] if Y == 1 else []):
        pl.semaphore_signal(barrier, inc=1, device_id=to, device_id_type=MESH)
    greeted = len(near)

    cin = pltpu.make_async_copy(tokens, x.at[pl.ds(0, rows)], csem.at[0])
    cup = pltpu.make_async_copy(upstream, up.at[pl.ds(0, rows)], csem.at[1])
    cin.start()
    cup.start()

    def padded(v):
        return v if RV == RB else jnp.concatenate([v, jnp.zeros((RB - RV, v.shape[1]), v.dtype)], axis=0)

    own = padded(packed[...].astype(F32))
    own = jnp.concatenate([own, jnp.zeros((RB, D - own.shape[1]), F32)], axis=1)
    frame[...] = pltpu.roll(own, 32 * col_i, 1)

    def turn(h):
        return lanes_of(lax.rem(h + col_i, 3), 128)

    for h in range(PAIRS):
        wpk[h, z, pd, :, lanes_of(pos, 128)] = frame[:, turn(h)].astype(BF16)
    own = padded(jnp.transpose(projection[...].astype(F32)))
    own = jnp.concatenate([own, jnp.zeros((RB, 128 - own.shape[1]), F32)], axis=1)
    ptr[z, pd, :, lanes_of(pos, 128)] = pltpu.roll(own, lax.rem(96 * col_i, 128), 1).astype(BF16)
    exr[z, pd, :, lanes_of(pos, D)] = padded(expansion[...])
    rtr[z, pd, :, lanes_of(pos, D)] = padded(jnp.transpose(reduction[...].astype(F32))).astype(BF16)
    vrow = jnp.concatenate([packed_bias[...].reshape(1, -1), jnp.zeros((1, D - packed_bias.shape[0]), F32)], axis=1)
    vrow = pltpu.roll(jnp.broadcast_to(vrow, (8, D)), 32 * col_i, 1)
    bias[pos] = jnp.concatenate([vrow[:4], jnp.broadcast_to(expansion_bias[...].reshape(1, -1), (4, D))], axis=0)

    chunks = [(wpk.at[h], 128) for h in range(PAIRS)] + [(ptr, 128), (exr, D), (rtr, D)]

    def zcopy(k, d):
        ref, width = chunks[k]
        slot = ref.at[z, pd, :, lanes_of(pos, width)]
        return remote(slot, slot, zs.at[k, d - 1], zr.at[k, d - 1], zpeer(d))

    def pcopy(k, d):
        ref, width = chunks[k]
        slot = ref.at[:, pd, :, lanes_of(pos, width)]
        return remote(slot, slot, ps.at[k, d - 1], pr.at[k, d - 1], ppeer(d))

    def kcopy(k):
        ref, width = chunks[k]
        slot = ref.at[:, :, :, lanes_of(core, Y * width)]
        return remote(slot, slot, ks.at[k], kr.at[k], sibling)

    def bcopy(d):
        return remote(bias.at[pos], bias.at[pos], bs.at[d - 1], br.at[d - 1], cpeer(d))

    def to_plane(k):
        for d in range(1, Z):
            zcopy(k, d).wait_recv()
        for d in range(1, PLANE):
            pcopy(k, d).start()

    def to_sibling(k):
        for d in range(1, PLANE):
            pcopy(k, d).wait_recv()
        kcopy(k).start()

    def settle(k):
        for d in range(1, Z):
            zcopy(k, d).wait_send()
        for d in range(1, PLANE):
            pcopy(k, d).wait_send()
        kcopy(k).wait_send()

    pl.semaphore_wait(barrier, greeted)
    for k in range(len(chunks)):
        for d in range(1, Z):
            zcopy(k, d).start()
        if k == 0:
            for d in range(1, 2 * Y):
                bcopy(d).start()

    x[rows:, :] = jnp.zeros((RP - rows, D), BF16)
    up[rows:, :] = jnp.zeros((RP - rows, D), BF16)
    for h in range(PAIRS):
        qkv[h, RP:, :] = jnp.zeros((qkv.shape[1] - RP, D), BF16)
    tail = attn.shape[0] - RP + 16
    attn[RP - 16:, :] = jnp.zeros((tail, D), BF16)
    ag[RP:, :] = jnp.zeros((ag.shape[0] - RP, D), BF16)
    rinv[RP - 16:, :] = jnp.zeros((tail, D), F32)
    pgr[:, RP - 16:, :] = jnp.zeros((PAIRS, tail, D), BF16)
    fs = first_scale[...].reshape(1, D)
    fh = first_shift[...].reshape(1, D)
    ss = second_scale[...].reshape(1, D)
    sh = second_shift[...].reshape(1, D)
    prb = projection_bias[...].reshape(1, D)
    rdb = reduction_bias[...].reshape(1, D)
    cin.wait()
    cup.wait()

    def ln1(i, _):
        s = rows_of(i, SMALL)
        v = x[s, :].astype(F32)
        avg = mean(v)
        inv = lax.rsqrt(mean(v * v) - avg * avg + EPS)
        normed = (v - avg) * inv
        n1[s, :] = normed
        inv1[s, :] = jnp.broadcast_to(inv, (SMALL, 128))
        rows1[s, :] = (normed * fs + fh).astype(BF16)
        hook(i, [(nsm // 2, lambda: to_plane(0))])
        return 0

    lax.fori_loop(0, nsm, ln1, 0)
    to_plane(1)
    to_sibling(0)
    to_plane(2)
    for d in range(1, 2 * Y):
        bcopy(d).wait_recv()

    lane = lax.broadcasted_iota(jnp.int32, (KEYS, 128), 1)
    even = lane < 64
    zero = jnp.zeros((KEYS, 128), BF16)
    one = jnp.ones((KEYS, 128), BF16)
    ones_e = jnp.where(even, one, zero)
    ones_o = jnp.where(even, zero, one)

    def place(c):
        return (c % 2) * Y + c // 2

    if RV != RB:
        wide = Z * PD * RB
        r_ = lax.broadcasted_iota(jnp.int32, (D, wide), 0)
        c_ = lax.broadcasted_iota(jnp.int32, (D, wide), 1)
        pick = jnp.where(c_ == (r_ // RV) * RB + lax.rem(r_, RV), 1.0, 0.0).astype(BF16)

    def compact(v):
        v = v.reshape(Z * PD * RB, v.shape[-1])
        return v if RV == RB else nn(pick, v).astype(BF16)

    def spread(v):
        v = v.astype(BF16)
        v = v if RV == RB else tn(pick, v).astype(BF16)
        return v.reshape(Z, PD, RB, v.shape[-1])

    def merged(tile, first, second, upto):
        if first == second:
            return tile(first)
        a, b = tile(first), tile(second)
        return jnp.where(lax.broadcasted_iota(jnp.int32, a.shape, 1) < upto, a, b)

    def assemble(h):
        kcopy(h).wait_recv()
        for j, (first, second, upto) in enumerate(TILES[h]):
            wp[h, :, j * 128:(j + 1) * 128] = merged(
                lambda c: compact(wpk[h, :, :, :, place(c) * 128:(place(c) + 1) * 128]), first, second, upto)

    def bias_of(h):
        def tile(c):
            t = (h + c) % 3
            return bias[place(c), 0:1, t * 128:(t + 1) * 128]
        return jnp.concatenate([merged(tile, *t) for t in TILES[h]], axis=1)

    def window(i):
        first = i * SEQ
        base = pl.multiple_of((first // 16) * 16, 16)
        return first - base, base

    ahead = (
        [(1, lambda: to_sibling(1)), (2, lambda: to_plane(3)), (3, lambda: to_plane(4)), (5, lambda: to_plane(5))],
        [(1, lambda: to_sibling(2)), (6, lambda: to_sibling(3))],
        [(2, lambda: to_sibling(4)), (6, lambda: to_sibling(5))],
    )
    for h in range(PAIRS):
        hl = pl.ds(h * 128, 128)
        assemble(h)
        pb = bias_of(h)

        def project(i, _):
            s = rows_of(i, BIG)
            qkv[h, s, :] = (nn(rows1[s, :], wp[h]) + pb).astype(BF16)
            return 0

        lax.fori_loop(0, nbig, project, 0)

        def attend(i, _):
            off, base = window(i)
            qs = pl.ds(base, WIN)
            kk = pl.ds(base, KEYS)
            q = qkv[h, qs, 0:128]
            k = qkv[h, kk, 128:256]
            v = qkv[h, kk, 256:384]
            col = lax.broadcasted_iota(jnp.int32, (WIN, KEYS), 1) - off
            ok = (col >= 0) & (col < SEQ)
            es = []
            for m in (even, ~even):
                s = nt(q, jnp.where(m, k, zero))
                s = jnp.where(ok, s, -1e30)
                top = jnp.max(s, axis=1, keepdims=True)
                es.append(jnp.exp((s - top) * 0.125).astype(BF16))
            est[h, i, 0] = es[0]
            est[h, i, 1] = es[1]
            mix = nn(es[0], jnp.concatenate([jnp.where(even, v, zero), ones_e], axis=1)) + nn(
                es[1], jnp.concatenate([jnp.where(even, zero, v), ones_o], axis=1))
            r = 1.0 / mix[:, 128:]
            o = mix[:, :128] * r
            rid = lax.broadcasted_iota(jnp.int32, (WIN, 128), 0) - off
            mine = (rid >= 0) & (rid < SEQ)
            attn[qs, hl] = jnp.where(mine, o, attn[qs, hl].astype(F32)).astype(BF16)
            rinv[qs, hl] = jnp.where(mine, r, rinv[qs, hl])
            hook(i, ahead[h])
            return 0

        lax.fori_loop(0, images, attend, 0)

    for k in (3, 4, 5):
        kcopy(k).wait_recv()
    lane_d = lax.broadcasted_iota(jnp.int32, (D, 128), 1)
    tiles = [compact(ptr[:, :, :, place(c) * 128:(place(c) + 1) * 128]) for c in range(4)]
    pt[:, 0:128] = jnp.where(lane_d < 96, tiles[0], tiles[1])
    pt[:, 128:256] = jnp.where(lane_d < 64, tiles[1], tiles[2])
    pt[:, 256:384] = jnp.where(lane_d < 32, tiles[2], tiles[3])
    if RV != RB:
        for c in range(0, FF, D):
            exc[:, c:c + D] = compact(exr[:, :, :, c:c + D])
            rtc[:, c:c + D] = compact(rtr[:, :, :, c:c + D])

    def ex_of(a, size):
        return exc[:, a:a + size] if RV != RB else exr[:, :, :, a:a + size].reshape(D, size)

    def rt_of(a, size):
        return rtc[:, a:a + size] if RV != RB else rtr[:, :, :, a:a + size].reshape(D, size)

    exb = jnp.concatenate([bias[p, 4:5, :] for p in range(4)], axis=1)
    acc2 = rg

    def ln2(i, _):
        s = rows_of(i, SMALL)
        v = x[s, :].astype(F32) + nt(attn[s, :], pt[...]) + prb
        avg = mean(v)
        inv = lax.rsqrt(mean(v * v) - avg * avg + EPS)
        normed = (v - avg) * inv
        acc1[s, :] = v + rdb
        n2[s, :] = normed
        inv2[s, :] = jnp.broadcast_to(inv, (SMALL, 128))
        rows2[s, :] = (normed * ss + sh).astype(BF16)
        acc2[s, :] = jnp.zeros((SMALL, D), F32)
        return 0

    lax.fori_loop(0, nsm, ln2, 0)

    SLOT = 2 * D + 128

    def put(lo, width, base, value):
        at = lo
        while at < lo + width:
            p, inner = at // D, at % D
            take = min(D - inner, lo + width - at)
            gm[:, :, :, p * SLOT + base + inner:p * SLOT + base + inner + take] = spread(value[:, at - lo:at - lo + take])
            at += take

    for c in range(FF // HC):
        lo = c * HC
        cs = pl.ds(lo, HC)

        def mlp(i, bsum):
            s = rows_of(i, BIG)
            pre = nn(rows2[s, :], ex_of(lo, HC)) + exb[:, lo:lo + HC]
            ug = nn(up[s, :], rt_of(lo, HC))
            cdf = 0.5 + 0.5 * lax.erf(pre * ROOT_HALF)
            act[s, :] = (pre * cdf).astype(BF16)
            g = ug * (cdf + pre * (jnp.exp(pre * pre * -0.5) * INV_ROOT_TAU))
            hg[s, :] = g.astype(BF16)
            acc1[s, :] += nt(act[s, :], rt_of(lo, HC))
            acc2[s, :] += nt(hg[s, :], ex_of(lo, HC))
            return bsum + jnp.sum(g, axis=0, keepdims=True)

        eb[0:1, cs] = lax.fori_loop(0, nbig, mlp, jnp.zeros((1, HC), F32))
        put(lo, HC, 0, tn(rows2[...], hg[...]))
        put(lo, HC, D, tn(up[...], act[...]))

    def ln2b(i, carry):
        s = rows_of(i, SMALL)
        u = up[s, :].astype(F32)
        x[s, :] = acc1[s, :].astype(BF16)
        g = acc2[s, :]
        normed = n2[s, :]
        inv = inv2[s, 0:1]
        scaled = g * ss
        d = u + inv * (scaled - mean(scaled) - normed * mean(scaled * normed))
        rg[s, :] = d
        rgb[s, :] = d.astype(BF16)
        ag[s, :] = nn(d.astype(BF16), pt[...]).astype(BF16)
        terms = (d, u, g * normed, g)
        return tuple(a + jnp.sum(t, axis=0, keepdims=True) for a, t in zip(carry, terms))

    zr1 = jnp.zeros((1, D), F32)
    sums = lax.fori_loop(0, nsm, ln2b, (zr1,) * 4)
    vec[...] = jnp.zeros(vec.shape, F32)
    for r, t in zip((0, 1, 4, 5), sums):
        vec[r:r + 1, :] = t
    gj = tn(rgb[...], attn[0:RP, :]).astype(BF16)
    t0, t1, t2 = gj[:, 0:128], gj[:, 128:256], gj[:, 256:384]
    for c, t in enumerate((t0, jnp.where(lane_d < 64, t1, t0), jnp.where(lane_d < 64, t2, t1), t2)):
        p = place(c) * SLOT
        gm[:, :, :, p + 2 * D:p + SLOT] = spread(t)
    cout = pltpu.make_async_copy(x.at[pl.ds(0, rows)], out_hbm, csem.at[0])
    cout.start()

    gsend = [gm] + [gh.at[h] for h in range(PAIRS)]
    r1s = [rm1] + [rh1.at[h] for h in range(PAIRS)]
    r2s = [rm2] + [rh2.at[h] for h in range(PAIRS)]
    r3s = [rm3] + [rh3.at[h] for h in range(PAIRS)]
    s1s = [sm1] + [sh1.at[h] for h in range(PAIRS)]
    s2s = [sm2] + [sh2.at[h] for h in range(PAIRS)]
    widths = [SLOT] + [128] * PAIRS

    def g1(k):
        half = Y * widths[k]
        return remote(gsend[k].at[:, :, :, lanes_of(1 - core, half)], r1s[k], gs.at[k, 0], gr_.at[k, 0], sibling)

    def g2(k, d):
        pp, yy = pplace(d)
        return remote(s1s[k].at[:, pp, :, lanes_of(yy, widths[k])], r2s[k].at[d - 1],
                      gs.at[k, d], gr_.at[k, d], ppeer(d))

    def g3(k, d):
        return remote(s2s[k].at[lax.rem(z + d, Z)], r3s[k].at[d - 1],
                      gs.at[k, PLANE - 1 + d], gr_.at[k, PLANE - 1 + d], zpeer(d))

    def sum1(k):
        half = Y * widths[k]
        g1(k).wait_recv()
        s1s[k][...] = (gsend[k][:, :, :, lanes_of(core, half)].astype(F32) + r1s[k][...].astype(F32)).astype(BF16)
        for d in range(1, PLANE):
            g2(k, d).start()

    def sum2(k):
        for d in range(1, PLANE):
            g2(k, d).wait_recv()
        total = s1s[k][:, pd, :, lanes_of(y, widths[k])].astype(F32)
        for d in range(1, PLANE):
            total += r2s[k][d - 1].astype(F32)
        s2s[k][...] = total.astype(BF16)
        for d in range(1, Z):
            g3(k, d).start()

    def sum3(k):
        for d in range(1, Z):
            g3(k, d).wait_recv()
        total = s2s[k][z].astype(F32)
        for d in range(1, Z):
            total += r3s[k][d - 1].astype(F32)
        return total

    def sent(k):
        g1(k).wait_send()
        for d in range(1, PLANE):
            g2(k, d).wait_send()
        for d in range(1, Z):
            g3(k, d).wait_send()

    g1(0).start()

    behind = (
        [(2, lambda: sum1(0))],
        [(0, lambda: sum1(1)), (3, lambda: sum2(0)), (6, lambda: sum2(1))],
        [(0, lambda: sum1(2)), (6, lambda: sum2(2))],
    )
    for h in range(PAIRS):
        hl = pl.ds(h * 128, 128)

        def attend_back(i, _):
            off, base = window(i)
            qs = pl.ds(base, WIN)
            kk = pl.ds(base, KEYS)
            q = qkv[h, qs, 0:128]
            k = qkv[h, kk, 128:256]
            v = qkv[h, kk, 256:384]
            rid = lax.broadcasted_iota(jnp.int32, (WIN, 128), 0) - off
            mine = (rid >= 0) & (rid < SEQ)
            do = jnp.where(mine, ag[qs, hl].astype(F32) * rinv[qs, hl], 0.0)
            dob = do.astype(BF16)
            xx = jnp.concatenate([dob, (do * attn[qs, hl].astype(F32)).astype(BF16)], axis=1)
            ev = even[:WIN]
            zw = zero[:WIN]
            e0 = est[h, i, 0]
            e1 = est[h, i, 1]
            d0 = (e0 * nt(xx, jnp.concatenate([jnp.where(even, v, zero), -ones_e], axis=1))).astype(BF16)
            d1 = (e1 * nt(xx, jnp.concatenate([jnp.where(even, zero, v), -ones_o], axis=1))).astype(BF16)
            dq = (nn(d0, jnp.where(even, k, zero)) + nn(d1, jnp.where(even, zero, k))) * 0.125
            dk = (tn(d0, jnp.where(ev, q, zw)) + tn(d1, jnp.where(ev, zw, q))) * 0.125
            dv = tn(e0, jnp.where(ev, dob, zw)) + tn(e1, jnp.where(ev, zw, dob))
            old = pgr[h, qs, :].astype(F32)
            pgr[h, qs, 0:128] = jnp.where(mine, dq, old[:, 0:128]).astype(BF16)
            pgr[h, qs, 128:256] = jnp.where(mine, dk[:WIN], old[:, 128:256]).astype(BF16)
            pgr[h, qs, 256:384] = jnp.where(mine, dv[:WIN], old[:, 256:384]).astype(BF16)
            hook(i, behind[h])
            return 0

        lax.fori_loop(0, images, attend_back, 0)
        gp = tn(rows1[...], pgr[h, 0:RP, :])
        for c, j in enumerate(SHARES[h]):
            gh[h, :, :, :, place(c) * 128:(place(c) + 1) * 128] = spread(gp[:, j * 128:(j + 1) * 128])
        g1(1 + h).start()

        def bias_sum(i, carry):
            s = rows_of(i, SMALL)
            return carry + jnp.sum(pgr[h, s, :].astype(F32), axis=0, keepdims=True)

        vec[6 + h:7 + h, :] = lax.fori_loop(0, nsm, bias_sum, zr1)

    def ln1b(i, carry):
        s = rows_of(i, SMALL)
        g = nt(pgr[0, s, :], wp[0]) + nt(pgr[1, s, :], wp[1]) + nt(pgr[2, s, :], wp[2])
        normed = n1[s, :]
        inv = inv1[s, 0:1]
        scaled = g * fs
        rg[s, :] = rg[s, :] + inv * (scaled - mean(scaled) - normed * mean(scaled * normed))
        terms = (g * normed, g)
        hook(i, [(3, lambda: sum1(3)), (nsm - 1, lambda: sum2(3))])
        return tuple(a + jnp.sum(t, axis=0, keepdims=True) for a, t in zip(carry, terms))

    sums = lax.fori_loop(0, nsm, ln1b, (zr1,) * 2)
    cg = pltpu.make_async_copy(rg.at[pl.ds(0, rows)], grad_hbm, csem.at[1])
    cg.start()

    for r, t in zip((2, 3), sums):
        vec[r:r + 1, :] = t
    for p in range(4):
        vec[9 + p:10 + p, :] = eb[0:1, p * D:(p + 1) * D]
    kv = len(gsend)

    def v1():
        return remote(vec, vr1, gs.at[kv, 0], gr_.at[kv, 0], sibling)

    def v2(d):
        return remote(vsum1, vr2.at[plane], gs.at[kv, d], gr_.at[kv, d], ppeer(d))

    def v3(d):
        return remote(vr3.at[z], vr3.at[z], gs.at[kv, PLANE - 1 + d], gr_.at[kv, PLANE - 1 + d], zpeer(d))

    v1().start()
    def finish_mlp():
        total = sum3(0)
        o_expansion[...] = total[:RV, 0:D]
        o_reduction[...] = jnp.transpose(total[:, D:2 * D])[:, :RV]
        t = pltpu.roll(total[:, 2 * D:], lax.rem(128 - lax.rem(96 * col_i, 128), 128), 1)
        o_projection[...] = jnp.transpose(t)[:96, :RV]

    finish_mlp()
    v1().wait_recv()
    vsum1[...] = vec[...] + vr1[...]
    for d in range(1, PLANE):
        v2(d).start()
    vr2[plane] = vsum1[...]
    for h in range(PAIRS - 1):
        frame[:, turn(h)] = sum3(1 + h)
    for d in range(1, PLANE):
        v2(d).wait_recv()
    total = vr2[0]
    for q in range(1, PLANE):
        total += vr2[q]
    vr3[z] = total
    for d in range(1, Z):
        v3(d).start()
    frame[:, turn(PAIRS - 1)] = sum3(PAIRS)
    back = lax.rem(D - 32 * col_i, D)
    wide_c = o_packed.shape[1]
    o_packed[...] = pltpu.roll(frame[...], back, 1)[:RV, :wide_c]
    for d in range(1, Z):
        v3(d).wait_recv()
    total = vr3[0]
    for q in range(1, Z):
        total += vr3[q]
    vec_all = total
    v1().wait_send()
    vec[...] = vec_all
    turned = pltpu.roll(vec_all[0:8, :], lax.rem(D - 96 * col_i, D), 1)
    for r, ref in enumerate((o_prb, o_rb, o_fs, o_fh, o_ss, o_sh)):
        ref[...] = turned[r:r + 1, :96].reshape(96)
    for h, j in enumerate((jnp.minimum(col_i, 2), (col_i + 1) // 2, jnp.maximum(col_i - 1, 0))):
        frame[0:1, turn(h)] = vec[6 + h:7 + h, lanes_of(j, 128)]
    o_pb[...] = pltpu.roll(frame[0:8, :], back, 1)[0:1, :wide_c].reshape(wide_c)
    o_eb[...] = vec[pl.ds(9 + pos, 1), :].reshape(D)

    for k in range(len(chunks)):
        settle(k)
    for d in range(1, 2 * Y):
        bcopy(d).wait_send()
    for k in range(len(gsend)):
        sent(k)
    for d in range(1, PLANE):
        v2(d).wait_send()
    for d in range(1, Z):
        v3(d).wait_send()
    cout.wait()
    cg.wait()


def finish_kernel(rows, *refs):
    n = 14
    ins, outs, (bx, bg, sem) = refs[:n], refs[n:2 * n], refs[2 * n:]
    a = pltpu.make_async_copy(ins[0], bx, sem.at[0])
    b = pltpu.make_async_copy(ins[1], bg, sem.at[1])
    a.start()
    b.start()
    for i in range(2, n):
        outs[i][...] = ins[i][...]
    a.wait()
    c = pltpu.make_async_copy(bx, outs[0], sem.at[0])
    c.start()
    b.wait()
    d = pltpu.make_async_copy(bg, outs[1], sem.at[1])
    d.start()
    c.wait()
    d.wait()


def body(dps, cols, tokens, packed, packed_bias, projection, projection_bias, expansion, expansion_bias, reduction,
         reduction_bias, first_scale, first_shift, second_scale, second_shift, upstream):
    args = (tokens, packed, packed_bias, projection, projection_bias, expansion, expansion_bias, reduction,
            reduction_bias, first_scale, first_shift, second_scale, second_shift, upstream)
    rows = tokens.shape[0]
    images = rows // SEQ
    Z = min(4, dps)
    PD = dps // Z
    Y = cols // 2
    RV = packed.shape[0]
    RB = -(-RV // 16) * 16
    PLANE = PD * Y
    RP = -(-rows // BIG) * BIG
    XP = RP + 80
    cfg = (Z, PD, Y, RB, RV, rows)
    V = pl.BlockSpec(memory_space=pltpu.VMEM)
    A = pl.BlockSpec(memory_space=pl.ANY)
    S = jax.ShapeDtypeStruct
    vm = pltpu.VMEM
    dma = pltpu.SemaphoreType.DMA
    SLOT = 2 * D + 128
    small = RV != RB
    outs = (
        S((rows, D), BF16), S((rows, D), F32),
        S(packed.shape, F32), S(projection.shape, F32), S(expansion.shape, F32), S(reduction.shape, F32),
        S(packed_bias.shape, F32), S((D // cols,), F32), S(expansion_bias.shape, F32),
    ) + (S((D // cols,), F32),) * 5
    scratch = [
        vm((RP, D), BF16), vm((RP, D), BF16),
        vm((RP, D), F32), vm((RP, D), BF16),
        vm((PAIRS, XP, D), BF16), vm((XP, D), BF16),
        vm((PAIRS, images, 2, WIN, KEYS), BF16), vm((XP, D), F32),
        vm((RP, D), F32), vm((RP, D), BF16),
        vm((RP, D), F32), vm((RP, D), F32),
        vm((RP, HC), BF16), vm((RP, HC), BF16),
        vm((RP, D), BF16), vm((XP, D), BF16),
        vm((PAIRS, XP, D), BF16), vm((RP, 128), F32), vm((RP, 128), F32),
        vm((PAIRS, Z, PD, RB, 4 * 128), BF16), vm((Z, PD, RB, 4 * 128), BF16),
        vm((Z, PD, RB, FF), BF16), vm((Z, PD, RB, FF), BF16),
        vm((PAIRS, D, D), BF16), vm((D, D), BF16),
        vm((D, FF) if small else (16, 128), BF16), vm((D, FF) if small else (16, 128), BF16),
        vm((4, 8, D), F32),
        vm((Z, PD, RB, 4 * SLOT), BF16), vm((PAIRS, Z, PD, RB, 4 * 128), BF16),
        vm((Z, PD, RB, Y * SLOT), BF16), vm((PLANE - 1, Z, RB, SLOT), BF16), vm((Z - 1, RB, SLOT), BF16),
        vm((PAIRS, Z, PD, RB, Y * 128), BF16), vm((PAIRS, PLANE - 1, Z, RB, 128), BF16), vm((PAIRS, Z - 1, RB, 128), BF16),
        vm((Z, PD, RB, Y * SLOT), BF16), vm((Z, RB, SLOT), BF16),
        vm((PAIRS, Z, PD, RB, Y * 128), BF16), vm((PAIRS, Z, RB, 128), BF16),
        vm((RB, D), F32), vm((16, D), F32), vm((16, D), F32),
        vm((16, D), F32), vm((PLANE, 16, D), F32), vm((Z, 16, D), F32), vm((8, FF), F32),
        dma((2,)), dma((6, Z - 1)), dma((6, Z - 1)), dma((6, PLANE - 1)), dma((6, PLANE - 1)), dma((6,)), dma((6,)),
        dma((2 * Y - 1,)), dma((2 * Y - 1,)), dma((5, PLANE + Z - 1)), dma((5, PLANE + Z - 1)),
    ]
    got = pl.pallas_call(
        functools.partial(layer_kernel, cfg),
        out_shape=outs,
        in_specs=[A] + [V] * 12 + [A],
        out_specs=(A, A) + (V,) * 12,
        scratch_shapes=scratch,
        compiler_params=pltpu.CompilerParams(vmem_limit_bytes=67043328, collective_id=0, has_side_effects=True),
    )(*args)
    return pl.pallas_call(
        functools.partial(finish_kernel, rows),
        out_shape=outs,
        in_specs=[A, A] + [V] * 12,
        out_specs=(A, A) + (V,) * 12,
        scratch_shapes=[vm((rows, D), BF16), vm((rows, D), F32), dma((2,))],
    )(*got)


def solution(mesh):
    placed = (
        P(("dp", "col"), None), P("dp", "col"), P("col"), P("col", "dp"), P(), P("dp", "col"), P("col"),
        P("col", "dp"), P(), P(), P(), P(), P(), P(("dp", "col"), None),
    )
    return jax.shard_map(
        functools.partial(body, mesh.shape["dp"], mesh.shape["col"]),
        mesh=mesh,
        in_specs=placed,
        out_specs=(
            P(("dp", "col"), None), P(("dp", "col"), None),
            P("dp", "col"), P("col", "dp"), P("dp", "col"), P("col", "dp"),
        ) + (P("col"),) * 8,
        check_vma=False,
    )
```

```python
import functools

import jax
import jax.numpy as jnp
from jax import lax
from jax.experimental import pallas as pl
from jax.experimental.pallas import tpu as pltpu
from jax.sharding import PartitionSpec as P

SEQ = 197
EPS = 1e-06
ROOT_HALF = 0.7071067811865476
INV_ROOT_TAU = 0.3989422804014327
F32, BF16 = jnp.float32, jnp.bfloat16
MESH = pl.DeviceIdType.MESH
D = 384
FF = 1536
PAIRS = 3
WIN = 224
KEYS = 256
BIG = 528
SMALL = 176
HC = 512


def nn(a, b):
    return lax.dot_general(a, b, (((1,), (0,)), ((), ())), preferred_element_type=F32)


def nt(a, b):
    return lax.dot_general(a, b, (((1,), (1,)), ((), ())), preferred_element_type=F32)


def tn(a, b):
    return lax.dot_general(a, b, (((0,), (0,)), ((), ())), preferred_element_type=F32)


def rows_of(i, size):
    return pl.ds(pl.multiple_of(i * size, 16), size)


def lanes_of(i, size):
    return pl.ds(pl.multiple_of(i * size, 128), size)


def mean(x):
    return jnp.sum(x, axis=1, keepdims=True) * (1.0 / x.shape[1])


def hook(i, steps):
    for at, step in steps:
        pl.when(i == at)(step)


def loop(lo, hi, function, init):
    with jax.named_scope(function.__name__):
        return lax.fori_loop(lo, hi, function, init)


def named(function):
    def inner(*a):
        with jax.named_scope(function.__name__ + "_".join(str(v) for v in a if isinstance(v, int))):
            return function(*a)
    return inner


TILES = (
    ((0, 0, 128), (1, 1, 128), (2, 3, 96)),
    ((0, 0, 128), (1, 2, 64), (3, 3, 128)),
    ((0, 1, 32), (2, 2, 128), (3, 3, 128)),
)
SHARES = ((0, 1, 2, 2), (0, 1, 1, 2), (0, 0, 1, 2))


def layer_kernel(cfg, *refs):
    Z, PD, Y, RB, RV, rows = cfg
    PLANE = PD * Y
    RP = -(-rows // BIG) * BIG
    images = rows // SEQ
    nsm, nbig = RP // SMALL, RP // BIG
    tokens, upstream, out_hbm, grad_hbm, small_hbm = refs[0], refs[13], refs[14], refs[15], refs[16]
    outside, refs = refs[1:13], refs[17:]
    (packed, packed_bias, projection, projection_bias, expansion, expansion_bias, reduction,
     reduction_bias, first_scale, first_shift, second_scale, second_shift, small,
     x, up, n1, rows1, qkv, attn, est, rinv, n2, rows2, acc1, rg, act, hg, rgb, ag, pgr, inv1, inv2,
     wpk, ptr, exr, rtr, wp, pt, exc, rtc, bias,
     gm, gh, rm1, rm2, rm3, rh1, rh2, rh3, sm1, sm2, sh1, sh2, frame, vec, vsum1, vr1, vr2, vr3, vall, gbuf,
     isem, csem, asend, zfirst, zr, pr, kr, bs, gsend, g1r, g2r, g3r, vs) = refs

    dp_i, col_i = lax.axis_index("dp"), lax.axis_index("col")
    z, pd = dp_i // PD, lax.rem(dp_i, PD)
    y, core = col_i // 2, lax.rem(col_i, 2)
    pos = core * Y + y
    plane = pd * Y + y

    def device(zz, pp, yy, cc):
        return (zz * PD + pp, yy * 2 + cc)

    def znear(s):
        rising = jnp.where(s < z, s, s + 1)
        down = Z - 1 - s
        falling = jnp.where(down > z, down, down - 1)
        return jnp.where(2 * z < Z, rising, falling)

    def zpeer(s):
        return device(znear(s - 1), pd, y, core)

    def pplace(d):
        q = lax.rem(plane + d, PLANE)
        return q // Y, lax.rem(q, Y)

    def ppeer(d):
        pp, yy = pplace(d)
        return device(z, pp, yy, core)

    sibling = device(z, pd, y, 1 - core)

    def cpeer(d):
        return (dp_i, lax.rem(col_i + d, 2 * Y))

    def remote(src, dst, send, recv, to):
        return pltpu.make_async_remote_copy(
            src_ref=src, dst_ref=dst, send_sem=send, recv_sem=recv, device_id=to, device_id_type=MESH)

    barrier = pltpu.get_barrier_semaphore()
    near = [zpeer(d) for d in range(1, Z)] + [ppeer(d) for d in range(1, PLANE)]
    near += [cpeer(d) for d in range(1, 2 * Y) if d != Y]
    for to in near + ([sibling] if Y == 1 else []):
        pl.semaphore_signal(barrier, inc=1, device_id=to, device_id_type=MESH)
    greeted = len(near)

    cin = pltpu.make_async_copy(tokens, x.at[pl.ds(0, rows)], csem.at[0])
    cup = pltpu.make_async_copy(upstream, up.at[pl.ds(0, rows)], csem.at[1])
    inside = (packed, packed_bias, projection, projection_bias, expansion, expansion_bias, reduction,
              reduction_bias, first_scale, first_shift, second_scale, second_shift)
    loads = [pltpu.make_async_copy(a, b, isem.at[n]) for n, (a, b) in enumerate(zip(outside, inside))]
    for n in (0, 2, 4, 6, 1, 5, 3, 7, 8, 9, 10, 11):
        loads[n].start()
    cin.start()
    cup.start()
    for load in loads:
        load.wait()

    def padded(v):
        return v if RV == RB else jnp.concatenate([v, jnp.zeros((RB - RV, v.shape[1]), v.dtype)], axis=0)

    own = padded(packed[...].astype(F32))
    own = jnp.concatenate([own, jnp.zeros((RB, D - own.shape[1]), F32)], axis=1)
    frame[...] = pltpu.roll(own, 32 * col_i, 1)

    def turn(h):
        return lanes_of(lax.rem(h + col_i, 3), 128)

    for h in range(PAIRS):
        wpk[h, z, pd, :, lanes_of(pos, 128)] = frame[:, turn(h)].astype(BF16)
    own = padded(projection[...].astype(F32))
    own = jnp.concatenate([own, jnp.zeros((RB, 128 - own.shape[1]), F32)], axis=1)
    ptr[z, pd, :, lanes_of(pos, 128)] = pltpu.roll(own, lax.rem(96 * col_i, 128), 1).astype(BF16)
    for j in range(FF // HC):
        exr[j, z, pd, :, lanes_of(pos, 128)] = padded(expansion[:, j * 128:(j + 1) * 128])
        rtr[j, z, pd, :, lanes_of(pos, 128)] = padded(reduction[:, j * 128:(j + 1) * 128])
    vrow = jnp.concatenate([packed_bias[...].reshape(1, -1), jnp.zeros((1, D - packed_bias.shape[0]), F32)], axis=1)
    vrow = pltpu.roll(jnp.broadcast_to(vrow, (8, D)), 32 * col_i, 1)
    bias[pos] = jnp.concatenate([vrow[:4], jnp.broadcast_to(expansion_bias[...].reshape(1, -1), (4, D))], axis=0)

    chunks = [wpk.at[h] for h in range(PAIRS)] + [ptr]
    for j in range(FF // HC):
        chunks += [exr.at[j], rtr.at[j]]
    mine_l = lanes_of(pos, 128)

    def span(slots):
        return inv1.at[0:slots * RB // 2]

    def vspan(count):
        return n1.at[0:count * 16]

    def arrived(sem, ref):
        remote(ref, ref, vs.at[0], sem, sibling).wait_recv()

    def left(sem, ref):
        remote(ref, ref, sem, vs.at[0], sibling).wait_send()

    def zcopy(k, d):
        slot = chunks[k].at[z, pd, :, mine_l]
        return remote(slot, slot, asend.at[k], zfirst.at[z] if k == 0 else zr.at[k], zpeer(d))

    def pcopy(k, d):
        slot = chunks[k].at[:, pd, :, mine_l]
        return remote(slot, slot, asend.at[k], pr.at[k], ppeer(d))

    def qcopy(d, q):
        slot = chunks[0].at[q, pd, :, mine_l]
        return remote(slot, slot, asend.at[0], pr.at[0], ppeer(d))

    def kcopy(k):
        slot = chunks[k].at[:, :, :, lanes_of(core, Y * 128)]
        return remote(slot, slot, asend.at[k], kr.at[k], sibling)

    def bcopy(d):
        return remote(bias.at[pos], bias.at[pos], bs.at[0], bs.at[1], cpeer(d))

    @named
    def to_plane(k):
        arrived(zr.at[k], span(Z - 1))
        for d in range(1, PLANE):
            pcopy(k, d).start()

    @named
    def to_sibling(k):
        arrived(pr.at[k], span((PLANE - 1) * Z))
        kcopy(k).start()

    ALL = Z - 1 + (PLANE - 1) * Z + PLANE * Z

    with jax.named_scope("barrier"):
        pl.semaphore_wait(barrier, greeted)
    for k in range(len(chunks)):
        for d in range(1, Z):
            zcopy(k, d).start()
        if k == 0:
            for d in range(1, PLANE):
                qcopy(d, z).start()
            for d in range(1, 2 * Y):
                bcopy(d).start()

    x[rows:, :] = jnp.zeros((RP - rows, D), BF16)
    up[rows:, :] = jnp.zeros((RP - rows, D), BF16)
    for h in range(PAIRS):
        qkv[h, RP:, :] = jnp.zeros((qkv.shape[1] - RP, D), BF16)
    tail = attn.shape[0] - RP + 16
    attn[RP - 16:, :] = jnp.zeros((tail, D), BF16)
    ag[RP:, :] = jnp.zeros((ag.shape[0] - RP, D), BF16)
    rinv[RP - 16:, :] = jnp.zeros((tail, D), F32)
    pgr[:, RP - 16:, :] = jnp.zeros((PAIRS, tail, D), BF16)
    fs = first_scale[...].reshape(1, D)
    fh = first_shift[...].reshape(1, D)
    ss = second_scale[...].reshape(1, D)
    sh = second_shift[...].reshape(1, D)
    prb = projection_bias[...].reshape(1, D)
    rdb = reduction_bias[...].reshape(1, D)
    cin.wait()
    cup.wait()

    def ln1(i, _):
        s = rows_of(i, SMALL)
        v = x[s, :].astype(F32)
        avg = mean(v)
        inv = lax.rsqrt(mean(v * v) - avg * avg + EPS)
        normed = (v - avg) * inv
        n1[s, :] = normed
        inv1[s, :] = jnp.broadcast_to(inv, (SMALL, 128))
        rows1[s, :] = (normed * fs + fh).astype(BF16)
        return 0

    @named
    def pass_on(d):
        q = znear(d - 1)
        arrived(zfirst.at[q], chunks[0].at[q, pd, :, mine_l])
        for e in range(1, PLANE):
            qcopy(e, q).start()

    loop(0, nsm, ln1, 0)
    for d in range(1, Z):
        pass_on(d)
    to_plane(1)
    with jax.named_scope("plane0"):
        arrived(pr.at[0], span((PLANE - 1) * Z))
    kcopy(0).start()
    to_plane(2)
    arrived(bs.at[1], n1.at[0:8 * (2 * Y - 1)])

    lane = lax.broadcasted_iota(jnp.int32, (KEYS, 128), 1)
    even = lane < 64
    zero = jnp.zeros((KEYS, 128), BF16)
    one = jnp.ones((KEYS, 128), BF16)
    ones_e = jnp.where(even, one, zero)
    ones_o = jnp.where(even, zero, one)

    def place(c):
        return (c % 2) * Y + c // 2

    if RV != RB:
        wide = Z * PD * RB
        r_ = lax.broadcasted_iota(jnp.int32, (D, wide), 0)
        c_ = lax.broadcasted_iota(jnp.int32, (D, wide), 1)
        pick = jnp.where(c_ == (r_ // RV) * RB + lax.rem(r_, RV), 1.0, 0.0).astype(BF16)

    def compact(v):
        v = v.reshape(Z * PD * RB, v.shape[-1])
        return v if RV == RB else nn(pick, v).astype(BF16)

    def spread(v):
        v = v.astype(BF16)
        v = v if RV == RB else tn(pick, v).astype(BF16)
        return v.reshape(Z, PD, RB, v.shape[-1])

    def merged(tile, first, second, upto):
        if first == second:
            return tile(first)
        a, b = tile(first), tile(second)
        return jnp.where(lax.broadcasted_iota(jnp.int32, a.shape, 1) < upto, a, b)

    @named
    def assemble(h):
        kcopy(h).wait_recv()
        for j, (first, second, upto) in enumerate(TILES[h]):
            wp[h, :, j * 128:(j + 1) * 128] = merged(
                lambda c: compact(wpk[h, :, :, :, place(c) * 128:(place(c) + 1) * 128]), first, second, upto)

    def bias_of(h):
        def tile(c):
            t = (h + c) % 3
            return bias[place(c), 0:1, t * 128:(t + 1) * 128]
        return jnp.concatenate([merged(tile, *t) for t in TILES[h]], axis=1)

    def window(i):
        first = i * SEQ
        base = pl.multiple_of((first // 16) * 16, 16)
        return first - base, base

    ahead = (
        [(1, lambda: to_sibling(1)), (2, lambda: to_plane(3)), (3, lambda: to_plane(4)), (4, lambda: to_plane(5)),
         (5, lambda: to_plane(6)), (6, lambda: to_plane(7)), (7, lambda: to_sibling(2))],
        [(1, lambda: to_plane(8)), (2, lambda: to_plane(9)), (4, lambda: to_sibling(3)), (7, lambda: to_sibling(4))],
        [(1, lambda: to_sibling(5)), (4, lambda: to_sibling(6)), (7, lambda: to_sibling(7))],
    )
    for h in range(PAIRS):
        hl = pl.ds(h * 128, 128)
        assemble(h)
        pb = bias_of(h)

        def project(i, _):
            s = rows_of(i, BIG)
            qkv[h, s, :] = (nn(rows1[s, :], wp[h]) + pb).astype(BF16)
            return 0

        loop(0, nbig, project, 0)

        def attend(i, _):
            off, base = window(i)
            qw = pl.ds(base, WIN)
            kk = pl.ds(base, KEYS)
            q = qkv[h, qw, 0:128]
            k = qkv[h, kk, 128:256]
            v = qkv[h, kk, 256:384]
            col = lax.broadcasted_iota(jnp.int32, (WIN, KEYS), 1) - off
            ok = (col >= 0) & (col < SEQ)
            es = []
            for m in (even, ~even):
                s = nt(q, jnp.where(m, k, zero))
                s = jnp.where(ok, s, -1e30)
                top = jnp.max(s, axis=1, keepdims=True)
                es.append(jnp.exp((s - top) * 0.125).astype(BF16))
            est[h, i, 0] = es[0]
            est[h, i, 1] = es[1]
            mix = nn(es[0], jnp.concatenate([jnp.where(even, v, zero), ones_e], axis=1)) + nn(
                es[1], jnp.concatenate([jnp.where(even, zero, v), ones_o], axis=1))
            r = 1.0 / mix[:, 128:]
            o = mix[:, :128] * r
            rid = lax.broadcasted_iota(jnp.int32, (WIN, 128), 0) - off
            mine = (rid >= 0) & (rid < SEQ)
            attn[qw, hl] = jnp.where(mine, o, attn[qw, hl].astype(F32)).astype(BF16)
            rinv[qw, hl] = jnp.where(mine, r, rinv[qw, hl])
            hook(i, ahead[h])
            return 0

        loop(0, images, attend, 0)

    kcopy(3).wait_recv()
    lane_d = lax.broadcasted_iota(jnp.int32, (D, 128), 1)
    tiles = [compact(ptr[:, :, :, place(c) * 128:(place(c) + 1) * 128]) for c in range(4)]
    pt[:, 0:128] = jnp.where(lane_d < 96, tiles[0], tiles[1])
    pt[:, 128:256] = jnp.where(lane_d < 64, tiles[1], tiles[2])
    pt[:, 256:384] = jnp.where(lane_d < 32, tiles[2], tiles[3])
    def exb_of(j):
        return jnp.concatenate([bias[p, 4:5, j * 128:(j + 1) * 128] for p in range(4)], axis=1)

    acc2 = rg

    def ln2(i, _):
        s = rows_of(i, SMALL)
        v = x[s, :].astype(F32) + nt(attn[s, :], pt[...]) + prb
        avg = mean(v)
        inv = lax.rsqrt(mean(v * v) - avg * avg + EPS)
        normed = (v - avg) * inv
        acc1[s, :] = v + rdb
        n2[s, :] = normed
        inv2[s, :] = jnp.broadcast_to(inv, (SMALL, 128))
        rows2[s, :] = (normed * ss + sh).astype(BF16)
        return 0

    loop(0, nsm, ln2, 0)

    def part(big, small, k):
        return big.at[k] if k < PAIRS else small.at[k - PAIRS]

    def width(k):
        return 256 if k < PAIRS else 128

    def g1(k):
        half = Y * width(k)
        return remote(part(gm, gh, k).at[:, :, :, lanes_of(1 - core, half)], part(rm1, rh1, k),
                      gsend.at[k], g1r.at[k], sibling)

    def g2(k, d):
        pp, yy = pplace(d)
        return remote(part(sm1, sh1, k).at[:, pp, :, lanes_of(yy, width(k))], part(rm2, rh2, k).at[d - 1],
                      gsend.at[k], g2r.at[k], ppeer(d))

    def g3(k, d):
        return remote(part(sm2, sh2, k).at[znear(d - 1)], part(rm3, rh3, k).at[z], gsend.at[k], g3r.at[k], zpeer(d))

    @named
    def sum1(k):
        g1(k).wait_recv()
        own = part(gm, gh, k)[:, :, :, lanes_of(core, Y * width(k))]
        part(sm1, sh1, k)[...] = (own.astype(F32) + part(rm1, rh1, k)[...].astype(F32)).astype(BF16)
        for d in range(1, PLANE):
            g2(k, d).start()

    @named
    def sum2(k):
        arrived(g2r.at[k], span((PLANE - 1) * Z * (width(k) // 128)))
        total = part(sm1, sh1, k)[:, pd, :, lanes_of(y, width(k))].astype(F32)
        for d in range(1, PLANE):
            total += part(rm2, rh2, k)[d - 1].astype(F32)
        part(sm2, sh2, k)[...] = total.astype(BF16)
        for d in range(1, Z):
            g3(k, d).start()

    @named
    def sum3(k):
        arrived(g3r.at[k], span((Z - 1) * (width(k) // 128)))
        total = part(sm2, sh2, k)[z].astype(F32)
        for d in range(1, Z):
            total += part(rm3, rh3, k)[znear(d - 1)].astype(F32)
        return total

    vec[...] = jnp.zeros(vec.shape, F32)
    spot = (
        [(1, lambda: to_sibling(8)), (2, lambda: to_sibling(9))],
        [(1, lambda: sum1(0))],
        [(1, lambda: sum1(1)), (2, lambda: sum2(0))],
    )
    for j in range(FF // HC):
        for k in (4 + 2 * j, 5 + 2 * j):
            kcopy(k).wait_recv()
        if RV != RB:
            exc[...] = compact(exr[j])
            rtc[...] = compact(rtr[j])

        def ex_of():
            return exc[...] if RV != RB else exr[j].reshape(D, HC)

        def rt_of():
            return rtc[...] if RV != RB else rtr[j].reshape(D, HC)

        exb = exb_of(j)

        def mlp(i, bsum):
            s = rows_of(i, BIG)
            pre = nn(rows2[s, :], ex_of()) + exb
            ug = nn(up[s, :], rt_of())
            cdf = 0.5 + 0.5 * lax.erf(pre * ROOT_HALF)
            act[s, :] = (pre * cdf).astype(BF16)
            g = ug * (cdf + pre * (jnp.exp(pre * pre * -0.5) * INV_ROOT_TAU))
            hg[s, :] = g.astype(BF16)
            acc1[s, :] += nt(act[s, :], rt_of())
            back = nt(hg[s, :], ex_of())
            acc2[s, :] = back if j == 0 else acc2[s, :] + back
            hook(i, spot[j])
            return bsum + jnp.sum(g, axis=0, keepdims=True)

        bsum = loop(0, nbig, mlp, jnp.zeros((1, HC), F32))
        for p in range(4):
            vec[9 + p:10 + p, j * 128:(j + 1) * 128] = bsum[:, p * 128:(p + 1) * 128]
        for base, g in ((0, tn(rows2[...], hg[...])), (128, tn(up[...], act[...]))):
            for p in range(4):
                gm[j, :, :, :, p * 256 + base:p * 256 + base + 128] = spread(g[:, p * 128:(p + 1) * 128])
        g1(j).start()

    def ln2b(i, carry):
        s = rows_of(i, SMALL)
        u = up[s, :].astype(F32)
        x[s, :] = acc1[s, :].astype(BF16)
        g = acc2[s, :]
        normed = n2[s, :]
        inv = inv2[s, 0:1]
        scaled = g * ss
        d = u + inv * (scaled - mean(scaled) - normed * mean(scaled * normed))
        rg[s, :] = d
        rgb[s, :] = d.astype(BF16)
        ag[s, :] = nn(d.astype(BF16), pt[...]).astype(BF16)
        terms = (d, u, g * normed, g)
        hook(i, [(nsm // 2, lambda: sum1(2)), (nsm - 1, lambda: sum2(1))])
        return tuple(a + jnp.sum(t, axis=0, keepdims=True) for a, t in zip(carry, terms))

    zr1 = jnp.zeros((1, D), F32)
    sums = loop(0, nsm, ln2b, (zr1,) * 4)
    for r, t in zip((0, 1, 4, 5), sums):
        vec[r:r + 1, :] = t
    gj = tn(rgb[...], attn[0:RP, :]).astype(BF16)
    t0, t1, t2 = gj[:, 0:128], gj[:, 128:256], gj[:, 256:384]
    for c, t in enumerate((t0, jnp.where(lane_d < 64, t1, t0), jnp.where(lane_d < 64, t2, t1), t2)):
        gh[0, :, :, :, place(c) * 128:(place(c) + 1) * 128] = spread(t)
    g1(3).start()
    cout = pltpu.make_async_copy(x.at[pl.ds(0, rows)], out_hbm, csem.at[0])
    cout.start()

    def finish_mlp(j):
        total = sum3(j)
        small[1, :, j * 128:(j + 1) * 128] = total[:, :128]
        small[2, :, j * 128:(j + 1) * 128] = total[:, 128:]

    def finish_projection():
        t = pltpu.roll(sum3(3), lax.rem(128 - lax.rem(96 * col_i, 128), 128), 1)
        small[3, :, 0:128] = t

    behind = (
        [(1, lambda: sum1(3)), (4, lambda: sum2(2)), (6, lambda: finish_mlp(0)), (7, lambda: sum2(3))],
        [(1, lambda: sum1(4)), (2, lambda: finish_mlp(1)), (4, lambda: finish_mlp(2)), (6, lambda: sum2(4))],
        [(1, lambda: sum1(5)), (2, lambda: finish_projection()), (6, lambda: sum2(5))],
    )
    for h in range(PAIRS):
        hl = pl.ds(h * 128, 128)

        def attend_back(i, _):
            off, base = window(i)
            qw = pl.ds(base, WIN)
            kk = pl.ds(base, KEYS)
            q = qkv[h, qw, 0:128]
            k = qkv[h, kk, 128:256]
            v = qkv[h, kk, 256:384]
            rid = lax.broadcasted_iota(jnp.int32, (WIN, 128), 0) - off
            mine = (rid >= 0) & (rid < SEQ)
            do = jnp.where(mine, ag[qw, hl].astype(F32) * rinv[qw, hl], 0.0)
            dob = do.astype(BF16)
            xx = jnp.concatenate([dob, (do * attn[qw, hl].astype(F32)).astype(BF16)], axis=1)
            ev = even[:WIN]
            zw = zero[:WIN]
            e0 = est[h, i, 0]
            e1 = est[h, i, 1]
            d0 = (e0 * nt(xx, jnp.concatenate([jnp.where(even, v, zero), -ones_e], axis=1))).astype(BF16)
            d1 = (e1 * nt(xx, jnp.concatenate([jnp.where(even, zero, v), -ones_o], axis=1))).astype(BF16)
            dq = (nn(d0, jnp.where(even, k, zero)) + nn(d1, jnp.where(even, zero, k))) * 0.125
            dk = (tn(d0, jnp.where(ev, q, zw)) + tn(d1, jnp.where(ev, zw, q))) * 0.125
            dv = tn(e0, jnp.where(ev, dob, zw)) + tn(e1, jnp.where(ev, zw, dob))
            old = pgr[h, qw, :].astype(F32)
            pgr[h, qw, 0:128] = jnp.where(mine, dq, old[:, 0:128]).astype(BF16)
            pgr[h, qw, 128:256] = jnp.where(mine, dk[:WIN], old[:, 128:256]).astype(BF16)
            pgr[h, qw, 256:384] = jnp.where(mine, dv[:WIN], old[:, 256:384]).astype(BF16)
            hook(i, behind[h])
            return 0

        loop(0, images, attend_back, 0)
        gp = tn(rows1[...], pgr[h, 0:RP, :])
        for c, j in enumerate(SHARES[h]):
            gh[1 + h, :, :, :, place(c) * 128:(place(c) + 1) * 128] = spread(gp[:, j * 128:(j + 1) * 128])
        g1(4 + h).start()

        def bias_sum(i, carry):
            s = rows_of(i, SMALL)
            return carry + jnp.sum(pgr[h, s, :].astype(F32), axis=0, keepdims=True)

        vec[6 + h:7 + h, :] = loop(0, nsm, bias_sum, zr1)

    def ln1b(i, carry):
        s = rows_of(i, SMALL)
        g = nt(pgr[0, s, :], wp[0]) + nt(pgr[1, s, :], wp[1]) + nt(pgr[2, s, :], wp[2])
        gbuf[s, :] = g
        terms = (g * n1[s, :], g)
        hook(i, [(nsm // 2, lambda: sum1(6))])
        return tuple(a + jnp.sum(t, axis=0, keepdims=True) for a, t in zip(carry, terms))

    sums = loop(0, nsm, ln1b, (zr1,) * 2)

    for r, t in zip((2, 3), sums):
        vec[r:r + 1, :] = t
    def v1():
        return remote(vec, vr1, vs.at[0], vs.at[1], sibling)

    def v2(d):
        return remote(vsum1, vr2.at[plane], vs.at[0], vs.at[2], ppeer(d))

    def v3(d):
        return remote(vr3.at[z], vr3.at[z], vs.at[0], vs.at[3], zpeer(d))

    def vector1():
        v1().wait_recv()
        vsum1[...] = vec[...] + vr1[...]
        for d in range(1, PLANE):
            v2(d).start()
        vr2[plane] = vsum1[...]

    def vector2():
        arrived(vs.at[2], vspan(PLANE - 1))
        total = vr2[0]
        for q in range(1, PLANE):
            total += vr2[q]
        vr3[z] = total
        for d in range(1, Z):
            v3(d).start()

    v1().start()

    def ln1c(i, _):
        s = rows_of(i, SMALL)
        normed = n1[s, :]
        inv = inv1[s, 0:1]
        scaled = gbuf[s, :] * fs
        rg[s, :] = rg[s, :] + inv * (scaled - mean(scaled) - normed * mean(scaled * normed))
        hook(i, [(nsm // 2 - 1, vector1), (nsm - 2, lambda: sum2(6)), (nsm - 1, vector2)])
        return 0

    loop(0, nsm, ln1c, 0)
    cg = pltpu.make_async_copy(rg.at[pl.ds(0, rows)], grad_hbm, csem.at[1])
    cg.start()
    for h in range(PAIRS):
        frame[:, turn(h)] = sum3(4 + h)
    back = lax.rem(D - 32 * col_i, D)
    small[0] = pltpu.roll(frame[...], back, 1)
    with jax.named_scope("vec3"):
        arrived(vs.at[3], vspan(Z - 1))
    total = vr3[0]
    for q in range(1, Z):
        total += vr3[q]
    vall[...] = total
    turned = pltpu.roll(total[0:8, :], lax.rem(D - 96 * col_i, D), 1)
    small[3, 0:8, 128:256] = turned[:, :128]
    for h, j in enumerate((jnp.minimum(col_i, 2), (col_i + 1) // 2, jnp.maximum(col_i - 1, 0))):
        frame[0:1, turn(h)] = vall[6 + h:7 + h, lanes_of(j, 128)]
    small[4, 0:8, :] = pltpu.roll(frame[0:8, :], back, 1)
    small[4, 8:9, :] = vall[pl.ds(9 + pos, 1), :]
    csmall = pltpu.make_async_copy(small, small_hbm, csem.at[2])
    csmall.start()

    with jax.named_scope("ends"):
        for k in range(len(chunks)):
            left(asend.at[k], span(ALL))
        left(bs.at[0], n1.at[0:8 * (2 * Y - 1)])
        for k in range(7):
            left(gsend.at[k], span(ALL * (width(k) // 128)))
        left(vs.at[0], vspan(PLANE + Z - 1))
        cout.wait()
        cg.wait()
        csmall.wait()


PIECES = 4


def finish_kernel(rows, *refs):
    rows_in, grad_in, small_in = refs[:3]
    outs, stage, (bx, bg, small, sem, osem, ssem) = refs[3:17], refs[17:29], refs[29:]
    step = -(-rows // (8 * PIECES)) * 8
    first = pltpu.make_async_copy(small_in, small, ssem.at[0])
    first.start()
    moves = []
    for c in range(PIECES):
        part = pl.ds(c * step, min(step, rows - c * step))
        for k, (src, buf, dst) in enumerate(((grad_in, bg, outs[1]), (rows_in, bx, outs[0]))):
            moves.append((
                pltpu.make_async_copy(src.at[part], buf.at[part], sem.at[0, k, c]),
                pltpu.make_async_copy(buf.at[part], dst.at[part], sem.at[1, k, c]),
            ))
    for take, _ in moves:
        take.start()
    first.wait()
    rv, wide = stage[0].shape
    stage[0][...] = small[0, :rv, :wide]
    stage[1][...] = small[3, :rv, :stage[1].shape[1]]
    stage[2][...] = small[1, :rv, :]
    stage[3][...] = small[2, :rv, :]
    stage[4][...] = small[4, 0:1, :wide].reshape(wide)
    stage[6][...] = small[4, 8:9, :].reshape(D)
    for r, k in enumerate((5, 7, 8, 9, 10, 11)):
        n = stage[k].shape[0]
        stage[k][...] = small[3, r:r + 1, 128:128 + n].reshape(n)
    gives = [pltpu.make_async_copy(stage[k], outs[2 + k], osem.at[k]) for k in range(12)]
    for give in gives:
        give.start()
    for take, give in moves:
        take.wait()
        give.start()
    for _, give in moves:
        give.wait()
    for give in gives:
        give.wait()


def body(dps, cols, tokens, packed, packed_bias, projection, projection_bias, expansion, expansion_bias, reduction,
         reduction_bias, first_scale, first_shift, second_scale, second_shift, upstream):
    args = (tokens, packed, packed_bias, projection.T, projection_bias, expansion, expansion_bias, reduction.T,
            reduction_bias, first_scale, first_shift, second_scale, second_shift, upstream)
    rows = tokens.shape[0]
    images = rows // SEQ
    Z = min(4, dps)
    PD = dps // Z
    Y = cols // 2
    RV = packed.shape[0]
    RB = -(-RV // 16) * 16
    PLANE = PD * Y
    RP = -(-rows // BIG) * BIG
    XP = RP + 80
    cfg = (Z, PD, Y, RB, RV, rows)
    V = pl.BlockSpec(memory_space=pltpu.VMEM)
    A = pl.BlockSpec(memory_space=pl.ANY)
    S = jax.ShapeDtypeStruct
    vm = pltpu.VMEM
    dma = pltpu.SemaphoreType.DMA
    NH = FF // HC
    NC = PAIRS + 1 + 2 * NH
    small = RV != RB
    outs = (
        S((rows, D), BF16), S((rows, D), F32),
        S(packed.shape, F32), S(projection.shape[::-1], F32), S(expansion.shape, F32), S(reduction.shape[::-1], F32),
        S(packed_bias.shape, F32), S((D // cols,), F32), S(expansion_bias.shape, F32),
    ) + (S((D // cols,), F32),) * 5
    narrow = (args[1], args[2], args[3], args[4], args[5], args[6], args[7]) + args[8:13]
    scratch = [vm(a.shape, a.dtype) for a in narrow] + [
        vm((5, RB, D), F32),
        vm((RP, D), BF16), vm((RP, D), BF16),
        vm((RP, D), F32), vm((RP, D), BF16),
        vm((PAIRS, XP, D), BF16), vm((XP, D), BF16),
        vm((PAIRS, images, 2, WIN, KEYS), BF16), vm((XP, D), F32),
        vm((RP, D), F32), vm((RP, D), BF16),
        vm((RP, D), F32), vm((RP, D), F32),
        vm((RP, HC), BF16), vm((RP, HC), BF16),
        vm((RP, D), BF16), vm((XP, D), BF16),
        vm((PAIRS, XP, D), BF16), vm((max(RP, (Z - 1 + (2 * PLANE - 1) * Z) * RB), 128), F32), vm((RP, 128), F32),
        vm((PAIRS, Z, PD, RB, 4 * 128), BF16), vm((Z, PD, RB, 4 * 128), BF16),
        vm((NH, Z, PD, RB, HC), BF16), vm((NH, Z, PD, RB, HC), BF16),
        vm((PAIRS, D, D), BF16), vm((D, D), BF16),
        vm((D, HC) if small else (16, 128), BF16), vm((D, HC) if small else (16, 128), BF16),
        vm((4, 8, D), F32),
        vm((NH, Z, PD, RB, 4 * 256), BF16), vm((4, Z, PD, RB, 4 * 128), BF16),
        vm((NH, Z, PD, RB, Y * 256), BF16), vm((NH, PLANE - 1, Z, RB, 256), BF16), vm((NH, Z, RB, 256), BF16),
        vm((4, Z, PD, RB, Y * 128), BF16), vm((4, PLANE - 1, Z, RB, 128), BF16), vm((4, Z, RB, 128), BF16),
        vm((NH, Z, PD, RB, Y * 256), BF16), vm((NH, Z, RB, 256), BF16),
        vm((4, Z, PD, RB, Y * 128), BF16), vm((4, Z, RB, 128), BF16),
        vm((RB, D), F32), vm((16, D), F32), vm((16, D), F32),
        vm((16, D), F32), vm((PLANE, 16, D), F32), vm((Z, 16, D), F32), vm((16, D), F32), vm((RP, D), F32),
        dma((12,)), dma((3,)), dma((NC,)), dma((Z,)), dma((NC,)), dma((NC,)), dma((NC,)),
        dma((2,)), dma((7,)), dma((7,)), dma((7,)), dma((7,)), dma((4,)),
    ]
    got = pl.pallas_call(
        functools.partial(layer_kernel, cfg),
        out_shape=(outs[0], outs[1], S((5, RB, D), F32)),
        in_specs=[A] * 14,
        out_specs=(A,) * 3,
        scratch_shapes=scratch,
        compiler_params=pltpu.CompilerParams(vmem_limit_bytes=67043328, collective_id=0, has_side_effects=True),
    )(*args)
    got = pl.pallas_call(
        functools.partial(finish_kernel, rows),
        out_shape=outs,
        in_specs=[A] * 3,
        out_specs=(A,) * 14,
        scratch_shapes=[vm(o.shape, o.dtype) for o in outs[2:]] + [
            vm((rows, D), BF16), vm((rows, D), F32), vm((5, RB, D), F32), dma((2, 2, PIECES)), dma((12,)), dma((1,))],
    )(*got)
    return got[:3] + (got[3].T, got[4], got[5].T) + tuple(got[6:])


def solution(mesh):
    placed = (
        P(("dp", "col"), None), P("dp", "col"), P("col"), P("col", "dp"), P(), P("dp", "col"), P("col"),
        P("col", "dp"), P(), P(), P(), P(), P(), P(("dp", "col"), None),
    )
    return jax.shard_map(
        functools.partial(body, mesh.shape["dp"], mesh.shape["col"]),
        mesh=mesh,
        in_specs=placed,
        out_specs=(
            P(("dp", "col"), None), P(("dp", "col"), None),
            P("dp", "col"), P("col", "dp"), P("dp", "col"), P("col", "dp"),
        ) + (P("col"),) * 8,
        check_vma=False,
    )
```

```python
import functools

import jax
import jax.numpy as jnp
from jax import lax
from jax.experimental import pallas as pl
from jax.experimental.pallas import tpu as pltpu
from jax.sharding import PartitionSpec as P

SEQ = 197
EPS = 1e-06
ROOT_HALF = 0.7071067811865476
INV_ROOT_TAU = 0.3989422804014327
F32, BF16 = jnp.float32, jnp.bfloat16
MESH = pl.DeviceIdType.MESH
D = 384
FF = 1536
PAIRS = 3
WIN = 224
KEYS = 256
BIG = 528
SMALL = 176
HC = 512
LIMIT = 60 * 1024 * 1024


def nn(a, b):
    return lax.dot_general(a, b, (((1,), (0,)), ((), ())), preferred_element_type=F32)


def nt(a, b):
    return lax.dot_general(a, b, (((1,), (1,)), ((), ())), preferred_element_type=F32)


def tn(a, b):
    return lax.dot_general(a, b, (((0,), (0,)), ((), ())), preferred_element_type=F32)


def rows_of(i, size):
    if isinstance(i, int):
        return pl.ds(i * size, size)
    return pl.ds(pl.multiple_of(i * size, 16), size)


def lanes_of(i, size):
    return pl.ds(pl.multiple_of(i * size, 128), size)


def mean(x):
    return jnp.sum(x, axis=1, keepdims=True) * (1.0 / x.shape[1])


def hook(i, steps):
    for at, step in steps:
        if isinstance(i, int):
            if i == at:
                step()
        else:
            pl.when(i == at)(lambda step=step: (step(), None)[1])


def unrolled(lo, hi, function, init):
    with jax.named_scope(function.__name__):
        for i in range(lo, hi):
            init = function(i, init)
    return init


def loop(lo, hi, function, init):
    with jax.named_scope(function.__name__):
        return lax.fori_loop(lo, hi, function, init)


def named(function):
    def inner(*a):
        with jax.named_scope(function.__name__ + "_".join(str(v) for v in a if isinstance(v, int))):
            return function(*a)
    return inner


TILES = (
    ((0, 0, 128), (1, 1, 128), (2, 3, 96)),
    ((0, 0, 128), (1, 2, 64), (3, 3, 128)),
    ((0, 1, 32), (2, 2, 128), (3, 3, 128)),
)
SHARES = ((0, 1, 2, 2), (0, 1, 1, 2), (0, 0, 1, 2))


def layer_kernel(cfg, *refs):
    Z, PD, Y, RB, RV, rows = cfg
    PLANE = PD * Y
    RP = -(-rows // BIG) * BIG
    images = rows // SEQ
    nsm, nbig = RP // SMALL, RP // BIG
    tokens, upstream, outside = refs[0], refs[13], refs[1:13]
    o_out, o_grad, small, refs = refs[14], refs[15], refs[16], refs[17:]
    (packed, packed_bias, projection, projection_bias, expansion, expansion_bias, reduction,
     reduction_bias, first_scale, first_shift, second_scale, second_shift,
     x, up, n1, rows1, qkv, attn, est, rinv, n2, rows2, acc1, rg, act, hg, pgr, inv1, inv2,
     wpk, ptr, exr, rtr, wp, pt, exc, rtc, bias,
     gm, gh, rm1, rm2, rm3, rh1, rh2, rh3, sm1, sm2, sh1, sh2, frame, vec, vsum1, vr1, vr2, vr3, vall,
     isem, csem, asend, zfirst, zr, pr, kr, bs, gsend, g1r, g2r, g3r, vs) = refs

    dp_i, col_i = lax.axis_index("dp"), lax.axis_index("col")
    z, pd = dp_i // PD, lax.rem(dp_i, PD)
    y, core = col_i // 2, lax.rem(col_i, 2)
    pos = core * Y + y
    plane = pd * Y + y

    def device(zz, pp, yy, cc):
        return (zz * PD + pp, yy * 2 + cc)

    def znear(s):
        rising = jnp.where(s < z, s, s + 1)
        down = Z - 1 - s
        falling = jnp.where(down > z, down, down - 1)
        return jnp.where(2 * z < Z, rising, falling)

    def zpeer(s):
        return device(znear(s - 1), pd, y, core)

    def pplace(d):
        q = lax.rem(plane + d, PLANE)
        return q // Y, lax.rem(q, Y)

    def ppeer(d):
        pp, yy = pplace(d)
        return device(z, pp, yy, core)

    sibling = device(z, pd, y, 1 - core)

    def cpeer(d):
        return (dp_i, lax.rem(col_i + d, 2 * Y))

    def remote(src, dst, send, recv, to):
        return pltpu.make_async_remote_copy(
            src_ref=src, dst_ref=dst, send_sem=send, recv_sem=recv, device_id=to, device_id_type=MESH)

    barrier = pltpu.get_barrier_semaphore()
    near = [zpeer(d) for d in range(1, Z)] + [ppeer(d) for d in range(1, PLANE)]
    near += [cpeer(d) for d in range(1, 2 * Y) if d != Y]
    for to in near + ([sibling] if Y == 1 else []):
        pl.semaphore_signal(barrier, inc=1, device_id=to, device_id_type=MESH)
    greeted = len(near)

    cin = pltpu.make_async_copy(tokens, x.at[pl.ds(0, rows)], csem.at[0])
    cup = pltpu.make_async_copy(upstream, up.at[pl.ds(0, rows)], csem.at[1])
    inside = (packed, packed_bias, projection, projection_bias, expansion, expansion_bias, reduction,
              reduction_bias, first_scale, first_shift, second_scale, second_shift)
    loads = [pltpu.make_async_copy(a, b, isem.at[n]) for n, (a, b) in enumerate(zip(outside, inside))]
    for n in (0, 2, 4, 6, 1, 5, 3, 7, 8, 9, 10, 11):
        loads[n].start()
    cin.start()
    cup.start()
    for load in loads:
        load.wait()

    def padded(v):
        return v if RV == RB else jnp.concatenate([v, jnp.zeros((RB - RV, v.shape[1]), v.dtype)], axis=0)

    own = padded(packed[...].astype(F32))
    own = jnp.concatenate([own, jnp.zeros((RB, D - own.shape[1]), F32)], axis=1)
    frame[...] = pltpu.roll(own, 32 * col_i, 1)

    def turn(h):
        return lanes_of(lax.rem(h + col_i, 3), 128)

    for h in range(PAIRS):
        wpk[h, z, pd, :, lanes_of(pos, 128)] = frame[:, turn(h)].astype(BF16)
    own = padded(projection[...].astype(F32))
    own = jnp.concatenate([own, jnp.zeros((RB, 128 - own.shape[1]), F32)], axis=1)
    ptr[z, pd, :, lanes_of(pos, 128)] = pltpu.roll(own, lax.rem(96 * col_i, 128), 1).astype(BF16)
    for j in range(FF // HC):
        exr[j, z, pd, :, lanes_of(pos, 128)] = padded(expansion[:, j * 128:(j + 1) * 128])
        rtr[j, z, pd, :, lanes_of(pos, 128)] = padded(reduction[:, j * 128:(j + 1) * 128])
    vrow = jnp.concatenate([packed_bias[...].reshape(1, -1), jnp.zeros((1, D - packed_bias.shape[0]), F32)], axis=1)
    vrow = pltpu.roll(jnp.broadcast_to(vrow, (8, D)), 32 * col_i, 1)
    bias[pos] = jnp.concatenate([vrow[:4], jnp.broadcast_to(expansion_bias[...].reshape(1, -1), (4, D))], axis=0)

    chunks = [wpk.at[h] for h in range(PAIRS)] + [ptr]
    for j in range(FF // HC):
        chunks += [exr.at[j], rtr.at[j]]
    mine_l = lanes_of(pos, 128)

    def span(slots):
        return inv1.at[0:slots * RB // 2]

    def vspan(count):
        return n1.at[0:count * 16]

    def arrived(sem, ref):
        remote(ref, ref, vs.at[0], sem, sibling).wait_recv()

    def left(sem, ref):
        remote(ref, ref, sem, vs.at[0], sibling).wait_send()

    def zcopy(k, d):
        slot = chunks[k].at[z, pd, :, mine_l]
        return remote(slot, slot, asend.at[k], zfirst.at[z] if k == 0 else zr.at[k], zpeer(d))

    def pcopy(k, d):
        slot = chunks[k].at[:, pd, :, mine_l]
        return remote(slot, slot, asend.at[k], pr.at[k], ppeer(d))

    def qcopy(d, q):
        slot = chunks[0].at[q, pd, :, mine_l]
        return remote(slot, slot, asend.at[0], pr.at[0], ppeer(d))

    def kcopy(k):
        slot = chunks[k].at[:, :, :, lanes_of(core, Y * 128)]
        return remote(slot, slot, asend.at[k], kr.at[k], sibling)

    def bcopy(d):
        return remote(bias.at[pos], bias.at[pos], bs.at[0], bs.at[1], cpeer(d))

    @named
    def to_plane(k):
        arrived(zr.at[k], span(Z - 1))
        for d in range(1, PLANE):
            pcopy(k, d).start()

    @named
    def to_sibling(k):
        arrived(pr.at[k], span((PLANE - 1) * Z))
        kcopy(k).start()

    ALL = Z - 1 + (PLANE - 1) * Z + PLANE * Z

    with jax.named_scope("barrier"):
        pl.semaphore_wait(barrier, greeted)
    def to_z(k):
        for d in range(1, Z):
            zcopy(k, d).start()

    to_z(0)
    for d in range(1, PLANE):
        qcopy(d, z).start()
    for d in range(1, 2 * Y):
        bcopy(d).start()

    x[rows:, :] = jnp.zeros((RP - rows, D), BF16)
    up[rows:, :] = jnp.zeros((RP - rows, D), BF16)
    for h in range(PAIRS):
        qkv[h, RP:, :] = jnp.zeros((qkv.shape[1] - RP, D), BF16)
    tail = attn.shape[0] - RP + 16
    attn[RP - 16:, :] = jnp.zeros((tail, D), BF16)
    act[RP:, :] = jnp.zeros((act.shape[0] - RP, HC), BF16)
    rinv[RP - 16:, :] = jnp.zeros((tail, D), F32)
    pgr[:, RP - 16:, :] = jnp.zeros((PAIRS, tail, D), BF16)
    fs = first_scale[...].reshape(1, D)
    fh = first_shift[...].reshape(1, D)
    ss = second_scale[...].reshape(1, D)
    sh = second_shift[...].reshape(1, D)
    prb = projection_bias[...].reshape(1, D)
    rdb = reduction_bias[...].reshape(1, D)
    cin.wait()
    cup.wait()

    def ln1(i, _):
        s = rows_of(i, SMALL)
        v = x[s, :].astype(F32)
        avg = mean(v)
        inv = lax.rsqrt(mean(v * v) - avg * avg + EPS)
        normed = (v - avg) * inv
        n1[s, :] = normed
        inv1[s, :] = jnp.broadcast_to(inv, (SMALL, 128))
        rows1[s, :] = (normed * fs + fh).astype(BF16)
        return 0

    @named
    def pass_on(d):
        q = znear(d - 1)
        arrived(zfirst.at[q], chunks[0].at[q, pd, :, mine_l])
        for e in range(1, PLANE):
            qcopy(e, q).start()

    loop(0, nsm, ln1, 0)
    to_z(1)
    for d in range(1, Z):
        pass_on(d)
    for k in range(2, len(chunks)):
        to_z(k)
    to_plane(1)
    with jax.named_scope("plane0"):
        arrived(pr.at[0], span((PLANE - 1) * Z))
    kcopy(0).start()
    arrived(bs.at[1], n1.at[0:8 * (2 * Y - 1)])

    lane = lax.broadcasted_iota(jnp.int32, (KEYS, 128), 1)
    even = lane < 64
    zero = jnp.zeros((KEYS, 128), BF16)
    one = jnp.ones((KEYS, 128), BF16)
    ones_e = jnp.where(even, one, zero)
    ones_o = jnp.where(even, zero, one)

    def place(c):
        return (c % 2) * Y + c // 2

    if RV != RB:
        wide = Z * PD * RB
        r_ = lax.broadcasted_iota(jnp.int32, (D, wide), 0)
        c_ = lax.broadcasted_iota(jnp.int32, (D, wide), 1)
        pick = jnp.where(c_ == (r_ // RV) * RB + lax.rem(r_, RV), 1.0, 0.0).astype(BF16)

    def compact(v):
        v = v.reshape(Z * PD * RB, v.shape[-1])
        return v if RV == RB else nn(pick, v).astype(BF16)

    def spread(v):
        v = v.astype(BF16)
        v = v if RV == RB else tn(pick, v).astype(BF16)
        return v.reshape(Z, PD, RB, v.shape[-1])

    def merged(tile, first, second, upto):
        if first == second:
            return tile(first)
        a, b = tile(first), tile(second)
        return jnp.where(lax.broadcasted_iota(jnp.int32, a.shape, 1) < upto, a, b)

    @named
    def assemble(h):
        kcopy(h).wait_recv()
        for j, (first, second, upto) in enumerate(TILES[h]):
            wp[h, :, j * 128:(j + 1) * 128] = merged(
                lambda c: compact(wpk[h, :, :, :, place(c) * 128:(place(c) + 1) * 128]), first, second, upto)

    def bias_of(h):
        def tile(c):
            t = (h + c) % 3
            return bias[place(c), 0:1, t * 128:(t + 1) * 128]
        return jnp.concatenate([merged(tile, *t) for t in TILES[h]], axis=1)

    def keep(ref, i, value):
        last = min(rows, (i + 1) * SMALL)
        ref[i * SMALL:last, :] = value[:last - i * SMALL]

    def window(i):
        first = i * SEQ
        base = (first // 16) * 16
        return first - base, base if isinstance(i, int) else pl.multiple_of(base, 16)

    before = ((to_sibling, 1), (to_plane, 2)), ((to_sibling, 2),), ((to_sibling, 3),)
    after = (tuple((to_plane, k) for k in (3, 4, 5, 6)), tuple((to_plane, k) for k in (7, 8, 9)), ((to_sibling, 4), (to_sibling, 5)))

    def do(steps):
        for step, k in steps:
            step(k)

    for h in range(PAIRS):
        hl = pl.ds(h * 128, 128)
        assemble(h)
        pb = bias_of(h)

        def project(i, _):
            s = rows_of(i, BIG)
            qkv[h, s, :] = (nn(rows1[s, :], wp[h]) + pb).astype(BF16)
            return 0

        loop(0, nbig, project, 0)

        def attend(i, _):
            off, base = window(i)
            qw = pl.ds(base, WIN)
            kk = pl.ds(base, KEYS)
            q = qkv[h, qw, 0:128]
            k = qkv[h, kk, 128:256]
            v = qkv[h, kk, 256:384]
            col = lax.broadcasted_iota(jnp.int32, (WIN, KEYS), 1) - off
            ok = (col >= 0) & (col < SEQ)
            es = []
            for m in (even, ~even):
                s = nt(q, jnp.where(m, k, zero))
                s = jnp.where(ok, s, -1e30)
                top = jnp.max(s, axis=1, keepdims=True)
                es.append(jnp.exp((s - top) * 0.125).astype(BF16))
            est[h, i, 0] = es[0]
            est[h, i, 1] = es[1]
            mix = nn(es[0], jnp.concatenate([jnp.where(even, v, zero), ones_e], axis=1)) + nn(
                es[1], jnp.concatenate([jnp.where(even, zero, v), ones_o], axis=1))
            r = 1.0 / mix[:, 128:]
            o = mix[:, :128] * r
            rid = lax.broadcasted_iota(jnp.int32, (WIN, 128), 0) - off
            mine = (rid >= 0) & (rid < SEQ)
            attn[qw, hl] = jnp.where(mine, o, attn[qw, hl].astype(F32)).astype(BF16)
            rinv[qw, hl] = jnp.where(mine, r, rinv[qw, hl])
            return 0

        do(before[h])
        unrolled(0, images, attend, 0)
        do(after[h])

    kcopy(3).wait_recv()
    lane_d = lax.broadcasted_iota(jnp.int32, (D, 128), 1)
    tiles = [compact(ptr[:, :, :, place(c) * 128:(place(c) + 1) * 128]) for c in range(4)]
    pt[:, 0:128] = jnp.where(lane_d < 96, tiles[0], tiles[1])
    pt[:, 128:256] = jnp.where(lane_d < 64, tiles[1], tiles[2])
    pt[:, 256:384] = jnp.where(lane_d < 32, tiles[2], tiles[3])
    def exb_of(j):
        return jnp.concatenate([bias[p, 4:5, j * 128:(j + 1) * 128] for p in range(4)], axis=1)

    acc2 = rg

    def ln2(i, _):
        s = rows_of(i, SMALL)
        v = x[s, :].astype(F32) + nt(attn[s, :], pt[...]) + prb
        avg = mean(v)
        inv = lax.rsqrt(mean(v * v) - avg * avg + EPS)
        normed = (v - avg) * inv
        acc1[s, :] = v + rdb
        n2[s, :] = normed
        inv2[s, :] = jnp.broadcast_to(inv, (SMALL, 128))
        rows2[s, :] = (normed * ss + sh).astype(BF16)
        return 0

    unrolled(0, nsm, ln2, 0)

    def part(big, small, k):
        return big.at[k] if k < PAIRS else small.at[k - PAIRS]

    def width(k):
        return 256 if k < PAIRS else 128

    def g1(k):
        half = Y * width(k)
        return remote(part(gm, gh, k).at[:, :, :, lanes_of(1 - core, half)], part(rm1, rh1, k),
                      gsend.at[k], g1r.at[k], sibling)

    def g2(k, d):
        pp, yy = pplace(d)
        return remote(part(sm1, sh1, k).at[:, pp, :, lanes_of(yy, width(k))], part(rm2, rh2, k).at[d - 1],
                      gsend.at[k], g2r.at[k], ppeer(d))

    def g3(k, d):
        return remote(part(sm2, sh2, k).at[znear(d - 1)], part(rm3, rh3, k).at[z], gsend.at[k], g3r.at[k], zpeer(d))

    @named
    def sum1(k):
        g1(k).wait_recv()
        own = part(gm, gh, k)[:, :, :, lanes_of(core, Y * width(k))]
        part(sm1, sh1, k)[...] = (own.astype(F32) + part(rm1, rh1, k)[...].astype(F32)).astype(BF16)
        for d in range(1, PLANE):
            g2(k, d).start()

    @named
    def sum2(k):
        arrived(g2r.at[k], span((PLANE - 1) * Z * (width(k) // 128)))
        total = part(sm1, sh1, k)[:, pd, :, lanes_of(y, width(k))].astype(F32)
        for d in range(1, PLANE):
            total += part(rm2, rh2, k)[d - 1].astype(F32)
        part(sm2, sh2, k)[...] = total.astype(BF16)
        for d in range(1, Z):
            g3(k, d).start()

    @named
    def sum3(k):
        arrived(g3r.at[k], span((Z - 1) * (width(k) // 128)))
        total = part(sm2, sh2, k)[z].astype(F32)
        for d in range(1, Z):
            total += part(rm3, rh3, k)[znear(d - 1)].astype(F32)
        return total

    vec[...] = jnp.zeros(vec.shape, F32)
    spot = (
        ((to_sibling, 6), (to_sibling, 7)),
        ((to_sibling, 8), (to_sibling, 9), (sum1, 0)),
        ((sum1, 1),),
    )
    for j in range(FF // HC):
        for k in (4 + 2 * j, 5 + 2 * j):
            kcopy(k).wait_recv()
        if RV != RB:
            exc[...] = compact(exr[j])
            rtc[...] = compact(rtr[j])

        def ex_of():
            return exc[...] if RV != RB else exr[j].reshape(D, HC)

        def rt_of():
            return rtc[...] if RV != RB else rtr[j].reshape(D, HC)

        exb = exb_of(j)

        def mlp(i, bsum):
            s = rows_of(i, BIG)
            pre = nn(rows2[s, :], ex_of()) + exb
            ug = nn(up[s, :], rt_of())
            cdf = 0.5 + 0.5 * lax.erf(pre * ROOT_HALF)
            act[s, :] = (pre * cdf).astype(BF16)
            g = ug * (cdf + pre * (jnp.exp(pre * pre * -0.5) * INV_ROOT_TAU))
            hg[s, :] = g.astype(BF16)
            acc1[s, :] += nt(act[s, :], rt_of())
            back = nt(hg[s, :], ex_of())
            acc2[s, :] = back if j == 0 else acc2[s, :] + back
            return bsum + jnp.sum(g, axis=0, keepdims=True)

        bsum = loop(0, nbig, mlp, jnp.zeros((1, HC), F32))
        do(spot[j])
        for p in range(4):
            vec[9 + p:10 + p, j * 128:(j + 1) * 128] = bsum[:, p * 128:(p + 1) * 128]
        for base, g in ((0, tn(rows2[...], hg[...])), (128, tn(up[...], act[0:RP, :]))):
            for p in range(4):
                gm[j, :, :, :, p * 256 + base:p * 256 + base + 128] = spread(g[:, p * 128:(p + 1) * 128])
        g1(j).start()

    def ln2b(i, carry):
        s = rows_of(i, SMALL)
        u = up[s, :].astype(F32)
        keep(o_out, i, acc1[s, :].astype(BF16))
        g = acc2[s, :]
        normed = n2[s, :]
        inv = inv2[s, 0:1]
        scaled = g * ss
        d = u + inv * (scaled - mean(scaled) - normed * mean(scaled * normed))
        rg[s, :] = d
        hg[s, 0:D] = d.astype(BF16)
        act[s, 0:D] = nn(d.astype(BF16), pt[...]).astype(BF16)
        terms = (d, u, g * normed, g)
        return tuple(a + jnp.sum(t, axis=0, keepdims=True) for a, t in zip(carry, terms))

    zr1 = jnp.zeros((1, D), F32)
    sums = unrolled(0, nsm, ln2b, (zr1,) * 4)
    for r, t in zip((0, 1, 4, 5), sums):
        vec[r:r + 1, :] = t
    sum1(2)
    sum2(0)
    gj = tn(hg[:, 0:D], attn[0:RP, :]).astype(BF16)
    t0, t1, t2 = gj[:, 0:128], gj[:, 128:256], gj[:, 256:384]
    for c, t in enumerate((t0, jnp.where(lane_d < 64, t1, t0), jnp.where(lane_d < 64, t2, t1), t2)):
        gh[0, :, :, :, place(c) * 128:(place(c) + 1) * 128] = spread(t)
    g1(3).start()

    def finish_mlp(j):
        total = sum3(j)
        small[1, :, j * 128:(j + 1) * 128] = total[:, :128]
        small[2, :, j * 128:(j + 1) * 128] = total[:, 128:]

    def finish_projection(_):
        t = pltpu.roll(sum3(3), lax.rem(128 - lax.rem(96 * col_i, 128), 128), 1)
        small[3, :, 0:128] = t

    behind = (
        ((sum1, 3), (sum2, 1)),
        ((sum1, 4), (sum2, 2), (sum2, 3), (finish_mlp, 0)),
        ((sum1, 5), (sum2, 4), (finish_mlp, 1)),
    )
    for h in range(PAIRS):
        hl = pl.ds(h * 128, 128)

        def attend_back(i, _):
            off, base = window(i)
            qw = pl.ds(base, WIN)
            kk = pl.ds(base, KEYS)
            q = qkv[h, qw, 0:128]
            k = qkv[h, kk, 128:256]
            v = qkv[h, kk, 256:384]
            rid = lax.broadcasted_iota(jnp.int32, (WIN, 128), 0) - off
            mine = (rid >= 0) & (rid < SEQ)
            do = jnp.where(mine, act[qw, hl].astype(F32) * rinv[qw, hl], 0.0)
            dob = do.astype(BF16)
            xx = jnp.concatenate([dob, (do * attn[qw, hl].astype(F32)).astype(BF16)], axis=1)
            ev = even[:WIN]
            zw = zero[:WIN]
            e0 = est[h, i, 0]
            e1 = est[h, i, 1]
            d0 = (e0 * nt(xx, jnp.concatenate([jnp.where(even, v, zero), -ones_e], axis=1))).astype(BF16)
            d1 = (e1 * nt(xx, jnp.concatenate([jnp.where(even, zero, v), -ones_o], axis=1))).astype(BF16)
            dq = (nn(d0, jnp.where(even, k, zero)) + nn(d1, jnp.where(even, zero, k))) * 0.125
            dk = (tn(d0, jnp.where(ev, q, zw)) + tn(d1, jnp.where(ev, zw, q))) * 0.125
            dv = tn(e0, jnp.where(ev, dob, zw)) + tn(e1, jnp.where(ev, zw, dob))
            old = pgr[h, qw, :].astype(F32)
            pgr[h, qw, 0:128] = jnp.where(mine, dq, old[:, 0:128]).astype(BF16)
            pgr[h, qw, 128:256] = jnp.where(mine, dk[:WIN], old[:, 128:256]).astype(BF16)
            pgr[h, qw, 256:384] = jnp.where(mine, dv[:WIN], old[:, 256:384]).astype(BF16)
            return 0

        unrolled(0, images, attend_back, 0)
        do(behind[h])
        gp = tn(rows1[...], pgr[h, 0:RP, :])
        for c, j in enumerate(SHARES[h]):
            gh[1 + h, :, :, :, place(c) * 128:(place(c) + 1) * 128] = spread(gp[:, j * 128:(j + 1) * 128])
        g1(4 + h).start()

        def bias_sum(i, carry):
            s = rows_of(i, SMALL)
            return carry + jnp.sum(pgr[h, s, :].astype(F32), axis=0, keepdims=True)

        vec[6 + h:7 + h, :] = unrolled(0, nsm, bias_sum, zr1)

    gbuf = acc1

    def ln1b(i, carry):
        s = rows_of(i, SMALL)
        g = nt(pgr[0, s, :], wp[0]) + nt(pgr[1, s, :], wp[1]) + nt(pgr[2, s, :], wp[2])
        gbuf[s, :] = g
        terms = (g * n1[s, :], g)
        hook(i, [(nsm // 2, lambda: sum1(6))])
        return tuple(a + jnp.sum(t, axis=0, keepdims=True) for a, t in zip(carry, terms))

    sums = unrolled(0, nsm, ln1b, (zr1,) * 2)

    for r, t in zip((2, 3), sums):
        vec[r:r + 1, :] = t
    def v1():
        return remote(vec, vr1, vs.at[0], vs.at[1], sibling)

    def v2(d):
        return remote(vsum1, vr2.at[plane], vs.at[0], vs.at[2], ppeer(d))

    def v3(d):
        return remote(vr3.at[z], vr3.at[z], vs.at[0], vs.at[3], zpeer(d))

    def vector1():
        v1().wait_recv()
        vsum1[...] = vec[...] + vr1[...]
        for d in range(1, PLANE):
            v2(d).start()
        vr2[plane] = vsum1[...]

    def vector2():
        arrived(vs.at[2], vspan(PLANE - 1))
        total = vr2[0]
        for q in range(1, PLANE):
            total += vr2[q]
        vr3[z] = total
        for d in range(1, Z):
            v3(d).start()

    v1().start()

    def ln1c(i, _):
        s = rows_of(i, SMALL)
        normed = n1[s, :]
        inv = inv1[s, 0:1]
        scaled = gbuf[s, :] * fs
        keep(o_grad, i, rg[s, :] + inv * (scaled - mean(scaled) - normed * mean(scaled * normed)))
        hook(i, [(nsm // 2, vector1)])
        return 0

    unrolled(0, nsm, ln1c, 0)
    do(((sum2, 5), (sum2, 6)))
    with jax.named_scope("vector2"):
        vector2()
    do(((finish_mlp, 2), (finish_projection, 3)))
    for h in range(PAIRS - 1):
        frame[:, turn(h)] = sum3(4 + h)
    frame[:, turn(PAIRS - 1)] = sum3(3 + PAIRS)
    back = lax.rem(D - 32 * col_i, D)
    small[0] = pltpu.roll(frame[...], back, 1)
    with jax.named_scope("vec3"):
        arrived(vs.at[3], vspan(Z - 1))
    total = vr3[0]
    for q in range(1, Z):
        total += vr3[q]
    vall[...] = total
    turned = pltpu.roll(total[0:8, :], lax.rem(D - 96 * col_i, D), 1)
    small[3, 0:8, 128:256] = turned[:, :128]
    for h, j in enumerate((jnp.minimum(col_i, 2), (col_i + 1) // 2, jnp.maximum(col_i - 1, 0))):
        frame[0:1, turn(h)] = vall[6 + h:7 + h, lanes_of(j, 128)]
    small[4, 0:8, :] = pltpu.roll(frame[0:8, :], back, 1)
    small[4, 8:9, :] = vall[pl.ds(9 + pos, 1), :]

    with jax.named_scope("ends"):
        for k in range(len(chunks)):
            left(asend.at[k], span(ALL))
        left(bs.at[0], n1.at[0:8 * (2 * Y - 1)])
        for k in range(7):
            left(gsend.at[k], span(ALL * (width(k) // 128)))
        left(vs.at[0], vspan(PLANE + Z - 1))


def finish_kernel(*refs):
    out, grad, small = refs[:3]
    outs, stage, sem = refs[3:17], refs[17:29], refs[29]
    moves = [pltpu.make_async_copy(a, b, sem.at[k]) for k, (a, b) in enumerate(zip((grad, out) + stage, (outs[1], outs[0]) + outs[2:]))]
    moves[0].start()
    moves[1].start()
    rv, wide = stage[0].shape
    stage[0][...] = small[0, :rv, :wide]
    stage[1][...] = small[3, :rv, :stage[1].shape[1]]
    stage[2][...] = small[1, :rv, :]
    stage[3][...] = small[2, :rv, :]
    stage[4][...] = small[4, 0:1, :wide].reshape(wide)
    stage[6][...] = small[4, 8:9, :].reshape(D)
    for r, k in enumerate((5, 7, 8, 9, 10, 11)):
        n = stage[k].shape[0]
        stage[k][...] = small[3, r:r + 1, 128:128 + n].reshape(n)
    for move in moves[2:]:
        move.start()
    for move in moves:
        move.wait()


def body(dps, cols, tokens, packed, packed_bias, projection, projection_bias, expansion, expansion_bias, reduction,
         reduction_bias, first_scale, first_shift, second_scale, second_shift, upstream):
    args = (tokens, packed, packed_bias, projection.T, projection_bias, expansion, expansion_bias, reduction.T,
            reduction_bias, first_scale, first_shift, second_scale, second_shift, upstream)
    rows = tokens.shape[0]
    images = rows // SEQ
    Z = min(4, dps)
    PD = dps // Z
    Y = cols // 2
    RV = packed.shape[0]
    RB = -(-RV // 16) * 16
    PLANE = PD * Y
    RP = -(-rows // BIG) * BIG
    XP = RP + 80
    cfg = (Z, PD, Y, RB, RV, rows)
    V = pl.BlockSpec(memory_space=pltpu.VMEM)
    A = pl.BlockSpec(memory_space=pl.ANY)
    S = jax.ShapeDtypeStruct
    vm = pltpu.VMEM
    dma = pltpu.SemaphoreType.DMA
    NH = FF // HC
    NC = PAIRS + 1 + 2 * NH
    small = RV != RB
    outs = (
        S((rows, D), BF16), S((rows, D), F32),
        S(packed.shape, F32), S(projection.shape[::-1], F32), S(expansion.shape, F32), S(reduction.shape[::-1], F32),
        S(packed_bias.shape, F32), S((D // cols,), F32), S(expansion_bias.shape, F32),
    ) + (S((D // cols,), F32),) * 5
    narrow = (args[1], args[2], args[3], args[4], args[5], args[6], args[7]) + args[8:13]
    scratch = [vm(a.shape, a.dtype) for a in narrow] + [
        vm((RP, D), BF16), vm((RP, D), BF16),
        vm((RP, D), F32), vm((RP, D), BF16),
        vm((PAIRS, XP, D), BF16), vm((XP, D), BF16),
        vm((PAIRS, images, 2, WIN, KEYS), BF16), vm((XP, D), F32),
        vm((RP, D), F32), vm((RP, D), BF16),
        vm((RP, D), F32), vm((RP, D), F32),
        vm((XP, HC), BF16), vm((RP, HC), BF16),
        vm((PAIRS, XP, D), BF16), vm((max(RP, (Z - 1 + (2 * PLANE - 1) * Z) * RB), 128), F32), vm((RP, 128), F32),
        vm((PAIRS, Z, PD, RB, 4 * 128), BF16), vm((Z, PD, RB, 4 * 128), BF16),
        vm((NH, Z, PD, RB, HC), BF16), vm((NH, Z, PD, RB, HC), BF16),
        vm((PAIRS, D, D), BF16), vm((D, D), BF16),
        vm((D, HC) if small else (16, 128), BF16), vm((D, HC) if small else (16, 128), BF16),
        vm((4, 8, D), F32),
        vm((NH, Z, PD, RB, 4 * 256), BF16), vm((4, Z, PD, RB, 4 * 128), BF16),
        vm((NH, Z, PD, RB, Y * 256), BF16), vm((NH, PLANE - 1, Z, RB, 256), BF16), vm((NH, Z, RB, 256), BF16),
        vm((4, Z, PD, RB, Y * 128), BF16), vm((4, PLANE - 1, Z, RB, 128), BF16), vm((4, Z, RB, 128), BF16),
        vm((NH, Z, PD, RB, Y * 256), BF16), vm((NH, Z, RB, 256), BF16),
        vm((4, Z, PD, RB, Y * 128), BF16), vm((4, Z, RB, 128), BF16),
        vm((RB, D), F32), vm((16, D), F32), vm((16, D), F32),
        vm((16, D), F32), vm((PLANE, 16, D), F32), vm((Z, 16, D), F32), vm((16, D), F32),
        dma((12,)), dma((2,)), dma((NC,)), dma((Z,)), dma((NC,)), dma((NC,)), dma((NC,)),
        dma((2,)), dma((7,)), dma((7,)), dma((7,)), dma((7,)), dma((4,)),
    ]
    got = pl.pallas_call(
        functools.partial(layer_kernel, cfg),
        out_shape=(vm((rows, D), BF16), vm((rows, D), F32), vm((5, RB, D), F32)),
        in_specs=[A] * 14,
        out_specs=(V,) * 3,
        scratch_shapes=scratch,
        compiler_params=pltpu.CompilerParams(vmem_limit_bytes=LIMIT, collective_id=0, has_side_effects=True),
    )(*args)
    got = pl.pallas_call(
        finish_kernel,
        out_shape=outs,
        in_specs=[V] * 3,
        out_specs=(A,) * 14,
        scratch_shapes=[vm(o.shape, o.dtype) for o in outs[2:]] + [dma((14,))],
        compiler_params=pltpu.CompilerParams(vmem_limit_bytes=2 * 1024 * 1024),
    )(*(pltpu.with_memory_space_constraint(v, pltpu.VMEM) for v in got))
    return got[:3] + (got[3].T, got[4], got[5].T) + tuple(got[6:])


def solution(mesh):
    placed = (
        P(("dp", "col"), None), P("dp", "col"), P("col"), P("col", "dp"), P(), P("dp", "col"), P("col"),
        P("col", "dp"), P(), P(), P(), P(), P(), P(("dp", "col"), None),
    )
    return jax.shard_map(
        functools.partial(body, mesh.shape["dp"], mesh.shape["col"]),
        mesh=mesh,
        in_specs=placed,
        out_specs=(
            P(("dp", "col"), None), P(("dp", "col"), None),
            P("dp", "col"), P("col", "dp"), P("dp", "col"), P("col", "dp"),
        ) + (P("col"),) * 8,
        check_vma=False,
    )
```

```python
import functools

import jax
import jax.numpy as jnp
from jax import lax
from jax.experimental import pallas as pl
from jax.experimental.pallas import tpu as pltpu
from jax.sharding import PartitionSpec as P

SEQ = 197
EPS = 1e-06
ROOT_HALF = 0.7071067811865476
INV_ROOT_TAU = 0.3989422804014327
F32, BF16 = jnp.float32, jnp.bfloat16
MESH = pl.DeviceIdType.MESH
D = 384
FF = 1536
PAIRS = 3
WIN = 224
KEYS = 256
BIG = 528
SMALL = 176
HC = 512
VMEM = 67_000_000


def nn(a, b):
    return lax.dot_general(a, b, (((1,), (0,)), ((), ())), preferred_element_type=F32)


def nt(a, b):
    return lax.dot_general(a, b, (((1,), (1,)), ((), ())), preferred_element_type=F32)


def tn(a, b):
    return lax.dot_general(a, b, (((0,), (0,)), ((), ())), preferred_element_type=F32)


def rows_of(i, size):
    if isinstance(i, int):
        return pl.ds(i * size, size)
    return pl.ds(pl.multiple_of(i * size, 16), size)


def lanes_of(i, size):
    return pl.ds(pl.multiple_of(i * size, 128), size)


def mean(x):
    return jnp.sum(x, axis=1, keepdims=True) * (1.0 / x.shape[1])


def hook(i, steps):
    for at, step in steps:
        if isinstance(i, int):
            if i == at:
                step()
        else:
            pl.when(i == at)(lambda step=step: (step(), None)[1])


def unrolled(lo, hi, function, init):
    with jax.named_scope(function.__name__):
        for i in range(lo, hi):
            init = function(i, init)
    return init


def loop(lo, hi, function, init):
    with jax.named_scope(function.__name__):
        return lax.fori_loop(lo, hi, function, init)


def named(function):
    def inner(*a):
        with jax.named_scope(function.__name__ + "_".join(str(v) for v in a if isinstance(v, int))):
            return function(*a)
    return inner


TILES = (
    ((0, 0, 128), (1, 1, 128), (2, 3, 96)),
    ((0, 0, 128), (1, 2, 64), (3, 3, 128)),
    ((0, 1, 32), (2, 2, 128), (3, 3, 128)),
)
SHARES = ((0, 1, 2, 2), (0, 1, 1, 2), (0, 0, 1, 2))


def layer_kernel(cfg, *refs):
    Z, PD, Y, RB, RV, rows = cfg
    PLANE = PD * Y
    RP = -(-rows // BIG) * BIG
    images = rows // SEQ
    nsm, nbig = RP // SMALL, RP // BIG
    tokens, upstream, outside = refs[0], refs[13], refs[1:13]
    o_out, o_grad, small, refs = refs[14], refs[15], refs[16], refs[17:]
    (packed, packed_bias, projection, projection_bias, expansion, expansion_bias, reduction,
     reduction_bias, first_scale, first_shift, second_scale, second_shift,
     x, up, n1, rows1, qkv, attn, est, rinv, n2, acc1, act, hg, pgr, inv1,
     wpk, ptr, exr, rtr, wp, pt, exc, rtc, bias,
     gm, gh, rm1, rm2, rm3, rh1, rh2, rh3, sm1, sm2, sh1, sh2, frame, vec, vq, vr2, vr3,
     asend, zfirst, pfirst, zr, pr, kr, bs, gsend, g1r, g2r, g3r, glast, vs) = refs

    dp_i, col_i = lax.axis_index("dp"), lax.axis_index("col")
    z, pd = dp_i // PD, lax.rem(dp_i, PD)
    y, core = col_i // 2, lax.rem(col_i, 2)
    pos = core * Y + y
    plane = pd * Y + y

    def device(zz, pp, yy, cc):
        return (zz * PD + pp, yy * 2 + cc)

    def znear(s):
        rising = jnp.where(s < z, s, s + 1)
        down = Z - 1 - s
        falling = jnp.where(down > z, down, down - 1)
        return jnp.where(2 * z < Z, rising, falling)

    def zpeer(s):
        return device(znear(s - 1), pd, y, core)

    def pplace(d):
        return lax.rem(pd + d // Y, PD), lax.rem(y + d % Y, Y)

    def psource(d):
        return lax.rem(pd + PD - d // Y, PD), lax.rem(y + Y - d % Y, Y)

    def ppeer(d):
        pp, yy = pplace(d)
        return device(z, pp, yy, core)

    def vpeer(d):
        pp, yy = pplace(d // 2)
        return device(z, pp, yy, lax.rem(core + d % 2, 2))

    sibling = device(z, pd, y, 1 - core)

    def cpeer(d):
        return (dp_i, lax.rem(col_i + d, 2 * Y))

    def remote(src, dst, send, recv, to):
        return pltpu.make_async_remote_copy(
            src_ref=src, dst_ref=dst, send_sem=send, recv_sem=recv, device_id=to, device_id_type=MESH)

    barrier = pltpu.get_barrier_semaphore()
    near = [zpeer(d) for d in range(1, Z)] + [vpeer(d) for d in range(1, 2 * PLANE)]
    for to in near:
        pl.semaphore_signal(barrier, inc=1, device_id=to, device_id_type=MESH)
    greeted = len(near)

    cin = pltpu.make_async_copy(tokens, x.at[pl.ds(0, rows)], gsend.at[5])
    cup = pltpu.make_async_copy(upstream, up.at[pl.ds(0, rows)], gsend.at[6])
    inside = (packed, packed_bias, projection, projection_bias, expansion, expansion_bias, reduction,
              reduction_bias, first_scale, first_shift, second_scale, second_shift)
    loads = [pltpu.make_async_copy(a, b, asend.at[n] if n < 8 else gsend.at[n - 8]) for n, (a, b) in enumerate(zip(outside, inside))]
    for n in (0, 2, 4, 6, 1, 5, 3, 7, 8, 9, 10, 11):
        loads[n].start()
    cin.start()
    cup.start()
    for load in loads:
        load.wait()

    def padded(v):
        return v if RV == RB else jnp.concatenate([v, jnp.zeros((RB - RV, v.shape[1]), v.dtype)], axis=0)

    own = padded(packed[...].astype(F32))
    own = jnp.concatenate([own, jnp.zeros((RB, D - own.shape[1]), F32)], axis=1)
    frame[...] = pltpu.roll(own, 32 * col_i, 1)

    def turn(h):
        return lanes_of(lax.rem(h + col_i, 3), 128)

    for h in range(PAIRS):
        wpk[h, z, pd, :, lanes_of(pos, 128)] = frame[:, turn(h)].astype(BF16)
    chunks = [wpk.at[h] for h in range(PAIRS)] + [ptr]
    for j in range(FF // HC):
        chunks += [exr.at[j], rtr.at[j]]
    mine_l = lanes_of(pos, 128)

    def span(slots):
        return inv1.at[0:slots * RB // 2]

    def vspan(count):
        return inv1.at[0:count * 16]

    def arrived(sem, ref):
        remote(ref, ref, vs.at[0], sem, sibling).wait_recv()

    def left(sem, ref):
        remote(ref, ref, sem, vs.at[0], sibling).wait_send()

    def zcopy(k, d):
        slot = chunks[k].at[z, pd, :, mine_l]
        return remote(slot, slot, asend.at[k], zfirst.at[z] if k == 0 else zr.at[k], zpeer(d))

    def pcopy(k, d):
        slot = chunks[k].at[:, pd, :, mine_l]
        return remote(slot, slot, asend.at[k], pr.at[k], ppeer(d))

    def qcopy(d, q):
        slot = chunks[0].at[q, pd, :, mine_l]
        return remote(slot, slot, asend.at[0], pfirst.at[d - 1], ppeer(d))

    def scopy(q):
        slot = chunks[0].at[q, pd, :, mine_l]
        return remote(slot, slot, asend.at[0], kr.at[0], sibling)

    def scopy_from(d):
        pp, yy = psource(d)
        slot = chunks[0].at[:, pp, :, lanes_of(core * Y + yy, 128)]
        return remote(slot, slot, asend.at[0], kr.at[0], sibling)

    def kcopy(k):
        slot = chunks[k].at[:, :, :, lanes_of(core, Y * 128)]
        return remote(slot, slot, asend.at[k], kr.at[k], sibling)

    def bcopy(d):
        return remote(bias.at[pos], bias.at[pos], bs.at[0], bs.at[1], cpeer(d))

    @named
    def to_plane(k):
        arrived(zr.at[k], span(Z - 1))
        for d in range(1, PLANE):
            pcopy(k, d).start()

    @named
    def to_sibling(k):
        arrived(pr.at[k], span((PLANE - 1) * Z))
        kcopy(k).start()

    ALL = Z - 1 + (PLANE - 1) * Z + PLANE * Z

    with jax.named_scope("barrier"):
        pl.semaphore_wait(barrier, greeted)
    def to_z(k):
        for d in range(1, Z):
            zcopy(k, d).start()

    to_z(0)
    for d in range(1, PLANE):
        qcopy(d, z).start()
    scopy(z).start()
    own = padded(projection[...].astype(F32))
    own = jnp.concatenate([own, jnp.zeros((RB, 128 - own.shape[1]), F32)], axis=1)
    ptr[z, pd, :, lanes_of(pos, 128)] = pltpu.roll(own, lax.rem(96 * col_i, 128), 1).astype(BF16)
    for j in range(FF // HC):
        exr[j, z, pd, :, lanes_of(pos, 128)] = padded(expansion[:, j * 128:(j + 1) * 128])
        rtr[j, z, pd, :, lanes_of(pos, 128)] = padded(reduction[:, j * 128:(j + 1) * 128])
    vrow = jnp.concatenate([packed_bias[...].reshape(1, -1), jnp.zeros((1, D - packed_bias.shape[0]), F32)], axis=1)
    vrow = pltpu.roll(jnp.broadcast_to(vrow, (8, D)), 32 * col_i, 1)
    bias[pos] = jnp.concatenate([vrow[:4], jnp.broadcast_to(expansion_bias[...].reshape(1, -1), (4, D))], axis=0)

    for d in range(1, 2 * Y):
        bcopy(d).start()

    x[rows:, :] = jnp.zeros((x.shape[0] - rows, D), BF16)
    up[rows:, :] = jnp.zeros((RP - rows, D), BF16)
    for h in range(PAIRS):
        qkv[h, RP:, :] = jnp.zeros((qkv.shape[1] - RP, D), BF16)
    tail = attn.shape[0] - RP + 16
    attn[RP - 16:, :] = jnp.zeros((tail, D), BF16)
    rinv[RP - 16:, :] = jnp.zeros((tail, D), F32)
    pgr[RP - 16:, :] = jnp.zeros((tail, PAIRS * D), BF16)
    fs = first_scale[...].reshape(1, D)
    fh = first_shift[...].reshape(1, D)
    ss = second_scale[...].reshape(1, D)
    sh = second_shift[...].reshape(1, D)
    prb = projection_bias[...].reshape(1, D)
    rdb = reduction_bias[...].reshape(1, D)
    cin.wait()
    cup.wait()

    def ln1(i, _):
        s = rows_of(i, SMALL)
        v = x[s, :].astype(F32)
        avg = mean(v)
        inv = lax.rsqrt(mean(v * v) - avg * avg + EPS)
        normed = (v - avg) * inv
        n1[s, :] = normed
        inv1[s, 0:64] = jnp.broadcast_to(inv, (SMALL, 64))
        rows1[s, :] = (normed * fs + fh).astype(BF16)
        return 0

    @named
    def pass_on(d):
        q = znear(d - 1)
        arrived(zfirst.at[q], chunks[0].at[q, pd, :, mine_l])
        for e in range(1, PLANE):
            qcopy(e, q).start()
        scopy(q).start()

    loop(0, nsm, ln1, 0)
    for k in (1, 2, 3):
        to_z(k)
    for d in range(1, Z):
        pass_on(d)
    for k in range(4, len(chunks)):
        to_z(k)
    with jax.named_scope("plane0"):
        for d in range(1, PLANE):
            if d == PLANE - 1:
                to_plane(1)
            arrived(pfirst.at[d - 1], span(Z))
            scopy_from(d).start()
    to_plane(2)
    arrived(bs.at[1], n1.at[0:8 * (2 * Y - 1)])

    lane = lax.broadcasted_iota(jnp.int32, (KEYS, 128), 1)
    even = lane < 64
    zero = jnp.zeros((KEYS, 128), BF16)
    one = jnp.ones((KEYS, 128), BF16)
    ones_e = jnp.where(even, one, zero)
    ones_o = jnp.where(even, zero, one)

    def place(c):
        return (c % 2) * Y + c // 2

    if RV != RB:
        wide = Z * PD * RB
        r_ = lax.broadcasted_iota(jnp.int32, (D, wide), 0)
        c_ = lax.broadcasted_iota(jnp.int32, (D, wide), 1)
        pick = jnp.where(c_ == (r_ // RV) * RB + lax.rem(r_, RV), 1.0, 0.0).astype(BF16)

    def compact(v):
        v = v.reshape(Z * PD * RB, v.shape[-1])
        return v if RV == RB else nn(pick, v).astype(BF16)

    def spread(v):
        v = v.astype(BF16)
        v = v if RV == RB else tn(pick, v).astype(BF16)
        return v.reshape(Z, PD, RB, v.shape[-1])

    def merged(tile, first, second, upto):
        if first == second:
            return tile(first)
        a, b = tile(first), tile(second)
        return jnp.where(lax.broadcasted_iota(jnp.int32, a.shape, 1) < upto, a, b)

    @named
    def assemble(h):
        kcopy(h).wait_recv()
        for j, (first, second, upto) in enumerate(TILES[h]):
            wp[:, h * D + j * 128:h * D + (j + 1) * 128] = merged(
                lambda c: compact(wpk[h, :, :, :, place(c) * 128:(place(c) + 1) * 128]), first, second, upto)

    def bias_of(h):
        def tile(c):
            t = (h + c) % 3
            return bias[place(c), 0:1, t * 128:(t + 1) * 128]
        return jnp.concatenate([merged(tile, *t) for t in TILES[h]], axis=1)

    def keep(ref, i, value):
        last = min(rows, (i + 1) * SMALL)
        ref[i * SMALL:last, :] = value[:last - i * SMALL]

    def again(ref, i):
        last = min(rows, (i + 1) * SMALL)
        value = ref[i * SMALL:last, :]
        more = (i + 1) * SMALL - last
        return value if not more else jnp.concatenate([value, jnp.zeros((more, D), value.dtype)], axis=0)

    def window(i):
        first = i * SEQ
        base = (first // 16) * 16
        return first - base, base if isinstance(i, int) else pl.multiple_of(base, 16)

    before = ((to_plane, 3), (to_plane, 4), (to_sibling, 1)), ((to_plane, 7),), ((to_plane, 9), (to_sibling, 3))
    after = (
        ((to_plane, 5), (to_sibling, 2), (to_plane, 6)),
        ((to_plane, 8),),
        ((to_sibling, 4),),
    )

    def do(steps):
        for step, k in steps:
            step(k)

    for h in range(PAIRS):
        hl = pl.ds(h * 128, 128)
        if h < 2:
            both = (0,) if h == 0 else tuple(range(1, PAIRS))
            for g in both:
                assemble(g)
            pb = jnp.concatenate([bias_of(g) for g in both], axis=1)

            def project(i, _):
                s = rows_of(i, BIG)
                v = (nn(rows1[s, :], wp[:, both[0] * D:(both[-1] + 1) * D]) + pb).astype(BF16)
                for n, g in enumerate(both):
                    qkv[g, s, :] = v[:, n * D:(n + 1) * D]
                return 0

            loop(0, nbig, project, 0)

        def attend(i, _):
            off, base = window(i)
            qw = pl.ds(base, WIN)
            kk = pl.ds(base, KEYS)
            q = qkv[h, qw, 0:128]
            k = qkv[h, kk, 128:256]
            v = qkv[h, kk, 256:384]
            col = lax.broadcasted_iota(jnp.int32, (WIN, KEYS), 1) - off
            ok = (col >= 0) & (col < SEQ)
            es = []
            for m in (even, ~even):
                s = nt(q, jnp.where(m, k, zero))
                s = jnp.where(ok, s, -1e30)
                top = jnp.max(s, axis=1, keepdims=True)
                es.append(jnp.exp((s - top) * 0.125).astype(BF16))
            est[h, i, 0] = es[0]
            est[h, i, 1] = es[1]
            mix = nn(es[0], jnp.concatenate([jnp.where(even, v, zero), ones_e], axis=1)) + nn(
                es[1], jnp.concatenate([jnp.where(even, zero, v), ones_o], axis=1))
            r = 1.0 / mix[:, 128:]
            o = mix[:, :128] * r
            rid = lax.broadcasted_iota(jnp.int32, (WIN, 128), 0) - off
            mine = (rid >= 0) & (rid < SEQ)
            attn[qw, hl] = jnp.where(mine, o, attn[qw, hl].astype(F32)).astype(BF16)
            rinv[qw, hl] = jnp.where(mine, r, rinv[qw, hl])
            return 0

        do(before[h])
        unrolled(0, images, attend, 0)
        do(after[h])

    kcopy(3).wait_recv()
    lane_d = lax.broadcasted_iota(jnp.int32, (D, 128), 1)
    tiles = [compact(ptr[:, :, :, place(c) * 128:(place(c) + 1) * 128]) for c in range(4)]
    pt[:, 0:128] = jnp.where(lane_d < 96, tiles[0], tiles[1])
    pt[:, 128:256] = jnp.where(lane_d < 64, tiles[1], tiles[2])
    pt[:, 256:384] = jnp.where(lane_d < 32, tiles[2], tiles[3])
    def exb_of(j):
        return jnp.concatenate([bias[p, 4:5, j * 128:(j + 1) * 128] for p in range(4)], axis=1)


    def ln2(i, _):
        s = rows_of(i, SMALL)
        v = x[s, :].astype(F32) + nt(attn[s, :], pt[...]) + prb
        avg = mean(v)
        inv = lax.rsqrt(mean(v * v) - avg * avg + EPS)
        normed = (v - avg) * inv
        acc1[s, :] = v + rdb
        n2[s, :] = normed
        inv1[s, 64:128] = jnp.broadcast_to(inv, (SMALL, 64))
        x[s, :] = (normed * ss + sh).astype(BF16)
        keep(o_grad, i, jnp.zeros((SMALL, D), F32))
        return 0

    unrolled(0, nsm, ln2, 0)
    to_sibling(5)

    def part(big, small, k):
        return big.at[k] if k < PAIRS else small.at[k - PAIRS]

    def width(k):
        return 256 if k < PAIRS else 128

    def g1(k):
        half = Y * width(k)
        return remote(part(gm, gh, k).at[:, :, :, lanes_of(1 - core, half)], part(rm1, rh1, k),
                      gsend.at[k], g1r.at[k], sibling)

    def g2(k, d):
        pp, yy = pplace(d)
        return remote(part(sm1, sh1, k).at[:, pp, :, lanes_of(yy, width(k))], part(rm2, rh2, k).at[d - 1],
                      gsend.at[k], g2r.at[k], ppeer(d))

    def g3(k, d):
        return remote(part(sm2, sh2, k).at[znear(d - 1)], part(rm3, rh3, k).at[z], gsend.at[k], g3r.at[k], zpeer(d))

    @named
    def sum1(k):
        g1(k).wait_recv()
        own = part(gm, gh, k)[:, :, :, lanes_of(core, Y * width(k))]
        part(sm1, sh1, k)[...] = (own.astype(F32) + part(rm1, rh1, k)[...].astype(F32)).astype(BF16)
        for d in range(1, PLANE):
            g2(k, d).start()

    LAST = 3 + PAIRS

    def piece1(d):
        pp, yy = pplace(d)
        return remote(gh.at[PAIRS, :, pp, :, lanes_of((1 - core) * Y + yy, 128)],
                      rh1.at[PAIRS, :, pp, :, lanes_of(yy, 128)], gsend.at[LAST], glast.at[d], sibling)

    def piece_sum(d):
        pp, yy = pplace(d)
        piece1(d).wait_recv()
        own = gh[PAIRS, :, pp, :, lanes_of(core * Y + yy, 128)]
        got = rh1[PAIRS, :, pp, :, lanes_of(yy, 128)]
        sh1[PAIRS, :, pp, :, lanes_of(yy, 128)] = (own.astype(F32) + got.astype(F32)).astype(BF16)
        if d:
            g2(LAST, d).start()

    @named
    def sum1_last(_):
        for d in list(range(1, PLANE)) + [0]:
            piece_sum(d)

    @named
    def sum2(k):
        arrived(g2r.at[k], span((PLANE - 1) * Z * (width(k) // 128)))
        total = part(sm1, sh1, k)[:, pd, :, lanes_of(y, width(k))].astype(F32)
        for d in range(1, PLANE):
            total += part(rm2, rh2, k)[d - 1].astype(F32)
        part(sm2, sh2, k)[...] = total.astype(BF16)
        for d in range(1, Z):
            g3(k, d).start()

    @named
    def sum3(k):
        arrived(g3r.at[k], span((Z - 1) * (width(k) // 128)))
        total = part(sm2, sh2, k)[z].astype(F32)
        for d in range(1, Z):
            total += part(rm3, rh3, k)[znear(d - 1)].astype(F32)
        return total

    vec[...] = jnp.zeros(vec.shape, F32)
    spot = (
        ((to_sibling, 6), (to_sibling, 7)),
        ((to_sibling, 8), (to_sibling, 9), (sum1, 0)),
        ((sum1, 1),),
    )
    NH = FF // HC
    mlp_in = [((kcopy, 4 + 2 * j), (kcopy, 5 + 2 * j)) for j in range(NH)]

    def chunk(j, _):
        for n in range(NH):
            pl.when(j == n)(lambda n=n: (kcopy(4 + 2 * n).wait_recv(), kcopy(5 + 2 * n).wait_recv(), None)[2])
        if RV != RB:
            exc[...] = compact(exr[j])
            rtc[...] = compact(rtr[j])

        def ex_of():
            return exc[...] if RV != RB else exr[j].reshape(D, HC)

        def rt_of():
            return rtc[...] if RV != RB else rtr[j].reshape(D, HC)

        tile = lanes_of(j, 128)
        exb = jnp.concatenate([bias[p, 4:5, tile] for p in range(4)], axis=1)
        bsum = jnp.zeros((1, HC), F32)
        for i in range(nbig):
            s = rows_of(i, BIG)
            pre = nn(x[s, :], ex_of()) + exb
            ug = nn(up[s, :], rt_of())
            cdf = 0.5 + 0.5 * lax.erf(pre * ROOT_HALF)
            act[j, s, :] = (pre * cdf).astype(BF16)
            g = ug * (cdf + pre * (jnp.exp(pre * pre * -0.5) * INV_ROOT_TAU))
            hg[s, :] = g.astype(BF16)
            last = min(rows, (i + 1) * BIG)
            back = nt(hg[s, :], ex_of())
            o_grad[i * BIG:last, :] += back[:last - i * BIG]
            bsum += jnp.sum(g, axis=0, keepdims=True)
        for p in range(4):
            vec[9 + p:10 + p, tile] = bsum[:, p * 128:(p + 1) * 128]
        for n in range(NH):
            pl.when(j == n)(lambda n=n: do(spot[n]))
        for base, g in ((0, tn(x[0:RP, :], hg[...])), (128, tn(up[...], act[j]))):
            for p in range(4):
                gm[j, :, :, :, p * 256 + base:p * 256 + base + 128] = spread(g[:, p * 128:(p + 1) * 128])
        for n in range(NH):
            pl.when(j == n)(lambda n=n: (g1(n).start(), None)[1])
        return 0

    loop(0, NH, chunk, 0)

    def ln2b(i, carry):
        s = rows_of(i, SMALL)
        u = up[s, :].astype(F32)
        g = again(o_grad, i)
        normed = n2[s, :]
        inv = inv1[s, 64:65]
        scaled = g * ss
        d = u + inv * (scaled - mean(scaled) - normed * mean(scaled * normed))
        keep(o_grad, i, d)
        hg[s, 0:D] = d.astype(BF16)
        x[s, :] = nn(d.astype(BF16), pt[...]).astype(BF16)
        terms = (d, u, g * normed, g)
        return tuple(a + jnp.sum(t, axis=0, keepdims=True) for a, t in zip(carry, terms))

    zr1 = jnp.zeros((1, D), F32)
    sums = unrolled(0, nsm, ln2b, (zr1,) * 4)
    for r, t in zip((0, 1, 4, 5), sums):
        vec[r:r + 1, :] = t
    sum1(2)
    sum2(0)
    gj = tn(hg[:, 0:D], attn[0:RP, :]).astype(BF16)
    t0, t1, t2 = gj[:, 0:128], gj[:, 128:256], gj[:, 256:384]
    for c, t in enumerate((t0, jnp.where(lane_d < 64, t1, t0), jnp.where(lane_d < 64, t2, t1), t2)):
        gh[0, :, :, :, place(c) * 128:(place(c) + 1) * 128] = spread(t)
    g1(3).start()

    def finish_mlp(j):
        total = sum3(j)
        small[1, :, j * 128:(j + 1) * 128] = total[:, :128]
        small[2, :, j * 128:(j + 1) * 128] = total[:, 128:]

    def finish_projection(_):
        t = pltpu.roll(sum3(3), lax.rem(128 - lax.rem(96 * col_i, 128), 128), 1)
        small[3, :, 0:128] = t

    behind = (
        ((sum1, 3), (sum2, 1)),
        ((sum1, 4), (sum2, 2), (sum2, 3), (finish_mlp, 0)),
        ((sum1, 5), (sum2, 4), (finish_mlp, 1)),
    )
    for h in range(PAIRS):
        hl = pl.ds(h * 128, 128)

        def attend_back(i, _):
            off, base = window(i)
            qw = pl.ds(base, WIN)
            kk = pl.ds(base, KEYS)
            q = qkv[h, qw, 0:128]
            k = qkv[h, kk, 128:256]
            v = qkv[h, kk, 256:384]
            rid = lax.broadcasted_iota(jnp.int32, (WIN, 128), 0) - off
            mine = (rid >= 0) & (rid < SEQ)
            do = jnp.where(mine, x[qw, hl].astype(F32) * rinv[qw, hl], 0.0)
            dob = do.astype(BF16)
            xx = jnp.concatenate([dob, (do * attn[qw, hl].astype(F32)).astype(BF16)], axis=1)
            ev = even[:WIN]
            zw = zero[:WIN]
            e0 = est[h, i, 0]
            e1 = est[h, i, 1]
            d0 = (e0 * nt(xx, jnp.concatenate([jnp.where(even, v, zero), -ones_e], axis=1))).astype(BF16)
            d1 = (e1 * nt(xx, jnp.concatenate([jnp.where(even, zero, v), -ones_o], axis=1))).astype(BF16)
            dq = (nn(d0, jnp.where(even, k, zero)) + nn(d1, jnp.where(even, zero, k))) * 0.125
            dk = (tn(d0, jnp.where(ev, q, zw)) + tn(d1, jnp.where(ev, zw, q))) * 0.125
            dv = tn(e0, jnp.where(ev, dob, zw)) + tn(e1, jnp.where(ev, zw, dob))
            old = pgr[qw, h * D:(h + 1) * D].astype(F32)
            pgr[qw, h * D:h * D + 128] = jnp.where(mine, dq, old[:, 0:128]).astype(BF16)
            pgr[qw, h * D + 128:h * D + 256] = jnp.where(mine, dk[:WIN], old[:, 128:256]).astype(BF16)
            pgr[qw, h * D + 256:h * D + 384] = jnp.where(mine, dv[:WIN], old[:, 256:384]).astype(BF16)
            return 0

        unrolled(0, images, attend_back, 0)
        do(behind[h])
        gp = tn(rows1[...], pgr[0:RP, h * D:(h + 1) * D])
        for c, j in enumerate(SHARES[h]):
            gh[1 + h, :, :, :, place(c) * 128:(place(c) + 1) * 128] = spread(gp[:, j * 128:(j + 1) * 128])
        if h < PAIRS - 1:
            g1(4 + h).start()
        else:
            for d in list(range(1, PLANE)) + [0]:
                piece1(d).start()

        def bias_sum(i, carry):
            s = rows_of(i, SMALL)
            return carry + jnp.sum(pgr[s, h * D:(h + 1) * D].astype(F32), axis=0, keepdims=True)

        vec[6 + h:7 + h, :] = unrolled(0, nsm, bias_sum, zr1)

    vq[...] = jnp.zeros(vq.shape, F32)
    for q in range(4):
        for h in range(PAIRS):
            j = SHARES[h][q]
            vq[q, 6 + h:7 + h, :] = vec[6 + h:7 + h, j * 128:(j + 1) * 128]
            vq[q, 9 + h:10 + h, :] = vec[9 + place(q):10 + place(q), h * 128:(h + 1) * 128]

    gbuf = n2

    def ln1b(i, carry):
        s = rows_of(i, SMALL)
        g = nt(pgr[s, :], wp[...])
        gbuf[s, :] = g
        terms = (g * n1[s, :], g)
        hook(i, [(nsm // 2 - 1, lambda: sum1_last(0))])
        return tuple(a + jnp.sum(t, axis=0, keepdims=True) for a, t in zip(carry, terms))

    sums = unrolled(0, nsm, ln1b, (zr1,) * 2)

    for r, t in zip((2, 3), sums):
        vec[r:r + 1, :] = t
    wide_d = D // 4
    for q in range(4):
        vq[q, 0:6, 0:wide_d] = vec[0:6, q * wide_d:(q + 1) * wide_d]
    me = plane * 2 + core

    def v2(d):
        to = vpeer(d)
        return remote(vq.at[to[1]], vr2.at[me], vs.at[0], vs.at[1], to)

    def v3(d):
        return remote(vr3.at[z], vr3.at[z], vs.at[0], vs.at[2], zpeer(d))

    def vector2():
        arrived(vs.at[1], vspan(2 * PLANE - 1))
        total = vr2[0]
        for q in range(1, 2 * PLANE):
            total += vr2[q]
        vr3[z] = total
        for d in range(1, Z):
            v3(d).start()

    for d in range(1, 2 * PLANE):
        v2(d).start()
    vr2[me] = vq[col_i]

    def ln1c(i, _):
        s = rows_of(i, SMALL)
        normed = n1[s, :]
        inv = inv1[s, 0:1]
        scaled = gbuf[s, :] * fs
        keep(o_grad, i, again(o_grad, i) + inv * (scaled - mean(scaled) - normed * mean(scaled * normed)))
        return 0

    unrolled(0, nsm, ln1c, 0)
    def emit(i):
        s = rows_of(i, BIG)
        last = min(rows, (i + 1) * BIG)
        value = acc1[s, :]
        for j in range(NH):
            value += nt(act[j, s, :], rtr[j].reshape(D, HC) if RV == RB else compact(rtr[j]))
        o_out[i * BIG:last, :] = value[:last - i * BIG].astype(BF16)

    with jax.named_scope("emit"):
        for i in range(nbig):
            emit(i)
            do((((sum2, 5), (finish_mlp, 2)), ((finish_projection, 3), (sum2, 6)))[i] if i < 2 else ())
            if i == min(1, nbig - 1):
                vector2()
    for h in range(PAIRS - 1):
        frame[:, turn(h)] = sum3(4 + h)
    frame[:, turn(PAIRS - 1)] = sum3(3 + PAIRS)
    back = lax.rem(D - 32 * col_i, D)
    small[0] = pltpu.roll(frame[...], back, 1)
    with jax.named_scope("vec3"):
        arrived(vs.at[2], vspan(Z - 1))
    total = vr3[0]
    for q in range(1, Z):
        total += vr3[q]
    small[3, 0:8, 128:256] = total[0:8]
    for h in range(PAIRS):
        frame[0:1, turn(h)] = total[6 + h:7 + h]
        small[4, 8:9, h * 128:(h + 1) * 128] = total[9 + h:10 + h]
    small[4, 0:8, :] = pltpu.roll(frame[0:8, :], back, 1)

    with jax.named_scope("ends"):
        for k in range(len(chunks)):
            left(asend.at[k], span(ALL))
        left(bs.at[0], n1.at[0:8 * (2 * Y - 1)])
        for k in range(7):
            left(gsend.at[k], span(ALL * (width(k) // 128)))
        left(vs.at[0], vspan(2 * PLANE + Z - 2))


def finish_kernel(*refs):
    out, grad, small = refs[:3]
    outs, stage, sem = refs[3:17], refs[17:29], refs[29]
    moves = [pltpu.make_async_copy(a, b, sem.at[k]) for k, (a, b) in enumerate(zip((grad, out) + stage, (outs[1], outs[0]) + outs[2:]))]
    moves[0].start()
    moves[1].start()
    rv, wide = stage[0].shape
    stage[0][...] = small[0, :rv, :wide]
    stage[1][...] = small[3, :rv, :stage[1].shape[1]]
    stage[2][...] = small[1, :rv, :]
    stage[3][...] = small[2, :rv, :]
    stage[4][...] = small[4, 0:1, :wide].reshape(wide)
    stage[6][...] = small[4, 8:9, :].reshape(D)
    for r, k in enumerate((5, 7, 8, 9, 10, 11)):
        n = stage[k].shape[0]
        stage[k][...] = small[3, r:r + 1, 128:128 + n].reshape(n)
    for move in moves[2:]:
        move.start()
    for move in moves:
        move.wait()


def body(dps, cols, tokens, packed, packed_bias, projection, projection_bias, expansion, expansion_bias, reduction,
         reduction_bias, first_scale, first_shift, second_scale, second_shift, upstream):
    args = (tokens, packed, packed_bias, projection.T, projection_bias, expansion, expansion_bias, reduction.T,
            reduction_bias, first_scale, first_shift, second_scale, second_shift, upstream)
    rows = tokens.shape[0]
    images = rows // SEQ
    Z = min(4, dps)
    PD = dps // Z
    Y = cols // 2
    RV = packed.shape[0]
    RB = -(-RV // 16) * 16
    PLANE = PD * Y
    RP = -(-rows // BIG) * BIG
    reach = ((images - 1) * SEQ) // 16 * 16
    XQ = max(RP + 16, reach + WIN)
    XP = max(RP + 16, reach + KEYS)
    cfg = (Z, PD, Y, RB, RV, rows)
    V = pl.BlockSpec(memory_space=pltpu.VMEM)
    A = pl.BlockSpec(memory_space=pl.ANY)
    S = jax.ShapeDtypeStruct
    vm = pltpu.VMEM
    dma = pltpu.SemaphoreType.DMA
    NH = FF // HC
    NC = PAIRS + 1 + 2 * NH
    small = RV != RB
    outs = (
        S((rows, D), BF16), S((rows, D), F32),
        S(packed.shape, F32), S(projection.shape[::-1], F32), S(expansion.shape, F32), S(reduction.shape[::-1], F32),
        S(packed_bias.shape, F32), S((D // cols,), F32), S(expansion_bias.shape, F32),
    ) + (S((D // cols,), F32),) * 5
    narrow = (args[1], args[2], args[3], args[4], args[5], args[6], args[7]) + args[8:13]
    scratch = [vm(a.shape, a.dtype) for a in narrow] + [
        vm((XQ, D), BF16), vm((RP, D), BF16),
        vm((RP, D), F32), vm((RP, D), BF16),
        vm((PAIRS, XP, D), BF16), vm((XQ, D), BF16),
        vm((PAIRS, images, 2, WIN, KEYS), BF16), vm((XQ, D), F32),
        vm((RP, D), F32), vm((RP, D), F32),
        vm((NH, RP, HC), BF16), vm((RP, HC), BF16),
        vm((XQ, PAIRS * D), BF16), vm((max(RP, (Z - 1 + (2 * PLANE - 1) * Z) * RB), 128), F32),
        vm((PAIRS, Z, PD, RB, 4 * 128), BF16), vm((Z, PD, RB, 4 * 128), BF16),
        vm((NH, Z, PD, RB, HC), BF16), vm((NH, Z, PD, RB, HC), BF16),
        vm((D, PAIRS * D), BF16), vm((D, D), BF16),
        vm((D, HC) if small else (16, 128), BF16), vm((D, HC) if small else (16, 128), BF16),
        vm((4, 8, D), F32),
        vm((NH, Z, PD, RB, 4 * 256), BF16), vm((4, Z, PD, RB, 4 * 128), BF16),
        vm((NH, Z, PD, RB, Y * 256), BF16), vm((NH, PLANE - 1, Z, RB, 256), BF16), vm((NH, Z, RB, 256), BF16),
        vm((4, Z, PD, RB, Y * 128), BF16), vm((4, PLANE - 1, Z, RB, 128), BF16), vm((4, Z, RB, 128), BF16),
        vm((NH, Z, PD, RB, Y * 256), BF16), vm((NH, Z, RB, 256), BF16),
        vm((4, Z, PD, RB, Y * 128), BF16), vm((4, Z, RB, 128), BF16),
        vm((RB, D), F32), vm((16, D), F32),
        vm((4, 16, 128), F32), vm((2 * PLANE, 16, 128), F32), vm((Z, 16, 128), F32),
        dma((NC,)), dma((Z,)), dma((PLANE - 1,)), dma((NC,)), dma((NC,)), dma((NC,)),
        dma((2,)), dma((7,)), dma((7,)), dma((7,)), dma((7,)), dma((PLANE,)), dma((3,)),
    ]
    got = pl.pallas_call(
        functools.partial(layer_kernel, cfg),
        out_shape=(vm((rows, D), BF16), vm((rows, D), F32), vm((5, RB, D), F32)),
        in_specs=[A] * 14,
        out_specs=(V,) * 3,
        scratch_shapes=scratch,
        compiler_params=pltpu.CompilerParams(vmem_limit_bytes=VMEM - rows * D * 6 - 5 * RB * D * 4 - 65536, collective_id=0, has_side_effects=True),
    )(*args)
    got = pl.pallas_call(
        finish_kernel,
        out_shape=outs,
        in_specs=[V] * 3,
        out_specs=(A,) * 14,
        scratch_shapes=[vm(o.shape, o.dtype) for o in outs[2:]] + [dma((14,))],
        compiler_params=pltpu.CompilerParams(vmem_limit_bytes=2 * 1024 * 1024),
    )(*(pltpu.with_memory_space_constraint(v, pltpu.VMEM) for v in got))
    return got[:3] + (got[3].T, got[4], got[5].T) + tuple(got[6:])


def solution(mesh):
    placed = (
        P(("dp", "col"), None), P("dp", "col"), P("col"), P("col", "dp"), P(), P("dp", "col"), P("col"),
        P("col", "dp"), P(), P(), P(), P(), P(), P(("dp", "col"), None),
    )
    return jax.shard_map(
        functools.partial(body, mesh.shape["dp"], mesh.shape["col"]),
        mesh=mesh,
        in_specs=placed,
        out_specs=(
            P(("dp", "col"), None), P(("dp", "col"), None),
            P("dp", "col"), P("col", "dp"), P("dp", "col"), P("col", "dp"),
        ) + (P("col"),) * 8,
        check_vma=False,
    )
```

```python
import functools

import jax
import jax.numpy as jnp
from jax import lax
from jax.experimental import pallas as pl
from jax.experimental.pallas import tpu as pltpu
from jax.sharding import PartitionSpec as P

SEQ = 197
EPS = 1e-06
ROOT_HALF = 0.7071067811865476
INV_ROOT_TAU = 0.3989422804014327
F32, BF16 = jnp.float32, jnp.bfloat16
MESH = pl.DeviceIdType.MESH
D = 384
FF = 1536
PAIRS = 3
WIN = 224
KEYS = 256
BIG = 528
SMALL = 176
HC = 512
VMEM = 67_000_000


def nn(a, b):
    return lax.dot_general(a, b, (((1,), (0,)), ((), ())), preferred_element_type=F32)


def nt(a, b):
    return lax.dot_general(a, b, (((1,), (1,)), ((), ())), preferred_element_type=F32)


def tn(a, b):
    return lax.dot_general(a, b, (((0,), (0,)), ((), ())), preferred_element_type=F32)


def rows_of(i, size):
    if isinstance(i, int):
        return pl.ds(i * size, size)
    return pl.ds(pl.multiple_of(i * size, 16), size)


def lanes_of(i, size):
    return pl.ds(pl.multiple_of(i * size, 128), size)


def mean(x):
    return jnp.sum(x, axis=1, keepdims=True) * (1.0 / x.shape[1])


def hook(i, steps):
    for at, step in steps:
        if isinstance(i, int):
            if i == at:
                step()
        else:
            pl.when(i == at)(lambda step=step: (step(), None)[1])


def unrolled(lo, hi, function, init):
    with jax.named_scope(function.__name__):
        for i in range(lo, hi):
            init = function(i, init)
    return init


def loop(lo, hi, function, init):
    with jax.named_scope(function.__name__):
        return lax.fori_loop(lo, hi, function, init)


def named(function):
    def inner(*a):
        with jax.named_scope(function.__name__ + "_".join(str(v) for v in a if isinstance(v, int))):
            return function(*a)
    return inner


TILES = (
    ((0, 0, 128), (1, 1, 128), (2, 3, 96)),
    ((0, 0, 128), (1, 2, 64), (3, 3, 128)),
    ((0, 1, 32), (2, 2, 128), (3, 3, 128)),
)
SHARES = ((0, 1, 2, 2), (0, 1, 1, 2), (0, 0, 1, 2))


def layer_kernel(cfg, *refs):
    Z, PD, Y, RB, RV, rows = cfg
    PLANE = PD * Y
    RP = -(-rows // BIG) * BIG
    images = rows // SEQ
    nsm, nbig = RP // SMALL, RP // BIG
    tokens, upstream, outside = refs[0], refs[13], refs[1:13]
    o_out, o_grad, small, refs = refs[14], refs[15], refs[16], refs[17:]
    (packed, packed_bias, projection, projection_bias, expansion, expansion_bias, reduction,
     reduction_bias, first_scale, first_shift, second_scale, second_shift,
     x, up, n1, rows1, qkv, attn, est, rinv, n2, acc1, act, hg, pgr, inv1,
     wpk, ptr, exr, rtr, wp, pt, exc, rtc, bias,
     gm, gh, rm1, rm2, rm3, rh1, rh2, rh3, sm1, sm2, sh1, sh2, frame, vec, vq, vr2, vr3,
     asend, zfirst, pfirst, zr, pr, kr, bs, gsend, g1r, g2r, g3r, glast, vs) = refs

    dp_i, col_i = lax.axis_index("dp"), lax.axis_index("col")
    z, pd = dp_i // PD, lax.rem(dp_i, PD)
    y, core = col_i // 2, lax.rem(col_i, 2)
    pos = core * Y + y
    plane = pd * Y + y

    def device(zz, pp, yy, cc):
        return (zz * PD + pp, yy * 2 + cc)

    def znear(s):
        rising = jnp.where(s < z, s, s + 1)
        down = Z - 1 - s
        falling = jnp.where(down > z, down, down - 1)
        return jnp.where(2 * z < Z, rising, falling)

    def zpeer(s):
        return device(znear(s - 1), pd, y, core)

    def pplace(d):
        return lax.rem(pd + d // Y, PD), lax.rem(y + d % Y, Y)

    def psource(d):
        return lax.rem(pd + PD - d // Y, PD), lax.rem(y + Y - d % Y, Y)

    def ppeer(d):
        pp, yy = pplace(d)
        return device(z, pp, yy, core)

    def vpeer(d):
        pp, yy = pplace(d // 2)
        return device(z, pp, yy, lax.rem(core + d % 2, 2))

    sibling = device(z, pd, y, 1 - core)

    def cpeer(d):
        return (dp_i, lax.rem(col_i + d, 2 * Y))

    def remote(src, dst, send, recv, to):
        return pltpu.make_async_remote_copy(
            src_ref=src, dst_ref=dst, send_sem=send, recv_sem=recv, device_id=to, device_id_type=MESH)

    barrier = pltpu.get_barrier_semaphore()
    near = [zpeer(d) for d in range(1, Z)] + [vpeer(d) for d in range(1, 2 * PLANE)]
    for to in near:
        pl.semaphore_signal(barrier, inc=1, device_id=to, device_id_type=MESH)
    greeted = len(near)

    cin = pltpu.make_async_copy(tokens, x.at[pl.ds(0, rows)], gsend.at[5])
    cup = pltpu.make_async_copy(upstream, up.at[pl.ds(0, rows)], gsend.at[6])
    inside = (packed, packed_bias, projection, projection_bias, expansion, expansion_bias, reduction,
              reduction_bias, first_scale, first_shift, second_scale, second_shift)
    loads = [pltpu.make_async_copy(a, b, asend.at[n] if n < 8 else gsend.at[n - 8]) for n, (a, b) in enumerate(zip(outside, inside))]
    for n in (0, 2, 4, 6, 1, 5, 3, 7, 8, 9, 10, 11):
        loads[n].start()
    cin.start()
    cup.start()
    loads[0].wait()

    def padded(v):
        return v if RV == RB else jnp.concatenate([v, jnp.zeros((RB - RV, v.shape[1]), v.dtype)], axis=0)

    own = padded(packed[...].astype(F32))
    own = jnp.concatenate([own, jnp.zeros((RB, D - own.shape[1]), F32)], axis=1)
    frame[...] = pltpu.roll(own, 32 * col_i, 1)

    def turn(h):
        return lanes_of(lax.rem(h + col_i, 3), 128)

    for h in range(PAIRS):
        wpk[h, z, pd, :, lanes_of(pos, 128)] = frame[:, turn(h)].astype(BF16)
    chunks = [wpk.at[h] for h in range(PAIRS)] + [ptr]
    for j in range(FF // HC):
        chunks += [exr.at[j], rtr.at[j]]
    mine_l = lanes_of(pos, 128)

    def span(slots):
        return inv1.at[0:slots * RB // 2]

    def vspan(count):
        return inv1.at[0:count * 16]

    def arrived(sem, ref):
        remote(ref, ref, vs.at[0], sem, sibling).wait_recv()

    def left(sem, ref):
        remote(ref, ref, sem, vs.at[0], sibling).wait_send()

    def zcopy(k, d):
        slot = chunks[k].at[z, pd, :, mine_l]
        return remote(slot, slot, asend.at[k], zfirst.at[z] if k == 0 else zr.at[k], zpeer(d))

    def pcopy(k, d):
        slot = chunks[k].at[:, pd, :, mine_l]
        return remote(slot, slot, asend.at[k], pr.at[k], ppeer(d))

    def qcopy(d, q):
        slot = chunks[0].at[q, pd, :, mine_l]
        return remote(slot, slot, asend.at[0], pfirst.at[d - 1], ppeer(d))

    def scopy(q):
        slot = chunks[0].at[q, pd, :, mine_l]
        return remote(slot, slot, asend.at[0], kr.at[0], sibling)

    def scopy_from(d):
        pp, yy = psource(d)
        slot = chunks[0].at[:, pp, :, lanes_of(core * Y + yy, 128)]
        return remote(slot, slot, asend.at[0], kr.at[0], sibling)

    def kcopy(k):
        slot = chunks[k].at[:, :, :, lanes_of(core, Y * 128)]
        return remote(slot, slot, asend.at[k], kr.at[k], sibling)

    def bcopy(d):
        return remote(bias.at[pos], bias.at[pos], bs.at[0], bs.at[1], cpeer(d))

    @named
    def to_plane(k):
        arrived(zr.at[k], span(Z - 1))
        for d in range(1, PLANE):
            pcopy(k, d).start()

    @named
    def to_sibling(k):
        arrived(pr.at[k], span((PLANE - 1) * Z))
        kcopy(k).start()

    ALL = Z - 1 + (PLANE - 1) * Z + PLANE * Z

    with jax.named_scope("barrier"):
        pl.semaphore_wait(barrier, greeted)
    def to_z(k):
        for d in range(1, Z):
            zcopy(k, d).start()

    to_z(0)
    for d in range(1, PLANE):
        qcopy(d, z).start()
    scopy(z).start()
    for load in loads[1:]:
        load.wait()
    own = padded(projection[...].astype(F32))
    own = jnp.concatenate([own, jnp.zeros((RB, 128 - own.shape[1]), F32)], axis=1)
    ptr[z, pd, :, lanes_of(pos, 128)] = pltpu.roll(own, lax.rem(96 * col_i, 128), 1).astype(BF16)
    for j in range(FF // HC):
        exr[j, z, pd, :, lanes_of(pos, 128)] = padded(expansion[:, j * 128:(j + 1) * 128])
        rtr[j, z, pd, :, lanes_of(pos, 128)] = padded(reduction[:, j * 128:(j + 1) * 128])
    vrow = jnp.concatenate([packed_bias[...].reshape(1, -1), jnp.zeros((1, D - packed_bias.shape[0]), F32)], axis=1)
    vrow = pltpu.roll(jnp.broadcast_to(vrow, (8, D)), 32 * col_i, 1)
    bias[pos] = jnp.concatenate([vrow[:4], jnp.broadcast_to(expansion_bias[...].reshape(1, -1), (4, D))], axis=0)

    for d in range(1, 2 * Y):
        bcopy(d).start()

    x[rows:, :] = jnp.zeros((x.shape[0] - rows, D), BF16)
    up[rows:, :] = jnp.zeros((RP - rows, D), BF16)
    for h in range(PAIRS):
        qkv[h, RP:, :] = jnp.zeros((qkv.shape[1] - RP, D), BF16)
    tail = attn.shape[0] - RP + 16
    attn[RP - 16:, :] = jnp.zeros((tail, D), BF16)
    rinv[RP - 16:, :] = jnp.zeros((tail, D), F32)
    pgr[RP - 16:, :] = jnp.zeros((tail, PAIRS * D), BF16)
    fs = first_scale[...].reshape(1, D)
    fh = first_shift[...].reshape(1, D)
    ss = second_scale[...].reshape(1, D)
    sh = second_shift[...].reshape(1, D)
    prb = projection_bias[...].reshape(1, D)
    rdb = reduction_bias[...].reshape(1, D)
    cin.wait()
    cup.wait()

    def ln1(i, _):
        s = rows_of(i, SMALL)
        v = x[s, :].astype(F32)
        avg = mean(v)
        inv = lax.rsqrt(mean(v * v) - avg * avg + EPS)
        normed = (v - avg) * inv
        n1[s, :] = normed
        inv1[s, 0:64] = jnp.broadcast_to(inv, (SMALL, 64))
        rows1[s, :] = (normed * fs + fh).astype(BF16)
        return 0

    @named
    def pass_on(d):
        q = znear(d - 1)
        arrived(zfirst.at[q], chunks[0].at[q, pd, :, mine_l])
        for e in range(1, PLANE):
            qcopy(e, q).start()
        scopy(q).start()

    loop(0, nsm, ln1, 0)
    for k in (1, 2, 3):
        to_z(k)
    for d in range(1, Z):
        pass_on(d)
    for k in range(4, len(chunks)):
        to_z(k)
    with jax.named_scope("plane0"):
        for d in range(1, PLANE):
            if d == PLANE - 1:
                to_plane(1)
            arrived(pfirst.at[d - 1], span(Z))
            scopy_from(d).start()
    to_plane(2)
    arrived(bs.at[1], n1.at[0:8 * (2 * Y - 1)])

    lane = lax.broadcasted_iota(jnp.int32, (KEYS, 128), 1)
    even = lane < 64
    zero = jnp.zeros((KEYS, 128), BF16)
    one = jnp.ones((KEYS, 128), BF16)
    ones_e = jnp.where(even, one, zero)
    ones_o = jnp.where(even, zero, one)

    def place(c):
        return (c % 2) * Y + c // 2

    if RV != RB:
        wide = Z * PD * RB
        r_ = lax.broadcasted_iota(jnp.int32, (D, wide), 0)
        c_ = lax.broadcasted_iota(jnp.int32, (D, wide), 1)
        pick = jnp.where(c_ == (r_ // RV) * RB + lax.rem(r_, RV), 1.0, 0.0).astype(BF16)

    def compact(v):
        v = v.reshape(Z * PD * RB, v.shape[-1])
        return v if RV == RB else nn(pick, v).astype(BF16)

    def spread(v):
        v = v.astype(BF16)
        v = v if RV == RB else tn(pick, v).astype(BF16)
        return v.reshape(Z, PD, RB, v.shape[-1])

    def merged(tile, first, second, upto):
        if first == second:
            return tile(first)
        a, b = tile(first), tile(second)
        return jnp.where(lax.broadcasted_iota(jnp.int32, a.shape, 1) < upto, a, b)

    @named
    def assemble(h):
        kcopy(h).wait_recv()
        for j, (first, second, upto) in enumerate(TILES[h]):
            wp[:, h * D + j * 128:h * D + (j + 1) * 128] = merged(
                lambda c: compact(wpk[h, :, :, :, place(c) * 128:(place(c) + 1) * 128]), first, second, upto)

    def bias_of(h):
        def tile(c):
            t = (h + c) % 3
            return bias[place(c), 0:1, t * 128:(t + 1) * 128]
        return jnp.concatenate([merged(tile, *t) for t in TILES[h]], axis=1)

    def keep(ref, i, value):
        last = min(rows, (i + 1) * SMALL)
        ref[i * SMALL:last, :] = value[:last - i * SMALL]

    def again(ref, i):
        last = min(rows, (i + 1) * SMALL)
        value = ref[i * SMALL:last, :]
        more = (i + 1) * SMALL - last
        return value if not more else jnp.concatenate([value, jnp.zeros((more, D), value.dtype)], axis=0)

    def window(i):
        first = i * SEQ
        base = (first // 16) * 16
        return first - base, base if isinstance(i, int) else pl.multiple_of(base, 16)

    before = ((to_plane, 3), (to_plane, 4), (to_sibling, 1)), ((to_plane, 7),), ((to_plane, 8), (to_plane, 9), (to_sibling, 3), (to_sibling, 4))
    after = (
        ((to_plane, 5), (to_sibling, 2), (to_plane, 6)),
        (),
        ((to_sibling, 5),),
    )

    def do(steps):
        for step, k in steps:
            step(k)

    for h in range(PAIRS):
        hl = pl.ds(h * 128, 128)
        if h < 2:
            both = (0,) if h == 0 else tuple(range(1, PAIRS))
            for g in both:
                assemble(g)
            pb = jnp.concatenate([bias_of(g) for g in both], axis=1)

            def project(i, _):
                s = rows_of(i, BIG)
                v = (nn(rows1[s, :], wp[:, both[0] * D:(both[-1] + 1) * D]) + pb).astype(BF16)
                for n, g in enumerate(both):
                    qkv[g, s, :] = v[:, n * D:(n + 1) * D]
                return 0

            loop(0, nbig, project, 0)

        def attend(i, _):
            off, base = window(i)
            qw = pl.ds(base, WIN)
            kk = pl.ds(base, KEYS)
            q = qkv[h, qw, 0:128]
            k = qkv[h, kk, 128:256]
            v = qkv[h, kk, 256:384]
            col = lax.broadcasted_iota(jnp.int32, (WIN, KEYS), 1) - off
            ok = (col >= 0) & (col < SEQ)
            es = []
            for m in (even, ~even):
                s = nt(q, jnp.where(m, k, zero))
                s = jnp.where(ok, s, -1e30)
                top = jnp.max(s, axis=1, keepdims=True)
                es.append(jnp.exp((s - top) * 0.125).astype(BF16))
            est[h, i, 0] = es[0]
            est[h, i, 1] = es[1]
            mix = nn(es[0], jnp.concatenate([jnp.where(even, v, zero), ones_e], axis=1)) + nn(
                es[1], jnp.concatenate([jnp.where(even, zero, v), ones_o], axis=1))
            r = 1.0 / mix[:, 128:]
            o = mix[:, :128] * r
            rid = lax.broadcasted_iota(jnp.int32, (WIN, 128), 0) - off
            mine = (rid >= 0) & (rid < SEQ)
            attn[qw, hl] = jnp.where(mine, o, attn[qw, hl].astype(F32)).astype(BF16)
            rinv[qw, hl] = jnp.where(mine, r, rinv[qw, hl])
            return 0

        do(before[h])
        unrolled(0, images, attend, 0)
        do(after[h])

    kcopy(3).wait_recv()
    lane_d = lax.broadcasted_iota(jnp.int32, (D, 128), 1)
    tiles = [compact(ptr[:, :, :, place(c) * 128:(place(c) + 1) * 128]) for c in range(4)]
    pt[:, 0:128] = jnp.where(lane_d < 96, tiles[0], tiles[1])
    pt[:, 128:256] = jnp.where(lane_d < 64, tiles[1], tiles[2])
    pt[:, 256:384] = jnp.where(lane_d < 32, tiles[2], tiles[3])
    def exb_of(j):
        return jnp.concatenate([bias[p, 4:5, j * 128:(j + 1) * 128] for p in range(4)], axis=1)


    def ln2(i, _):
        s = rows_of(i, SMALL)
        v = x[s, :].astype(F32) + nt(attn[s, :], pt[...]) + prb
        avg = mean(v)
        inv = lax.rsqrt(mean(v * v) - avg * avg + EPS)
        normed = (v - avg) * inv
        acc1[s, :] = v + rdb
        n2[s, :] = normed
        inv1[s, 64:128] = jnp.broadcast_to(inv, (SMALL, 64))
        x[s, :] = (normed * ss + sh).astype(BF16)
        keep(o_grad, i, jnp.zeros((SMALL, D), F32))
        return 0

    unrolled(0, nsm, ln2, 0)

    def part(big, small, k):
        return big.at[k] if k < PAIRS else small.at[k - PAIRS]

    def width(k):
        return 256 if k < PAIRS else 128

    def g1(k):
        half = Y * width(k)
        return remote(part(gm, gh, k).at[:, :, :, lanes_of(1 - core, half)], part(rm1, rh1, k),
                      gsend.at[k], g1r.at[k], sibling)

    def g2(k, d):
        pp, yy = pplace(d)
        return remote(part(sm1, sh1, k).at[:, pp, :, lanes_of(yy, width(k))], part(rm2, rh2, k).at[d - 1],
                      gsend.at[k], g2r.at[k], ppeer(d))

    def g3(k, d):
        return remote(part(sm2, sh2, k).at[znear(d - 1)], part(rm3, rh3, k).at[z], gsend.at[k], g3r.at[k], zpeer(d))

    @named
    def sum1(k):
        g1(k).wait_recv()
        own = part(gm, gh, k)[:, :, :, lanes_of(core, Y * width(k))]
        part(sm1, sh1, k)[...] = (own.astype(F32) + part(rm1, rh1, k)[...].astype(F32)).astype(BF16)
        for d in range(1, PLANE):
            g2(k, d).start()

    LAST = 3 + PAIRS

    def piece1(d):
        pp, yy = pplace(d)
        return remote(gh.at[PAIRS, :, pp, :, lanes_of((1 - core) * Y + yy, 128)],
                      rh1.at[PAIRS, :, pp, :, lanes_of(yy, 128)], gsend.at[LAST], glast.at[d], sibling)

    def piece_sum(d):
        pp, yy = pplace(d)
        piece1(d).wait_recv()
        own = gh[PAIRS, :, pp, :, lanes_of(core * Y + yy, 128)]
        got = rh1[PAIRS, :, pp, :, lanes_of(yy, 128)]
        sh1[PAIRS, :, pp, :, lanes_of(yy, 128)] = (own.astype(F32) + got.astype(F32)).astype(BF16)
        if d:
            g2(LAST, d).start()

    @named
    def sum1_last(_):
        for d in list(range(1, PLANE)) + [0]:
            piece_sum(d)

    @named
    def sum2(k):
        arrived(g2r.at[k], span((PLANE - 1) * Z * (width(k) // 128)))
        total = part(sm1, sh1, k)[:, pd, :, lanes_of(y, width(k))].astype(F32)
        for d in range(1, PLANE):
            total += part(rm2, rh2, k)[d - 1].astype(F32)
        part(sm2, sh2, k)[...] = total.astype(BF16)
        for d in range(1, Z):
            g3(k, d).start()

    @named
    def sum3(k):
        arrived(g3r.at[k], span((Z - 1) * (width(k) // 128)))
        total = part(sm2, sh2, k)[z].astype(F32)
        for d in range(1, Z):
            total += part(rm3, rh3, k)[znear(d - 1)].astype(F32)
        return total

    vec[...] = jnp.zeros(vec.shape, F32)
    spot = (
        ((to_sibling, 6), (to_sibling, 7)),
        ((to_sibling, 8), (to_sibling, 9), (sum1, 0)),
        ((sum1, 1),),
    )
    NH = FF // HC
    mlp_in = [((kcopy, 4 + 2 * j), (kcopy, 5 + 2 * j)) for j in range(NH)]

    def chunk(j, _):
        for n in range(NH):
            pl.when(j == n)(lambda n=n: (kcopy(4 + 2 * n).wait_recv(), kcopy(5 + 2 * n).wait_recv(), None)[2])
        if RV != RB:
            exc[...] = compact(exr[j])
            rtc[...] = compact(rtr[j])

        def ex_of():
            return exc[...] if RV != RB else exr[j].reshape(D, HC)

        def rt_of():
            return rtc[...] if RV != RB else rtr[j].reshape(D, HC)

        tile = lanes_of(j, 128)
        exb = jnp.concatenate([bias[p, 4:5, tile] for p in range(4)], axis=1)
        bsum = jnp.zeros((1, HC), F32)
        for i in range(nbig):
            s = rows_of(i, BIG)
            pre = nn(x[s, :], ex_of()) + exb
            ug = nn(up[s, :], rt_of())
            cdf = 0.5 + 0.5 * lax.erf(pre * ROOT_HALF)
            act[j, s, :] = (pre * cdf).astype(BF16)
            g = ug * (cdf + pre * (jnp.exp(pre * pre * -0.5) * INV_ROOT_TAU))
            hg[s, :] = g.astype(BF16)
            last = min(rows, (i + 1) * BIG)
            back = nt(hg[s, :], ex_of())
            o_grad[i * BIG:last, :] += back[:last - i * BIG]
            bsum += jnp.sum(g, axis=0, keepdims=True)
        for p in range(4):
            vec[9 + p:10 + p, tile] = bsum[:, p * 128:(p + 1) * 128]
        for n in range(NH):
            pl.when(j == n)(lambda n=n: do(spot[n]))
        for base, g in ((0, tn(x[0:RP, :], hg[...])), (128, tn(up[...], act[j]))):
            for p in range(4):
                gm[j, :, :, :, p * 256 + base:p * 256 + base + 128] = spread(g[:, p * 128:(p + 1) * 128])
        for n in range(NH):
            pl.when(j == n)(lambda n=n: (g1(n).start(), None)[1])
        return 0

    loop(0, NH, chunk, 0)

    def ln2b(i, carry):
        s = rows_of(i, SMALL)
        u = up[s, :].astype(F32)
        g = again(o_grad, i)
        normed = n2[s, :]
        inv = inv1[s, 64:65]
        scaled = g * ss
        d = u + inv * (scaled - mean(scaled) - normed * mean(scaled * normed))
        keep(o_grad, i, d)
        hg[s, 0:D] = d.astype(BF16)
        x[s, :] = nn(d.astype(BF16), pt[...]).astype(BF16)
        terms = (d, u, g * normed, g)
        return tuple(a + jnp.sum(t, axis=0, keepdims=True) for a, t in zip(carry, terms))

    zr1 = jnp.zeros((1, D), F32)
    sums = unrolled(0, nsm, ln2b, (zr1,) * 4)
    for r, t in zip((0, 1, 4, 5), sums):
        vec[r:r + 1, :] = t
    sum1(2)
    sum2(0)
    gj = tn(hg[:, 0:D], attn[0:RP, :]).astype(BF16)
    t0, t1, t2 = gj[:, 0:128], gj[:, 128:256], gj[:, 256:384]
    for c, t in enumerate((t0, jnp.where(lane_d < 64, t1, t0), jnp.where(lane_d < 64, t2, t1), t2)):
        gh[0, :, :, :, place(c) * 128:(place(c) + 1) * 128] = spread(t)
    g1(3).start()

    def finish_mlp(j):
        total = sum3(j)
        small[1, :, j * 128:(j + 1) * 128] = total[:, :128]
        small[2, :, j * 128:(j + 1) * 128] = total[:, 128:]

    def finish_projection(_):
        t = pltpu.roll(sum3(3), lax.rem(128 - lax.rem(96 * col_i, 128), 128), 1)
        small[3, :, 0:128] = t

    behind = (
        ((sum1, 3), (sum2, 1)),
        ((sum1, 4), (sum2, 2)),
        ((sum1, 5),),
    )

    for h in range(PAIRS):
        hl = pl.ds(h * 128, 128)

        def attend_back(i, _):
            off, base = window(i)
            qw = pl.ds(base, WIN)
            kk = pl.ds(base, KEYS)
            q = qkv[h, qw, 0:128]
            k = qkv[h, kk, 128:256]
            v = qkv[h, kk, 256:384]
            rid = lax.broadcasted_iota(jnp.int32, (WIN, 128), 0) - off
            mine = (rid >= 0) & (rid < SEQ)
            do = jnp.where(mine, x[qw, hl].astype(F32) * rinv[qw, hl], 0.0)
            dob = do.astype(BF16)
            xx = jnp.concatenate([dob, (do * attn[qw, hl].astype(F32)).astype(BF16)], axis=1)
            ev = even[:WIN]
            zw = zero[:WIN]
            e0 = est[h, i, 0]
            e1 = est[h, i, 1]
            d0 = (e0 * nt(xx, jnp.concatenate([jnp.where(even, v, zero), -ones_e], axis=1))).astype(BF16)
            d1 = (e1 * nt(xx, jnp.concatenate([jnp.where(even, zero, v), -ones_o], axis=1))).astype(BF16)
            dq = (nn(d0, jnp.where(even, k, zero)) + nn(d1, jnp.where(even, zero, k))) * 0.125
            dk = (tn(d0, jnp.where(ev, q, zw)) + tn(d1, jnp.where(ev, zw, q))) * 0.125
            dv = tn(e0, jnp.where(ev, dob, zw)) + tn(e1, jnp.where(ev, zw, dob))
            old = pgr[qw, h * D:(h + 1) * D].astype(F32)
            pgr[qw, h * D:h * D + 128] = jnp.where(mine, dq, old[:, 0:128]).astype(BF16)
            pgr[qw, h * D + 128:h * D + 256] = jnp.where(mine, dk[:WIN], old[:, 128:256]).astype(BF16)
            pgr[qw, h * D + 256:h * D + 384] = jnp.where(mine, dv[:WIN], old[:, 256:384]).astype(BF16)
            return 0

        unrolled(0, images, attend_back, 0)
        do(behind[h])
        gp = tn(rows1[...], pgr[0:RP, h * D:(h + 1) * D])
        for c, j in enumerate(SHARES[h]):
            gh[1 + h, :, :, :, place(c) * 128:(place(c) + 1) * 128] = spread(gp[:, j * 128:(j + 1) * 128])
        if h < PAIRS - 1:
            g1(4 + h).start()
        else:
            for d in list(range(1, PLANE)) + [0]:
                piece1(d).start()
            do(((sum2, 3), (sum2, 4), (finish_mlp, 0), (finish_mlp, 1)))

        def bias_sum(i, carry):
            s = rows_of(i, SMALL)
            return carry + jnp.sum(pgr[s, h * D:(h + 1) * D].astype(F32), axis=0, keepdims=True)

        vec[6 + h:7 + h, :] = unrolled(0, nsm, bias_sum, zr1)

    vq[...] = jnp.zeros(vq.shape, F32)
    for q in range(4):
        for h in range(PAIRS):
            j = SHARES[h][q]
            vq[q, 6 + h:7 + h, :] = vec[6 + h:7 + h, j * 128:(j + 1) * 128]
            vq[q, 9 + h:10 + h, :] = vec[9 + place(q):10 + place(q), h * 128:(h + 1) * 128]

    gbuf = n2

    def ln1b(i, carry):
        s = rows_of(i, SMALL)
        g = nt(pgr[s, :], wp[...])
        gbuf[s, :] = g
        terms = (g * n1[s, :], g)
        hook(i, [(nsm // 2 - 1, lambda: sum1_last(0))])
        return tuple(a + jnp.sum(t, axis=0, keepdims=True) for a, t in zip(carry, terms))

    sums = unrolled(0, nsm, ln1b, (zr1,) * 2)

    for r, t in zip((2, 3), sums):
        vec[r:r + 1, :] = t
    wide_d = D // 4
    for q in range(4):
        vq[q, 0:6, 0:wide_d] = vec[0:6, q * wide_d:(q + 1) * wide_d]
    me = plane * 2 + core

    def v2(d):
        to = vpeer(d)
        return remote(vq.at[to[1]], vr2.at[me], vs.at[0], vs.at[1], to)

    def v3(d):
        return remote(vr3.at[z], vr3.at[z], vs.at[0], vs.at[2], zpeer(d))

    def vector2():
        arrived(vs.at[1], vspan(2 * PLANE - 1))
        total = vr2[0]
        for q in range(1, 2 * PLANE):
            total += vr2[q]
        vr3[z] = total
        for d in range(1, Z):
            v3(d).start()

    for d in range(1, 2 * PLANE):
        v2(d).start()
    vr2[me] = vq[col_i]

    def ln1c(i, _):
        s = rows_of(i, SMALL)
        normed = n1[s, :]
        inv = inv1[s, 0:1]
        scaled = gbuf[s, :] * fs
        keep(o_grad, i, again(o_grad, i) + inv * (scaled - mean(scaled) - normed * mean(scaled * normed)))
        return 0

    unrolled(0, nsm, ln1c, 0)
    def emit(i):
        s = rows_of(i, BIG)
        last = min(rows, (i + 1) * BIG)
        value = acc1[s, :]
        for j in range(NH):
            value += nt(act[j, s, :], rtr[j].reshape(D, HC) if RV == RB else compact(rtr[j]))
        o_out[i * BIG:last, :] = value[:last - i * BIG].astype(BF16)

    do(((sum2, 5),))
    with jax.named_scope("emit"):
        for i in range(nbig):
            emit(i)
            if i == 0:
                do(((sum2, 6),))
            if i == min(1, nbig - 1):
                vector2()
        do(((finish_mlp, 2), (finish_projection, 3)))
    for h in range(PAIRS - 1):
        frame[:, turn(h)] = sum3(4 + h)
    frame[:, turn(PAIRS - 1)] = sum3(3 + PAIRS)
    back = lax.rem(D - 32 * col_i, D)
    small[0] = pltpu.roll(frame[...], back, 1)
    with jax.named_scope("vec3"):
        arrived(vs.at[2], vspan(Z - 1))
    total = vr3[0]
    for q in range(1, Z):
        total += vr3[q]
    small[3, 0:8, 128:256] = total[0:8]
    for h in range(PAIRS):
        frame[0:1, turn(h)] = total[6 + h:7 + h]
        small[4, 8:9, h * 128:(h + 1) * 128] = total[9 + h:10 + h]
    small[4, 0:8, :] = pltpu.roll(frame[0:8, :], back, 1)

    with jax.named_scope("ends"):
        for k in range(len(chunks)):
            left(asend.at[k], span(ALL))
        left(bs.at[0], n1.at[0:8 * (2 * Y - 1)])
        for k in range(7):
            left(gsend.at[k], span(ALL * (width(k) // 128)))
        left(vs.at[0], vspan(2 * PLANE + Z - 2))


def finish_kernel(*refs):
    out, grad, small = refs[:3]
    outs, stage, sem = refs[3:17], refs[17:29], refs[29]
    moves = [pltpu.make_async_copy(a, b, sem.at[k]) for k, (a, b) in enumerate(zip((grad, out) + stage, (outs[1], outs[0]) + outs[2:]))]
    moves[0].start()
    moves[1].start()
    rv, wide = stage[0].shape
    stage[0][...] = small[0, :rv, :wide]
    stage[1][...] = small[3, :rv, :stage[1].shape[1]]
    stage[2][...] = small[1, :rv, :]
    stage[3][...] = small[2, :rv, :]
    stage[4][...] = small[4, 0:1, :wide].reshape(wide)
    stage[6][...] = small[4, 8:9, :].reshape(D)
    for r, k in enumerate((5, 7, 8, 9, 10, 11)):
        n = stage[k].shape[0]
        stage[k][...] = small[3, r:r + 1, 128:128 + n].reshape(n)
    for move in moves[2:]:
        move.start()
    for move in moves:
        move.wait()


def body(dps, cols, tokens, packed, packed_bias, projection, projection_bias, expansion, expansion_bias, reduction,
         reduction_bias, first_scale, first_shift, second_scale, second_shift, upstream):
    args = (tokens, packed, packed_bias, projection.T, projection_bias, expansion, expansion_bias, reduction.T,
            reduction_bias, first_scale, first_shift, second_scale, second_shift, upstream)
    rows = tokens.shape[0]
    images = rows // SEQ
    Z = min(4, dps)
    PD = dps // Z
    Y = cols // 2
    RV = packed.shape[0]
    RB = -(-RV // 16) * 16
    PLANE = PD * Y
    RP = -(-rows // BIG) * BIG
    reach = ((images - 1) * SEQ) // 16 * 16
    XQ = max(RP + 16, reach + WIN)
    XP = max(RP + 16, reach + KEYS)
    cfg = (Z, PD, Y, RB, RV, rows)
    V = pl.BlockSpec(memory_space=pltpu.VMEM)
    A = pl.BlockSpec(memory_space=pl.ANY)
    S = jax.ShapeDtypeStruct
    vm = pltpu.VMEM
    dma = pltpu.SemaphoreType.DMA
    NH = FF // HC
    NC = PAIRS + 1 + 2 * NH
    small = RV != RB
    outs = (
        S((rows, D), BF16), S((rows, D), F32),
        S(packed.shape, F32), S(projection.shape[::-1], F32), S(expansion.shape, F32), S(reduction.shape[::-1], F32),
        S(packed_bias.shape, F32), S((D // cols,), F32), S(expansion_bias.shape, F32),
    ) + (S((D // cols,), F32),) * 5
    narrow = (args[1], args[2], args[3], args[4], args[5], args[6], args[7]) + args[8:13]
    scratch = [vm(a.shape, a.dtype) for a in narrow] + [
        vm((XQ, D), BF16), vm((RP, D), BF16),
        vm((RP, D), F32), vm((RP, D), BF16),
        vm((PAIRS, XP, D), BF16), vm((XQ, D), BF16),
        vm((PAIRS, images, 2, WIN, KEYS), BF16), vm((XQ, D), F32),
        vm((RP, D), F32), vm((RP, D), F32),
        vm((NH, RP, HC), BF16), vm((RP, HC), BF16),
        vm((XQ, PAIRS * D), BF16), vm((max(RP, (Z - 1 + (2 * PLANE - 1) * Z) * RB), 128), F32),
        vm((PAIRS, Z, PD, RB, 4 * 128), BF16), vm((Z, PD, RB, 4 * 128), BF16),
        vm((NH, Z, PD, RB, HC), BF16), vm((NH, Z, PD, RB, HC), BF16),
        vm((D, PAIRS * D), BF16), vm((D, D), BF16),
        vm((D, HC) if small else (16, 128), BF16), vm((D, HC) if small else (16, 128), BF16),
        vm((4, 8, D), F32),
        vm((NH, Z, PD, RB, 4 * 256), BF16), vm((4, Z, PD, RB, 4 * 128), BF16),
        vm((NH, Z, PD, RB, Y * 256), BF16), vm((NH, PLANE - 1, Z, RB, 256), BF16), vm((NH, Z, RB, 256), BF16),
        vm((4, Z, PD, RB, Y * 128), BF16), vm((4, PLANE - 1, Z, RB, 128), BF16), vm((4, Z, RB, 128), BF16),
        vm((NH, Z, PD, RB, Y * 256), BF16), vm((NH, Z, RB, 256), BF16),
        vm((4, Z, PD, RB, Y * 128), BF16), vm((4, Z, RB, 128), BF16),
        vm((RB, D), F32), vm((16, D), F32),
        vm((4, 16, 128), F32), vm((2 * PLANE, 16, 128), F32), vm((Z, 16, 128), F32),
        dma((NC,)), dma((Z,)), dma((PLANE - 1,)), dma((NC,)), dma((NC,)), dma((NC,)),
        dma((2,)), dma((7,)), dma((7,)), dma((7,)), dma((7,)), dma((PLANE,)), dma((3,)),
    ]
    got = pl.pallas_call(
        functools.partial(layer_kernel, cfg),
        out_shape=(vm((rows, D), BF16), vm((rows, D), F32), vm((5, RB, D), F32)),
        in_specs=[A] * 14,
        out_specs=(V,) * 3,
        scratch_shapes=scratch,
        compiler_params=pltpu.CompilerParams(vmem_limit_bytes=VMEM - rows * D * 6 - 5 * RB * D * 4 - 65536, collective_id=0, has_side_effects=True),
    )(*args)
    got = pl.pallas_call(
        finish_kernel,
        out_shape=outs,
        in_specs=[V] * 3,
        out_specs=(A,) * 14,
        scratch_shapes=[vm(o.shape, o.dtype) for o in outs[2:]] + [dma((14,))],
        compiler_params=pltpu.CompilerParams(vmem_limit_bytes=2 * 1024 * 1024),
    )(*(pltpu.with_memory_space_constraint(v, pltpu.VMEM) for v in got))
    return got[:3] + (got[3].T, got[4], got[5].T) + tuple(got[6:])


def solution(mesh):
    placed = (
        P(("dp", "col"), None), P("dp", "col"), P("col"), P("col", "dp"), P(), P("dp", "col"), P("col"),
        P("col", "dp"), P(), P(), P(), P(), P(), P(("dp", "col"), None),
    )
    return jax.shard_map(
        functools.partial(body, mesh.shape["dp"], mesh.shape["col"]),
        mesh=mesh,
        in_specs=placed,
        out_specs=(
            P(("dp", "col"), None), P(("dp", "col"), None),
            P("dp", "col"), P("col", "dp"), P("dp", "col"), P("col", "dp"),
        ) + (P("col"),) * 8,
        check_vma=False,
    )
```

```python
import functools

import jax
import jax.numpy as jnp
from jax import lax
from jax.experimental import pallas as pl
from jax.experimental.pallas import tpu as pltpu
from jax.sharding import PartitionSpec as P

SEQ = 197
EPS = 1e-06
ROOT_HALF = 0.7071067811865476
INV_ROOT_TAU = 0.3989422804014327
F32, BF16 = jnp.float32, jnp.bfloat16
MESH = pl.DeviceIdType.MESH
D = 384
FF = 1536
PAIRS = 3
WIN = 224
KEYS = 256
BIG = 528
SMALL = 176
HC = 512
VMEM = 67_000_000


def nn(a, b):
    return lax.dot_general(a, b, (((1,), (0,)), ((), ())), preferred_element_type=F32)


def nt(a, b):
    return lax.dot_general(a, b, (((1,), (1,)), ((), ())), preferred_element_type=F32)


def tn(a, b):
    return lax.dot_general(a, b, (((0,), (0,)), ((), ())), preferred_element_type=F32)


def rows_of(i, size):
    if isinstance(i, int):
        return pl.ds(i * size, size)
    return pl.ds(pl.multiple_of(i * size, 16), size)


def lanes_of(i, size):
    return pl.ds(pl.multiple_of(i * size, 128), size)


def mean(x):
    return jnp.sum(x, axis=1, keepdims=True) * (1.0 / x.shape[1])


def hook(i, steps):
    for at, step in steps:
        if isinstance(i, int):
            if i == at:
                step()
        else:
            pl.when(i == at)(lambda step=step: (step(), None)[1])


def unrolled(lo, hi, function, init):
    with jax.named_scope(function.__name__):
        for i in range(lo, hi):
            init = function(i, init)
    return init


def loop(lo, hi, function, init):
    with jax.named_scope(function.__name__):
        return lax.fori_loop(lo, hi, function, init)


def named(function):
    def inner(*a):
        with jax.named_scope(function.__name__ + "_".join(str(v) for v in a if isinstance(v, int))):
            return function(*a)
    return inner


TILES = (
    ((0, 0, 128), (1, 1, 128), (2, 3, 96)),
    ((0, 0, 128), (1, 2, 64), (3, 3, 128)),
    ((0, 1, 32), (2, 2, 128), (3, 3, 128)),
)
SHARES = ((0, 1, 2, 2), (0, 1, 1, 2), (0, 0, 1, 2))


def layer_kernel(cfg, *refs):
    Z, PD, Y, RB, RV, rows = cfg
    PLANE = PD * Y
    RP = -(-rows // BIG) * BIG
    images = rows // SEQ
    nsm, nbig = RP // SMALL, RP // BIG
    tokens, upstream, outside = refs[0], refs[13], refs[1:13]
    o_out, o_grad, small, refs = refs[14], refs[15], refs[16], refs[17:]
    (packed, packed_bias, projection, projection_bias, expansion, expansion_bias, reduction,
     reduction_bias, first_scale, first_shift, second_scale, second_shift,
     x, up, n1, rows1, qkv, attn, est, rinv, n2, acc1, act, hg, pgr, inv1,
     wpk, ptr, exr, rtr, wp, pt, exc, rtc, bias,
     gm, gh, rm1, rm2, rm3, rh1, rh2, rh3, sm1, sm2, sh1, sh2, frame, vec, vq, vr2, vr3,
     asend, zfirst, pfirst, zr, pr, kr, bs, gsend, g1r, g2r, g3r, glast, vs) = refs

    dp_i, col_i = lax.axis_index("dp"), lax.axis_index("col")
    z, pd = dp_i // PD, lax.rem(dp_i, PD)
    y, core = col_i // 2, lax.rem(col_i, 2)
    pos = core * Y + y
    plane = pd * Y + y

    def device(zz, pp, yy, cc):
        return (zz * PD + pp, yy * 2 + cc)

    def znear(s):
        rising = jnp.where(s < z, s, s + 1)
        down = Z - 1 - s
        falling = jnp.where(down > z, down, down - 1)
        return jnp.where(2 * z < Z, rising, falling)

    def zpeer(s):
        return device(znear(s - 1), pd, y, core)

    def pplace(d):
        return lax.rem(pd + d // Y, PD), lax.rem(y + d % Y, Y)

    def psource(d):
        return lax.rem(pd + PD - d // Y, PD), lax.rem(y + Y - d % Y, Y)

    def ppeer(d):
        pp, yy = pplace(d)
        return device(z, pp, yy, core)

    def vpeer(d):
        pp, yy = pplace(d // 2)
        return device(z, pp, yy, lax.rem(core + d % 2, 2))

    sibling = device(z, pd, y, 1 - core)

    def cpeer(d):
        return (dp_i, lax.rem(col_i + d, 2 * Y))

    def remote(src, dst, send, recv, to):
        return pltpu.make_async_remote_copy(
            src_ref=src, dst_ref=dst, send_sem=send, recv_sem=recv, device_id=to, device_id_type=MESH)

    barrier = pltpu.get_barrier_semaphore()
    near = [zpeer(d) for d in range(1, Z)] + [vpeer(d) for d in range(1, 2 * PLANE)]
    for to in near:
        pl.semaphore_signal(barrier, inc=1, device_id=to, device_id_type=MESH)
    greeted = len(near)

    cin = pltpu.make_async_copy(tokens, x.at[pl.ds(0, rows)], gsend.at[5])
    cup = pltpu.make_async_copy(upstream, up.at[pl.ds(0, rows)], gsend.at[6])
    inside = (packed, packed_bias, projection, projection_bias, expansion, expansion_bias, reduction,
              reduction_bias, first_scale, first_shift, second_scale, second_shift)
    loads = [pltpu.make_async_copy(a, b, asend.at[n] if n < 8 else gsend.at[n - 8]) for n, (a, b) in enumerate(zip(outside, inside))]
    for n in (0, 2, 4, 6, 1, 5, 3, 7, 8, 9, 10, 11):
        loads[n].start()
    cin.start()
    cup.start()
    loads[0].wait()

    def padded(v):
        return v if RV == RB else jnp.concatenate([v, jnp.zeros((RB - RV, v.shape[1]), v.dtype)], axis=0)

    own = padded(packed[...].astype(F32))
    own = jnp.concatenate([own, jnp.zeros((RB, D - own.shape[1]), F32)], axis=1)
    frame[...] = pltpu.roll(own, 32 * col_i, 1)

    def turn(h):
        return lanes_of(lax.rem(h + col_i, 3), 128)

    for h in range(PAIRS):
        wpk[h, z, pd, :, lanes_of(pos, 128)] = frame[:, turn(h)].astype(BF16)
    chunks = [wpk.at[h] for h in range(PAIRS)] + [ptr]
    for j in range(FF // HC):
        chunks += [exr.at[j], rtr.at[j]]
    mine_l = lanes_of(pos, 128)

    def span(slots):
        return inv1.at[0:slots * RB // 2]

    def vspan(count):
        return inv1.at[0:count * 16]

    def arrived(sem, ref):
        remote(ref, ref, vs.at[0], sem, sibling).wait_recv()

    def left(sem, ref):
        remote(ref, ref, sem, vs.at[0], sibling).wait_send()

    def zcopy(k, d):
        slot = chunks[k].at[z, pd, :, mine_l]
        return remote(slot, slot, asend.at[k], zfirst.at[z] if k == 0 else zr.at[k], zpeer(d))

    def pcopy(k, d):
        slot = chunks[k].at[:, pd, :, mine_l]
        return remote(slot, slot, asend.at[k], pr.at[k], ppeer(d))

    def qcopy(d, q):
        slot = chunks[0].at[q, pd, :, mine_l]
        return remote(slot, slot, asend.at[0], pfirst.at[d - 1], ppeer(d))

    def scopy(q):
        slot = chunks[0].at[q, pd, :, mine_l]
        return remote(slot, slot, asend.at[0], kr.at[0], sibling)

    def scopy_from(d):
        pp, yy = psource(d)
        slot = chunks[0].at[:, pp, :, lanes_of(core * Y + yy, 128)]
        return remote(slot, slot, asend.at[0], kr.at[0], sibling)

    def kcopy(k):
        slot = chunks[k].at[:, :, :, lanes_of(core, Y * 128)]
        return remote(slot, slot, asend.at[k], kr.at[k], sibling)

    def bcopy(d):
        return remote(bias.at[pos], bias.at[pos], bs.at[0], bs.at[1], cpeer(d))

    @named
    def to_plane(k):
        arrived(zr.at[k], span(Z - 1))
        for d in range(PLANE - 1, 0, -1):
            pcopy(k, d).start()

    @named
    def to_sibling(k):
        arrived(pr.at[k], span((PLANE - 1) * Z))
        kcopy(k).start()

    ALL = Z - 1 + (PLANE - 1) * Z + PLANE * Z

    with jax.named_scope("barrier"):
        pl.semaphore_wait(barrier, greeted)
    def to_z(k):
        for d in range(Z - 1, 0, -1):
            zcopy(k, d).start()

    to_z(0)
    for d in range(PLANE - 1, 0, -1):
        qcopy(d, z).start()
    scopy(z).start()
    for load in loads[1:]:
        load.wait()
    own = padded(projection[...].astype(F32))
    own = jnp.concatenate([own, jnp.zeros((RB, 128 - own.shape[1]), F32)], axis=1)
    ptr[z, pd, :, lanes_of(pos, 128)] = pltpu.roll(own, lax.rem(96 * col_i, 128), 1).astype(BF16)
    for j in range(FF // HC):
        exr[j, z, pd, :, lanes_of(pos, 128)] = padded(expansion[:, j * 128:(j + 1) * 128])
        rtr[j, z, pd, :, lanes_of(pos, 128)] = padded(reduction[:, j * 128:(j + 1) * 128])
    vrow = jnp.concatenate([packed_bias[...].reshape(1, -1), jnp.zeros((1, D - packed_bias.shape[0]), F32)], axis=1)
    vrow = pltpu.roll(jnp.broadcast_to(vrow, (8, D)), 32 * col_i, 1)
    bias[pos] = jnp.concatenate([vrow[:4], jnp.broadcast_to(expansion_bias[...].reshape(1, -1), (4, D))], axis=0)

    for d in range(1, 2 * Y):
        bcopy(d).start()

    x[rows:, :] = jnp.zeros((x.shape[0] - rows, D), BF16)
    up[rows:, :] = jnp.zeros((RP - rows, D), BF16)
    for h in range(PAIRS):
        qkv[h, RP:, :] = jnp.zeros((qkv.shape[1] - RP, D), BF16)
    tail = attn.shape[0] - RP + 16
    attn[RP - 16:, :] = jnp.zeros((tail, D), BF16)
    rinv[RP - 16:, :] = jnp.zeros((tail, D), F32)
    pgr[RP - 16:, :] = jnp.zeros((tail, PAIRS * D), BF16)
    fs = first_scale[...].reshape(1, D)
    fh = first_shift[...].reshape(1, D)
    ss = second_scale[...].reshape(1, D)
    sh = second_shift[...].reshape(1, D)
    prb = projection_bias[...].reshape(1, D)
    rdb = reduction_bias[...].reshape(1, D)
    cin.wait()
    cup.wait()

    def ln1(i, _):
        s = rows_of(i, SMALL)
        v = x[s, :].astype(F32)
        avg = mean(v)
        inv = lax.rsqrt(mean(v * v) - avg * avg + EPS)
        normed = (v - avg) * inv
        n1[s, :] = normed
        inv1[s, 0:64] = jnp.broadcast_to(inv, (SMALL, 64))
        rows1[s, :] = (normed * fs + fh).astype(BF16)
        return 0

    @named
    def pass_on(d):
        q = znear(d - 1)
        arrived(zfirst.at[q], chunks[0].at[q, pd, :, mine_l])
        for e in range(PLANE - 1, 0, -1):
            qcopy(e, q).start()
        scopy(q).start()

    loop(0, nsm, ln1, 0)
    for k in (1, 2, 3):
        to_z(k)
    for d in range(1, Z):
        pass_on(d)
    for k in range(4, len(chunks)):
        to_z(k)
    with jax.named_scope("plane0"):
        for d in range(1, PLANE):
            if d == PLANE - 1:
                to_plane(1)
            arrived(pfirst.at[d - 1], span(Z))
            scopy_from(d).start()
    to_plane(2)
    arrived(bs.at[1], n1.at[0:8 * (2 * Y - 1)])

    lane = lax.broadcasted_iota(jnp.int32, (KEYS, 128), 1)
    even = lane < 64
    zero = jnp.zeros((KEYS, 128), BF16)
    one = jnp.ones((KEYS, 128), BF16)
    ones_e = jnp.where(even, one, zero)
    ones_o = jnp.where(even, zero, one)

    def place(c):
        return (c % 2) * Y + c // 2

    if RV != RB:
        wide = Z * PD * RB
        r_ = lax.broadcasted_iota(jnp.int32, (D, wide), 0)
        c_ = lax.broadcasted_iota(jnp.int32, (D, wide), 1)
        pick = jnp.where(c_ == (r_ // RV) * RB + lax.rem(r_, RV), 1.0, 0.0).astype(BF16)

    def compact(v):
        v = v.reshape(Z * PD * RB, v.shape[-1])
        return v if RV == RB else nn(pick, v).astype(BF16)

    def spread(v):
        v = v.astype(BF16)
        v = v if RV == RB else tn(pick, v).astype(BF16)
        return v.reshape(Z, PD, RB, v.shape[-1])

    def merged(tile, first, second, upto):
        if first == second:
            return tile(first)
        a, b = tile(first), tile(second)
        return jnp.where(lax.broadcasted_iota(jnp.int32, a.shape, 1) < upto, a, b)

    @named
    def assemble(h):
        kcopy(h).wait_recv()
        for j, (first, second, upto) in enumerate(TILES[h]):
            wp[:, h * D + j * 128:h * D + (j + 1) * 128] = merged(
                lambda c: compact(wpk[h, :, :, :, place(c) * 128:(place(c) + 1) * 128]), first, second, upto)

    def bias_of(h):
        def tile(c):
            t = (h + c) % 3
            return bias[place(c), 0:1, t * 128:(t + 1) * 128]
        return jnp.concatenate([merged(tile, *t) for t in TILES[h]], axis=1)

    def keep(ref, i, value):
        last = min(rows, (i + 1) * SMALL)
        ref[i * SMALL:last, :] = value[:last - i * SMALL]

    def again(ref, i):
        last = min(rows, (i + 1) * SMALL)
        value = ref[i * SMALL:last, :]
        more = (i + 1) * SMALL - last
        return value if not more else jnp.concatenate([value, jnp.zeros((more, D), value.dtype)], axis=0)

    def window(i):
        first = i * SEQ
        base = (first // 16) * 16
        return first - base, base if isinstance(i, int) else pl.multiple_of(base, 16)

    before = ((to_plane, 3), (to_plane, 4), (to_sibling, 1)), ((to_plane, 7),), ((to_plane, 8), (to_plane, 9), (to_sibling, 3), (to_sibling, 4))
    after = (
        ((to_plane, 5), (to_sibling, 2), (to_plane, 6)),
        (),
        ((to_sibling, 5),),
    )

    def do(steps):
        for step, k in steps:
            step(k)

    for h in range(PAIRS):
        hl = pl.ds(h * 128, 128)
        if h < 2:
            both = (0,) if h == 0 else tuple(range(1, PAIRS))
            for g in both:
                assemble(g)
            pb = jnp.concatenate([bias_of(g) for g in both], axis=1)

            def project(i, _):
                s = rows_of(i, BIG)
                v = (nn(rows1[s, :], wp[:, both[0] * D:(both[-1] + 1) * D]) + pb).astype(BF16)
                for n, g in enumerate(both):
                    qkv[g, s, :] = v[:, n * D:(n + 1) * D]
                return 0

            loop(0, nbig, project, 0)

        def attend(i, _):
            off, base = window(i)
            qw = pl.ds(base, WIN)
            kk = pl.ds(base, KEYS)
            q = qkv[h, qw, 0:128]
            k = qkv[h, kk, 128:256]
            v = qkv[h, kk, 256:384]
            col = lax.broadcasted_iota(jnp.int32, (WIN, KEYS), 1) - off
            ok = (col >= 0) & (col < SEQ)
            es = []
            for m in (even, ~even):
                s = nt(q, jnp.where(m, k, zero))
                s = jnp.where(ok, s, -1e30)
                top = jnp.max(s, axis=1, keepdims=True)
                es.append(jnp.exp((s - top) * 0.125).astype(BF16))
            est[h, i, 0] = es[0]
            est[h, i, 1] = es[1]
            mix = nn(es[0], jnp.concatenate([jnp.where(even, v, zero), ones_e], axis=1)) + nn(
                es[1], jnp.concatenate([jnp.where(even, zero, v), ones_o], axis=1))
            r = 1.0 / mix[:, 128:]
            o = mix[:, :128] * r
            rid = lax.broadcasted_iota(jnp.int32, (WIN, 128), 0) - off
            mine = (rid >= 0) & (rid < SEQ)
            attn[qw, hl] = jnp.where(mine, o, attn[qw, hl].astype(F32)).astype(BF16)
            rinv[qw, hl] = jnp.where(mine, r, rinv[qw, hl])
            return 0

        do(before[h])
        unrolled(0, images, attend, 0)
        do(after[h])

    kcopy(3).wait_recv()
    lane_d = lax.broadcasted_iota(jnp.int32, (D, 128), 1)
    tiles = [compact(ptr[:, :, :, place(c) * 128:(place(c) + 1) * 128]) for c in range(4)]
    pt[:, 0:128] = jnp.where(lane_d < 96, tiles[0], tiles[1])
    pt[:, 128:256] = jnp.where(lane_d < 64, tiles[1], tiles[2])
    pt[:, 256:384] = jnp.where(lane_d < 32, tiles[2], tiles[3])
    def exb_of(j):
        return jnp.concatenate([bias[p, 4:5, j * 128:(j + 1) * 128] for p in range(4)], axis=1)


    def ln2(i, _):
        s = rows_of(i, SMALL)
        v = x[s, :].astype(F32) + nt(attn[s, :], pt[...]) + prb
        avg = mean(v)
        inv = lax.rsqrt(mean(v * v) - avg * avg + EPS)
        normed = (v - avg) * inv
        acc1[s, :] = v + rdb
        n2[s, :] = normed
        inv1[s, 64:128] = jnp.broadcast_to(inv, (SMALL, 64))
        x[s, :] = (normed * ss + sh).astype(BF16)
        keep(o_grad, i, jnp.zeros((SMALL, D), F32))
        return 0

    unrolled(0, nsm, ln2, 0)

    def part(big, small, k):
        return big.at[k] if k < PAIRS else small.at[k - PAIRS]

    def width(k):
        return 256 if k < PAIRS else 128

    def g1(k):
        half = Y * width(k)
        return remote(part(gm, gh, k).at[:, :, :, lanes_of(1 - core, half)], part(rm1, rh1, k),
                      gsend.at[k], g1r.at[k], sibling)

    def g2(k, d):
        pp, yy = pplace(d)
        return remote(part(sm1, sh1, k).at[:, pp, :, lanes_of(yy, width(k))], part(rm2, rh2, k).at[d - 1],
                      gsend.at[k], g2r.at[k], ppeer(d))

    def g3(k, d):
        return remote(part(sm2, sh2, k).at[znear(d - 1)], part(rm3, rh3, k).at[z], gsend.at[k], g3r.at[k], zpeer(d))

    @named
    def sum1(k):
        g1(k).wait_recv()
        own = part(gm, gh, k)[:, :, :, lanes_of(core, Y * width(k))]
        part(sm1, sh1, k)[...] = (own.astype(F32) + part(rm1, rh1, k)[...].astype(F32)).astype(BF16)
        for d in range(PLANE - 1, 0, -1):
            g2(k, d).start()

    LAST = 3 + PAIRS

    def piece1(d):
        pp, yy = pplace(d)
        return remote(gh.at[PAIRS, :, pp, :, lanes_of((1 - core) * Y + yy, 128)],
                      rh1.at[PAIRS, :, pp, :, lanes_of(yy, 128)], gsend.at[LAST], glast.at[d], sibling)

    def piece_sum(d):
        pp, yy = pplace(d)
        piece1(d).wait_recv()
        own = gh[PAIRS, :, pp, :, lanes_of(core * Y + yy, 128)]
        got = rh1[PAIRS, :, pp, :, lanes_of(yy, 128)]
        sh1[PAIRS, :, pp, :, lanes_of(yy, 128)] = (own.astype(F32) + got.astype(F32)).astype(BF16)
        if d:
            g2(LAST, d).start()

    @named
    def sum1_last(_):
        for d in range(PLANE - 1, -1, -1):
            piece_sum(d)

    @named
    def sum2(k):
        arrived(g2r.at[k], span((PLANE - 1) * Z * (width(k) // 128)))
        total = part(sm1, sh1, k)[:, pd, :, lanes_of(y, width(k))].astype(F32)
        for d in range(1, PLANE):
            total += part(rm2, rh2, k)[d - 1].astype(F32)
        part(sm2, sh2, k)[...] = total.astype(BF16)
        for d in range(Z - 1, 0, -1):
            g3(k, d).start()

    @named
    def sum3(k):
        arrived(g3r.at[k], span((Z - 1) * (width(k) // 128)))
        total = part(sm2, sh2, k)[z].astype(F32)
        for d in range(1, Z):
            total += part(rm3, rh3, k)[znear(d - 1)].astype(F32)
        return total

    vec[...] = jnp.zeros(vec.shape, F32)
    spot = (
        ((to_sibling, 6), (to_sibling, 7)),
        ((to_sibling, 8), (to_sibling, 9), (sum1, 0)),
        ((sum1, 1),),
    )
    NH = FF // HC
    mlp_in = [((kcopy, 4 + 2 * j), (kcopy, 5 + 2 * j)) for j in range(NH)]

    def chunk(j, _):
        for n in range(NH):
            pl.when(j == n)(lambda n=n: (kcopy(4 + 2 * n).wait_recv(), kcopy(5 + 2 * n).wait_recv(), None)[2])
        if RV != RB:
            exc[...] = compact(exr[j])
            rtc[...] = compact(rtr[j])

        def ex_of():
            return exc[...] if RV != RB else exr[j].reshape(D, HC)

        def rt_of():
            return rtc[...] if RV != RB else rtr[j].reshape(D, HC)

        tile = lanes_of(j, 128)
        exb = jnp.concatenate([bias[p, 4:5, tile] for p in range(4)], axis=1)
        bsum = jnp.zeros((1, HC), F32)
        for i in range(nbig):
            s = rows_of(i, BIG)
            pre = nn(x[s, :], ex_of()) + exb
            ug = nn(up[s, :], rt_of())
            cdf = 0.5 + 0.5 * lax.erf(pre * ROOT_HALF)
            act[j, s, :] = (pre * cdf).astype(BF16)
            g = ug * (cdf + pre * (jnp.exp(pre * pre * -0.5) * INV_ROOT_TAU))
            hg[s, :] = g.astype(BF16)
            last = min(rows, (i + 1) * BIG)
            back = nt(hg[s, :], ex_of())
            o_grad[i * BIG:last, :] += back[:last - i * BIG]
            bsum += jnp.sum(g, axis=0, keepdims=True)
        for p in range(4):
            vec[9 + p:10 + p, tile] = bsum[:, p * 128:(p + 1) * 128]
        for n in range(NH):
            pl.when(j == n)(lambda n=n: do(spot[n]))
        for base, g in ((0, tn(x[0:RP, :], hg[...])), (128, tn(up[...], act[j]))):
            for p in range(4):
                gm[j, :, :, :, p * 256 + base:p * 256 + base + 128] = spread(g[:, p * 128:(p + 1) * 128])
        for n in range(NH):
            pl.when(j == n)(lambda n=n: (g1(n).start(), None)[1])
        return 0

    loop(0, NH, chunk, 0)

    def ln2b(i, carry):
        s = rows_of(i, SMALL)
        u = up[s, :].astype(F32)
        g = again(o_grad, i)
        normed = n2[s, :]
        inv = inv1[s, 64:65]
        scaled = g * ss
        d = u + inv * (scaled - mean(scaled) - normed * mean(scaled * normed))
        keep(o_grad, i, d)
        hg[s, 0:D] = d.astype(BF16)
        x[s, :] = nn(d.astype(BF16), pt[...]).astype(BF16)
        terms = (d, u, g * normed, g)
        return tuple(a + jnp.sum(t, axis=0, keepdims=True) for a, t in zip(carry, terms))

    zr1 = jnp.zeros((1, D), F32)
    sums = unrolled(0, nsm, ln2b, (zr1,) * 4)
    for r, t in zip((0, 1, 4, 5), sums):
        vec[r:r + 1, :] = t
    sum1(2)
    sum2(0)
    gj = tn(hg[:, 0:D], attn[0:RP, :]).astype(BF16)
    t0, t1, t2 = gj[:, 0:128], gj[:, 128:256], gj[:, 256:384]
    for c, t in enumerate((t0, jnp.where(lane_d < 64, t1, t0), jnp.where(lane_d < 64, t2, t1), t2)):
        gh[0, :, :, :, place(c) * 128:(place(c) + 1) * 128] = spread(t)
    g1(3).start()

    def finish_mlp(j):
        total = sum3(j)
        small[1, :, j * 128:(j + 1) * 128] = total[:, :128]
        small[2, :, j * 128:(j + 1) * 128] = total[:, 128:]

    def finish_projection(_):
        t = pltpu.roll(sum3(3), lax.rem(128 - lax.rem(96 * col_i, 128), 128), 1)
        small[3, :, 0:128] = t

    behind = (
        ((sum1, 3), (sum2, 1)),
        ((sum1, 4), (sum2, 2)),
        ((sum1, 5),),
    )

    for h in range(PAIRS):
        hl = pl.ds(h * 128, 128)

        def attend_back(i, _):
            off, base = window(i)
            qw = pl.ds(base, WIN)
            kk = pl.ds(base, KEYS)
            q = qkv[h, qw, 0:128]
            k = qkv[h, kk, 128:256]
            v = qkv[h, kk, 256:384]
            rid = lax.broadcasted_iota(jnp.int32, (WIN, 128), 0) - off
            mine = (rid >= 0) & (rid < SEQ)
            do = jnp.where(mine, x[qw, hl].astype(F32) * rinv[qw, hl], 0.0)
            dob = do.astype(BF16)
            xx = jnp.concatenate([dob, (do * attn[qw, hl].astype(F32)).astype(BF16)], axis=1)
            ev = even[:WIN]
            zw = zero[:WIN]
            e0 = est[h, i, 0]
            e1 = est[h, i, 1]
            d0 = (e0 * nt(xx, jnp.concatenate([jnp.where(even, v, zero), -ones_e], axis=1))).astype(BF16)
            d1 = (e1 * nt(xx, jnp.concatenate([jnp.where(even, zero, v), -ones_o], axis=1))).astype(BF16)
            dq = (nn(d0, jnp.where(even, k, zero)) + nn(d1, jnp.where(even, zero, k))) * 0.125
            dk = (tn(d0, jnp.where(ev, q, zw)) + tn(d1, jnp.where(ev, zw, q))) * 0.125
            dv = tn(e0, jnp.where(ev, dob, zw)) + tn(e1, jnp.where(ev, zw, dob))
            old = pgr[qw, h * D:(h + 1) * D].astype(F32)
            pgr[qw, h * D:h * D + 128] = jnp.where(mine, dq, old[:, 0:128]).astype(BF16)
            pgr[qw, h * D + 128:h * D + 256] = jnp.where(mine, dk[:WIN], old[:, 128:256]).astype(BF16)
            pgr[qw, h * D + 256:h * D + 384] = jnp.where(mine, dv[:WIN], old[:, 256:384]).astype(BF16)
            return 0

        unrolled(0, images, attend_back, 0)
        do(behind[h])
        gp = tn(rows1[...], pgr[0:RP, h * D:(h + 1) * D])
        for c, j in enumerate(SHARES[h]):
            gh[1 + h, :, :, :, place(c) * 128:(place(c) + 1) * 128] = spread(gp[:, j * 128:(j + 1) * 128])
        if h < PAIRS - 1:
            g1(4 + h).start()
        else:
            for d in range(PLANE - 1, -1, -1):
                piece1(d).start()
            do(((sum2, 3), (sum2, 4), (finish_mlp, 0), (finish_mlp, 1)))

    def bias_sum(i, carry):
        s = rows_of(i, SMALL)
        return carry + jnp.sum(pgr[s, :].astype(F32), axis=0, keepdims=True)

    bsum = unrolled(0, nsm, bias_sum, jnp.zeros((1, PAIRS * D), F32))
    for h in range(PAIRS):
        vec[6 + h:7 + h, :] = bsum[:, h * D:(h + 1) * D]
    vq[...] = jnp.zeros(vq.shape, F32)
    for q in range(4):
        for h in range(PAIRS):
            j = SHARES[h][q]
            vq[q, 6 + h:7 + h, :] = vec[6 + h:7 + h, j * 128:(j + 1) * 128]
            vq[q, 9 + h:10 + h, :] = vec[9 + place(q):10 + place(q), h * 128:(h + 1) * 128]

    gbuf = n2

    def ln1b(i, carry):
        s = rows_of(i, SMALL)
        g = nt(pgr[s, :], wp[...])
        gbuf[s, :] = g
        terms = (g * n1[s, :], g)
        hook(i, [(nsm // 2 - 2, lambda: sum1_last(0))])
        return tuple(a + jnp.sum(t, axis=0, keepdims=True) for a, t in zip(carry, terms))

    sums = unrolled(0, nsm, ln1b, (zr1,) * 2)

    for r, t in zip((2, 3), sums):
        vec[r:r + 1, :] = t
    wide_d = D // 4
    for q in range(4):
        vq[q, 0:6, 0:wide_d] = vec[0:6, q * wide_d:(q + 1) * wide_d]
    me = plane * 2 + core

    def v2(d):
        to = vpeer(d)
        return remote(vq.at[to[1]], vr2.at[me], vs.at[0], vs.at[1], to)

    def v3(d):
        return remote(vr3.at[z], vr3.at[z], vs.at[0], vs.at[2], zpeer(d))

    def vector2():
        arrived(vs.at[1], vspan(2 * PLANE - 1))
        total = vr2[0]
        for q in range(1, 2 * PLANE):
            total += vr2[q]
        vr3[z] = total
        for d in range(Z - 1, 0, -1):
            v3(d).start()

    for d in range(2 * PLANE - 1, 0, -1):
        v2(d).start()
    vr2[me] = vq[col_i]

    def ln1c(i, _):
        s = rows_of(i, SMALL)
        normed = n1[s, :]
        inv = inv1[s, 0:1]
        scaled = gbuf[s, :] * fs
        keep(o_grad, i, again(o_grad, i) + inv * (scaled - mean(scaled) - normed * mean(scaled * normed)))
        return 0

    unrolled(0, nsm, ln1c, 0)
    def emit(i):
        s = rows_of(i, BIG)
        last = min(rows, (i + 1) * BIG)
        value = acc1[s, :]
        for j in range(NH):
            value += nt(act[j, s, :], rtr[j].reshape(D, HC) if RV == RB else compact(rtr[j]))
        o_out[i * BIG:last, :] = value[:last - i * BIG].astype(BF16)

    do(((sum2, 5),))
    with jax.named_scope("emit"):
        for i in range(nbig):
            emit(i)
            if i == 0:
                do(((sum2, 6),))
            if i == min(1, nbig - 1):
                vector2()
        do(((finish_mlp, 2), (finish_projection, 3)))
    for h in range(PAIRS - 1):
        frame[:, turn(h)] = sum3(4 + h)
    frame[:, turn(PAIRS - 1)] = sum3(3 + PAIRS)
    back = lax.rem(D - 32 * col_i, D)
    small[0] = pltpu.roll(frame[...], back, 1)
    with jax.named_scope("vec3"):
        arrived(vs.at[2], vspan(Z - 1))
    total = vr3[0]
    for q in range(1, Z):
        total += vr3[q]
    small[3, 0:8, 128:256] = total[0:8]
    for h in range(PAIRS):
        frame[0:1, turn(h)] = total[6 + h:7 + h]
        small[4, 8:9, h * 128:(h + 1) * 128] = total[9 + h:10 + h]
    small[4, 0:8, :] = pltpu.roll(frame[0:8, :], back, 1)

    with jax.named_scope("ends"):
        for k in range(len(chunks)):
            left(asend.at[k], span(ALL))
        left(bs.at[0], n1.at[0:8 * (2 * Y - 1)])
        for k in range(7):
            left(gsend.at[k], span(ALL * (width(k) // 128)))
        left(vs.at[0], vspan(2 * PLANE + Z - 2))


def finish_kernel(*refs):
    out, grad, small = refs[:3]
    outs, stage, sem = refs[3:17], refs[17:29], refs[29]
    moves = [pltpu.make_async_copy(a, b, sem.at[k]) for k, (a, b) in enumerate(zip((grad, out) + stage, (outs[1], outs[0]) + outs[2:]))]
    moves[0].start()
    moves[1].start()
    rv, wide = stage[0].shape
    stage[0][...] = small[0, :rv, :wide]
    stage[1][...] = small[3, :rv, :stage[1].shape[1]]
    stage[2][...] = small[1, :rv, :]
    stage[3][...] = small[2, :rv, :]
    stage[4][...] = small[4, 0:1, :wide].reshape(wide)
    stage[6][...] = small[4, 8:9, :].reshape(D)
    for r, k in enumerate((5, 7, 8, 9, 10, 11)):
        n = stage[k].shape[0]
        stage[k][...] = small[3, r:r + 1, 128:128 + n].reshape(n)
    for move in moves[2:]:
        move.start()
    for move in moves:
        move.wait()


def body(dps, cols, tokens, packed, packed_bias, projection, projection_bias, expansion, expansion_bias, reduction,
         reduction_bias, first_scale, first_shift, second_scale, second_shift, upstream):
    args = (tokens, packed, packed_bias, projection.T, projection_bias, expansion, expansion_bias, reduction.T,
            reduction_bias, first_scale, first_shift, second_scale, second_shift, upstream)
    rows = tokens.shape[0]
    images = rows // SEQ
    Z = min(4, dps)
    PD = dps // Z
    Y = cols // 2
    RV = packed.shape[0]
    RB = -(-RV // 16) * 16
    PLANE = PD * Y
    RP = -(-rows // BIG) * BIG
    reach = ((images - 1) * SEQ) // 16 * 16
    XQ = max(RP + 16, reach + WIN)
    XP = max(RP + 16, reach + KEYS)
    cfg = (Z, PD, Y, RB, RV, rows)
    V = pl.BlockSpec(memory_space=pltpu.VMEM)
    A = pl.BlockSpec(memory_space=pl.ANY)
    S = jax.ShapeDtypeStruct
    vm = pltpu.VMEM
    dma = pltpu.SemaphoreType.DMA
    NH = FF // HC
    NC = PAIRS + 1 + 2 * NH
    small = RV != RB
    outs = (
        S((rows, D), BF16), S((rows, D), F32),
        S(packed.shape, F32), S(projection.shape[::-1], F32), S(expansion.shape, F32), S(reduction.shape[::-1], F32),
        S(packed_bias.shape, F32), S((D // cols,), F32), S(expansion_bias.shape, F32),
    ) + (S((D // cols,), F32),) * 5
    narrow = (args[1], args[2], args[3], args[4], args[5], args[6], args[7]) + args[8:13]
    scratch = [vm(a.shape, a.dtype) for a in narrow] + [
        vm((XQ, D), BF16), vm((RP, D), BF16),
        vm((RP, D), F32), vm((RP, D), BF16),
        vm((PAIRS, XP, D), BF16), vm((XQ, D), BF16),
        vm((PAIRS, images, 2, WIN, KEYS), BF16), vm((XQ, D), F32),
        vm((RP, D), F32), vm((RP, D), F32),
        vm((NH, RP, HC), BF16), vm((RP, HC), BF16),
        vm((XQ, PAIRS * D), BF16), vm((max(RP, (Z - 1 + (2 * PLANE - 1) * Z) * RB), 128), F32),
        vm((PAIRS, Z, PD, RB, 4 * 128), BF16), vm((Z, PD, RB, 4 * 128), BF16),
        vm((NH, Z, PD, RB, HC), BF16), vm((NH, Z, PD, RB, HC), BF16),
        vm((D, PAIRS * D), BF16), vm((D, D), BF16),
        vm((D, HC) if small else (16, 128), BF16), vm((D, HC) if small else (16, 128), BF16),
        vm((4, 8, D), F32),
        vm((NH, Z, PD, RB, 4 * 256), BF16), vm((4, Z, PD, RB, 4 * 128), BF16),
        vm((NH, Z, PD, RB, Y * 256), BF16), vm((NH, PLANE - 1, Z, RB, 256), BF16), vm((NH, Z, RB, 256), BF16),
        vm((4, Z, PD, RB, Y * 128), BF16), vm((4, PLANE - 1, Z, RB, 128), BF16), vm((4, Z, RB, 128), BF16),
        vm((NH, Z, PD, RB, Y * 256), BF16), vm((NH, Z, RB, 256), BF16),
        vm((4, Z, PD, RB, Y * 128), BF16), vm((4, Z, RB, 128), BF16),
        vm((RB, D), F32), vm((16, D), F32),
        vm((4, 16, 128), F32), vm((2 * PLANE, 16, 128), F32), vm((Z, 16, 128), F32),
        dma((NC,)), dma((Z,)), dma((PLANE - 1,)), dma((NC,)), dma((NC,)), dma((NC,)),
        dma((2,)), dma((7,)), dma((7,)), dma((7,)), dma((7,)), dma((PLANE,)), dma((3,)),
    ]
    got = pl.pallas_call(
        functools.partial(layer_kernel, cfg),
        out_shape=(vm((rows, D), BF16), vm((rows, D), F32), vm((5, RB, D), F32)),
        in_specs=[A] * 14,
        out_specs=(V,) * 3,
        scratch_shapes=scratch,
        compiler_params=pltpu.CompilerParams(vmem_limit_bytes=VMEM - rows * D * 6 - 5 * RB * D * 4 - 65536, collective_id=0, has_side_effects=True),
    )(*args)
    got = pl.pallas_call(
        finish_kernel,
        out_shape=outs,
        in_specs=[V] * 3,
        out_specs=(A,) * 14,
        scratch_shapes=[vm(o.shape, o.dtype) for o in outs[2:]] + [dma((14,))],
        compiler_params=pltpu.CompilerParams(vmem_limit_bytes=2 * 1024 * 1024),
    )(*(pltpu.with_memory_space_constraint(v, pltpu.VMEM) for v in got))
    return got[:3] + (got[3].T, got[4], got[5].T) + tuple(got[6:])


def solution(mesh):
    placed = (
        P(("dp", "col"), None), P("dp", "col"), P("col"), P("col", "dp"), P(), P("dp", "col"), P("col"),
        P("col", "dp"), P(), P(), P(), P(), P(), P(("dp", "col"), None),
    )
    return jax.shard_map(
        functools.partial(body, mesh.shape["dp"], mesh.shape["col"]),
        mesh=mesh,
        in_specs=placed,
        out_specs=(
            P(("dp", "col"), None), P(("dp", "col"), None),
            P("dp", "col"), P("col", "dp"), P("dp", "col"), P("col", "dp"),
        ) + (P("col"),) * 8,
        check_vma=False,
    )
```

```python
import functools

import jax
import jax.numpy as jnp
from jax import lax
from jax.experimental import pallas as pl
from jax.experimental.pallas import tpu as pltpu
from jax.sharding import PartitionSpec as P

SEQ = 197
EPS = 1e-06
ROOT_HALF = 0.7071067811865476
INV_ROOT_TAU = 0.3989422804014327
F32, BF16 = jnp.float32, jnp.bfloat16
MESH = pl.DeviceIdType.MESH
D = 384
FF = 1536
PAIRS = 3
WIN = 224
KEYS = 256
BIG = 528
SMALL = 176
HC = 512
VMEM = 67_000_000


def nn(a, b):
    return lax.dot_general(a, b, (((1,), (0,)), ((), ())), preferred_element_type=F32)


def nt(a, b):
    return lax.dot_general(a, b, (((1,), (1,)), ((), ())), preferred_element_type=F32)


def tn(a, b):
    return lax.dot_general(a, b, (((0,), (0,)), ((), ())), preferred_element_type=F32)


def rows_of(i, size):
    if isinstance(i, int):
        return pl.ds(i * size, size)
    return pl.ds(pl.multiple_of(i * size, 16), size)


def lanes_of(i, size):
    return pl.ds(pl.multiple_of(i * size, 128), size)


def mean(x):
    return jnp.sum(x, axis=1, keepdims=True) * (1.0 / x.shape[1])


def hook(i, steps):
    for at, step in steps:
        if isinstance(i, int):
            if i == at:
                step()
        else:
            pl.when(i == at)(lambda step=step: (step(), None)[1])


def unrolled(lo, hi, function, init):
    with jax.named_scope(function.__name__):
        for i in range(lo, hi):
            init = function(i, init)
    return init


def loop(lo, hi, function, init):
    with jax.named_scope(function.__name__):
        return lax.fori_loop(lo, hi, function, init)


def named(function):
    def inner(*a):
        with jax.named_scope(function.__name__ + "_".join(str(v) for v in a if isinstance(v, int))):
            return function(*a)
    return inner


TILES = (
    ((0, 0, 128), (1, 1, 128), (2, 3, 96)),
    ((0, 0, 128), (1, 2, 64), (3, 3, 128)),
    ((0, 1, 32), (2, 2, 128), (3, 3, 128)),
)
SHARES = ((0, 1, 2, 2), (0, 1, 1, 2), (0, 0, 1, 2))


def layer_kernel(cfg, *refs):
    Z, PD, Y, RB, RV, rows = cfg
    PLANE = PD * Y
    RP = -(-rows // BIG) * BIG
    images = rows // SEQ
    nsm, nbig = RP // SMALL, RP // BIG
    tokens, upstream, outside = refs[0], refs[13], refs[1:13]
    o_out, o_grad, small, refs = refs[14], refs[15], refs[16], refs[17:]
    (packed, packed_bias, projection, projection_bias, expansion, expansion_bias, reduction,
     reduction_bias, first_scale, first_shift, second_scale, second_shift,
     x, up, n1, rows1, qkv, attn, est, rinv, n2, acc1, act, hg, pgr, inv1,
     wpk, ptr, exr, rtr, wp, pt, exc, rtc, bias,
     gm, gh, rm1, rm2, rm3, rh1, rh2, rh3, sm1, sm2, sh1, sh2, frame, vec, vq, vr2, vr3,
     asend, zfirst, pfirst, zr, pr, kr, bs, gsend, g1r, g2r, g3r, glast, vs) = refs

    dp_i, col_i = lax.axis_index("dp"), lax.axis_index("col")
    z, pd = dp_i // PD, lax.rem(dp_i, PD)
    y, core = col_i // 2, lax.rem(col_i, 2)
    pos = core * Y + y
    plane = pd * Y + y

    def device(zz, pp, yy, cc):
        return (zz * PD + pp, yy * 2 + cc)

    def znear(s):
        rising = jnp.where(s < z, s, s + 1)
        down = Z - 1 - s
        falling = jnp.where(down > z, down, down - 1)
        return jnp.where(2 * z < Z, rising, falling)

    def zpeer(s):
        return device(znear(s - 1), pd, y, core)

    def pplace(d):
        return lax.rem(pd + d // Y, PD), lax.rem(y + d % Y, Y)

    def psource(d):
        return lax.rem(pd + PD - d // Y, PD), lax.rem(y + Y - d % Y, Y)

    def ppeer(d):
        pp, yy = pplace(d)
        return device(z, pp, yy, core)

    def vpeer(d):
        pp, yy = pplace(d // 2)
        return device(z, pp, yy, lax.rem(core + d % 2, 2))

    sibling = device(z, pd, y, 1 - core)

    def cpeer(d):
        return (dp_i, lax.rem(col_i + d, 2 * Y))

    def remote(src, dst, send, recv, to):
        return pltpu.make_async_remote_copy(
            src_ref=src, dst_ref=dst, send_sem=send, recv_sem=recv, device_id=to, device_id_type=MESH)

    barrier = pltpu.get_barrier_semaphore()
    near = [zpeer(d) for d in range(1, Z)] + [vpeer(d) for d in range(1, 2 * PLANE)]
    for to in near:
        pl.semaphore_signal(barrier, inc=1, device_id=to, device_id_type=MESH)
    greeted = len(near)

    cin = pltpu.make_async_copy(tokens, x.at[pl.ds(0, rows)], gsend.at[5])
    cup = pltpu.make_async_copy(upstream, up.at[pl.ds(0, rows)], gsend.at[6])
    inside = (packed, packed_bias, projection, projection_bias, expansion, expansion_bias, reduction,
              reduction_bias, first_scale, first_shift, second_scale, second_shift)
    loads = [pltpu.make_async_copy(a, b, asend.at[n] if n < 8 else gsend.at[n - 8]) for n, (a, b) in enumerate(zip(outside, inside))]
    for n in (0, 2, 4, 6, 1, 5, 3, 7, 8, 9, 10, 11):
        loads[n].start()
    cin.start()
    cup.start()
    loads[0].wait()

    def padded(v):
        return v if RV == RB else jnp.concatenate([v, jnp.zeros((RB - RV, v.shape[1]), v.dtype)], axis=0)

    own = padded(packed[...].astype(F32))
    own = jnp.concatenate([own, jnp.zeros((RB, D - own.shape[1]), F32)], axis=1)
    frame[...] = pltpu.roll(own, 32 * col_i, 1)

    def turn(h):
        return lanes_of(lax.rem(h + col_i, 3), 128)

    for h in range(PAIRS):
        wpk[h, z, pd, :, lanes_of(pos, 128)] = frame[:, turn(h)].astype(BF16)
    chunks = [wpk.at[h] for h in range(PAIRS)] + [ptr]
    for j in range(FF // HC):
        chunks += [exr.at[j], rtr.at[j]]
    mine_l = lanes_of(pos, 128)

    def span(slots):
        return inv1.at[0:slots * RB // 2]

    def vspan(count):
        return inv1.at[0:count * 16]

    def arrived(sem, ref):
        remote(ref, ref, vs.at[0], sem, sibling).wait_recv()

    def left(sem, ref):
        remote(ref, ref, sem, vs.at[0], sibling).wait_send()

    def zcopy(k, d):
        slot = chunks[k].at[z, pd, :, mine_l]
        return remote(slot, slot, asend.at[k], zfirst.at[z] if k == 0 else zr.at[k], zpeer(d))

    def pcopy(k, d):
        slot = chunks[k].at[:, pd, :, mine_l]
        return remote(slot, slot, asend.at[k], pr.at[k], ppeer(d))

    def qcopy(d, q):
        slot = chunks[0].at[q, pd, :, mine_l]
        return remote(slot, slot, asend.at[0], pfirst.at[d - 1], ppeer(d))

    def scopy(q):
        slot = chunks[0].at[q, pd, :, mine_l]
        return remote(slot, slot, asend.at[0], kr.at[0], sibling)

    def scopy_from(d):
        pp, yy = psource(d)
        slot = chunks[0].at[:, pp, :, lanes_of(core * Y + yy, 128)]
        return remote(slot, slot, asend.at[0], kr.at[0], sibling)

    def kcopy(k):
        slot = chunks[k].at[:, :, :, lanes_of(core, Y * 128)]
        return remote(slot, slot, asend.at[k], kr.at[k], sibling)

    def bcopy(d):
        return remote(bias.at[pos], bias.at[pos], bs.at[0], bs.at[1], cpeer(d))

    @named
    def to_plane(k):
        arrived(zr.at[k], span(Z - 1))
        for d in range(PLANE - 1, 0, -1):
            pcopy(k, d).start()

    @named
    def to_sibling(k):
        arrived(pr.at[k], span((PLANE - 1) * Z))
        kcopy(k).start()

    ALL = Z - 1 + (PLANE - 1) * Z + PLANE * Z

    with jax.named_scope("barrier"):
        pl.semaphore_wait(barrier, greeted)
    def to_z(k):
        for d in range(Z - 1, 0, -1):
            zcopy(k, d).start()

    to_z(0)
    for d in range(PLANE - 1, 0, -1):
        qcopy(d, z).start()
    scopy(z).start()
    for load in loads[1:]:
        load.wait()
    own = padded(projection[...].astype(F32))
    own = jnp.concatenate([own, jnp.zeros((RB, 128 - own.shape[1]), F32)], axis=1)
    ptr[z, pd, :, lanes_of(pos, 128)] = pltpu.roll(own, lax.rem(96 * col_i, 128), 1).astype(BF16)
    for j in range(FF // HC):
        exr[j, z, pd, :, lanes_of(pos, 128)] = padded(expansion[:, j * 128:(j + 1) * 128])
        rtr[j, z, pd, :, lanes_of(pos, 128)] = padded(reduction[:, j * 128:(j + 1) * 128])
    vrow = jnp.concatenate([packed_bias[...].reshape(1, -1), jnp.zeros((1, D - packed_bias.shape[0]), F32)], axis=1)
    vrow = pltpu.roll(jnp.broadcast_to(vrow, (8, D)), 32 * col_i, 1)
    bias[pos] = jnp.concatenate([vrow[:4], jnp.broadcast_to(expansion_bias[...].reshape(1, -1), (4, D))], axis=0)

    for d in range(1, 2 * Y):
        bcopy(d).start()

    x[rows:, :] = jnp.zeros((x.shape[0] - rows, D), BF16)
    up[rows:, :] = jnp.zeros((RP - rows, D), BF16)
    for h in range(PAIRS):
        qkv[h, RP:, :] = jnp.zeros((qkv.shape[1] - RP, D), BF16)
    tail = attn.shape[0] - RP + 16
    attn[RP - 16:, :] = jnp.zeros((tail, D), BF16)
    rinv[RP - 16:, :] = jnp.zeros((tail, D), F32)
    pgr[RP - 16:, :] = jnp.zeros((tail, PAIRS * D), BF16)
    fs = first_scale[...].reshape(1, D)
    fh = first_shift[...].reshape(1, D)
    ss = second_scale[...].reshape(1, D)
    sh = second_shift[...].reshape(1, D)
    prb = projection_bias[...].reshape(1, D)
    rdb = reduction_bias[...].reshape(1, D)
    cin.wait()
    cup.wait()

    def ln1(i, _):
        s = rows_of(i, SMALL)
        v = x[s, :].astype(F32)
        avg = mean(v)
        inv = lax.rsqrt(mean(v * v) - avg * avg + EPS)
        normed = (v - avg) * inv
        n1[s, :] = normed
        inv1[s, 0:64] = jnp.broadcast_to(inv, (SMALL, 64))
        rows1[s, :] = (normed * fs + fh).astype(BF16)
        return 0

    @named
    def pass_on(d):
        q = znear(d - 1)
        arrived(zfirst.at[q], chunks[0].at[q, pd, :, mine_l])
        for e in range(PLANE - 1, 0, -1):
            qcopy(e, q).start()
        scopy(q).start()

    loop(0, nsm, ln1, 0)
    for k in (1, 2, 3):
        to_z(k)
    for d in range(1, Z):
        pass_on(d)
    for k in range(4, len(chunks)):
        to_z(k)
    with jax.named_scope("plane0"):
        for d in range(1, PLANE):
            if d == PLANE - 1:
                to_plane(1)
            arrived(pfirst.at[d - 1], span(Z))
            scopy_from(d).start()
    to_plane(2)
    arrived(bs.at[1], n1.at[0:8 * (2 * Y - 1)])

    lane = lax.broadcasted_iota(jnp.int32, (KEYS, 128), 1)
    even = lane < 64
    zero = jnp.zeros((KEYS, 128), BF16)
    one = jnp.ones((KEYS, 128), BF16)
    ones_e = jnp.where(even, one, zero)
    ones_o = jnp.where(even, zero, one)

    def place(c):
        return (c % 2) * Y + c // 2

    if RV != RB:
        wide = Z * PD * RB
        r_ = lax.broadcasted_iota(jnp.int32, (D, wide), 0)
        c_ = lax.broadcasted_iota(jnp.int32, (D, wide), 1)
        pick = jnp.where(c_ == (r_ // RV) * RB + lax.rem(r_, RV), 1.0, 0.0).astype(BF16)

    def compact(v):
        v = v.reshape(Z * PD * RB, v.shape[-1])
        return v if RV == RB else nn(pick, v).astype(BF16)

    def spread(v):
        v = v.astype(BF16)
        v = v if RV == RB else tn(pick, v).astype(BF16)
        return v.reshape(Z, PD, RB, v.shape[-1])

    def merged(tile, first, second, upto):
        if first == second:
            return tile(first)
        a, b = tile(first), tile(second)
        return jnp.where(lax.broadcasted_iota(jnp.int32, a.shape, 1) < upto, a, b)

    @named
    def assemble(h):
        kcopy(h).wait_recv()
        for j, (first, second, upto) in enumerate(TILES[h]):
            wp[:, h * D + j * 128:h * D + (j + 1) * 128] = merged(
                lambda c: compact(wpk[h, :, :, :, place(c) * 128:(place(c) + 1) * 128]), first, second, upto)

    def bias_of(h):
        def tile(c):
            t = (h + c) % 3
            return bias[place(c), 0:1, t * 128:(t + 1) * 128]
        return jnp.concatenate([merged(tile, *t) for t in TILES[h]], axis=1)

    def keep(ref, i, value):
        last = min(rows, (i + 1) * SMALL)
        ref[i * SMALL:last, :] = value[:last - i * SMALL]

    def again(ref, i):
        last = min(rows, (i + 1) * SMALL)
        value = ref[i * SMALL:last, :]
        more = (i + 1) * SMALL - last
        return value if not more else jnp.concatenate([value, jnp.zeros((more, D), value.dtype)], axis=0)

    def window(i):
        first = i * SEQ
        base = (first // 16) * 16
        return first - base, base if isinstance(i, int) else pl.multiple_of(base, 16)

    before = ((to_plane, 3),), ((to_plane, 7),), ((to_plane, 8), (to_plane, 9), (to_sibling, 3), (to_sibling, 4))
    after = (
        ((to_plane, 4), (to_sibling, 1), (to_plane, 5), (to_sibling, 2), (to_plane, 6)),
        (),
        ((to_sibling, 5),),
    )

    def do(steps):
        for step, k in steps:
            step(k)

    for h in range(PAIRS):
        hl = pl.ds(h * 128, 128)
        if h < 2:
            both = (0,) if h == 0 else tuple(range(1, PAIRS))
            for g in both:
                assemble(g)
            pb = jnp.concatenate([bias_of(g) for g in both], axis=1)

            def project(i, _):
                s = rows_of(i, BIG)
                v = (nn(rows1[s, :], wp[:, both[0] * D:(both[-1] + 1) * D]) + pb).astype(BF16)
                for n, g in enumerate(both):
                    qkv[g, s, :] = v[:, n * D:(n + 1) * D]
                return 0

            loop(0, nbig, project, 0)

        def attend(i, _):
            off, base = window(i)
            qw = pl.ds(base, WIN)
            kk = pl.ds(base, KEYS)
            q = qkv[h, qw, 0:128]
            k = qkv[h, kk, 128:256]
            v = qkv[h, kk, 256:384]
            col = lax.broadcasted_iota(jnp.int32, (WIN, KEYS), 1) - off
            ok = (col >= 0) & (col < SEQ)
            es = []
            for m in (even, ~even):
                s = nt(q, jnp.where(m, k, zero))
                s = jnp.where(ok, s, -1e30)
                top = jnp.max(s, axis=1, keepdims=True)
                es.append(jnp.exp((s - top) * 0.125).astype(BF16))
            est[h, i, 0] = es[0]
            est[h, i, 1] = es[1]
            mix = nn(es[0], jnp.concatenate([jnp.where(even, v, zero), ones_e], axis=1)) + nn(
                es[1], jnp.concatenate([jnp.where(even, zero, v), ones_o], axis=1))
            r = 1.0 / mix[:, 128:]
            o = mix[:, :128] * r
            rid = lax.broadcasted_iota(jnp.int32, (WIN, 128), 0) - off
            mine = (rid >= 0) & (rid < SEQ)
            attn[qw, hl] = jnp.where(mine, o, attn[qw, hl].astype(F32)).astype(BF16)
            rinv[qw, hl] = jnp.where(mine, r, rinv[qw, hl])
            return 0

        do(before[h])
        unrolled(0, images, attend, 0)
        do(after[h])

    kcopy(3).wait_recv()
    lane_d = lax.broadcasted_iota(jnp.int32, (D, 128), 1)
    tiles = [compact(ptr[:, :, :, place(c) * 128:(place(c) + 1) * 128]) for c in range(4)]
    pt[:, 0:128] = jnp.where(lane_d < 96, tiles[0], tiles[1])
    pt[:, 128:256] = jnp.where(lane_d < 64, tiles[1], tiles[2])
    pt[:, 256:384] = jnp.where(lane_d < 32, tiles[2], tiles[3])
    def exb_of(j):
        return jnp.concatenate([bias[p, 4:5, j * 128:(j + 1) * 128] for p in range(4)], axis=1)


    def ln2(i, _):
        s = rows_of(i, SMALL)
        v = x[s, :].astype(F32) + nt(attn[s, :], pt[...]) + prb
        avg = mean(v)
        inv = lax.rsqrt(mean(v * v) - avg * avg + EPS)
        normed = (v - avg) * inv
        acc1[s, :] = v + rdb
        n2[s, :] = normed
        inv1[s, 64:128] = jnp.broadcast_to(inv, (SMALL, 64))
        x[s, :] = (normed * ss + sh).astype(BF16)
        keep(o_grad, i, jnp.zeros((SMALL, D), F32))
        return 0

    unrolled(0, nsm, ln2, 0)

    def part(big, small, k):
        return big.at[k] if k < PAIRS else small.at[k - PAIRS]

    def width(k):
        return 256 if k < PAIRS else 128

    def g1(k):
        half = Y * width(k)
        return remote(part(gm, gh, k).at[:, :, :, lanes_of(1 - core, half)], part(rm1, rh1, k),
                      gsend.at[k], g1r.at[k], sibling)

    def g2(k, d):
        pp, yy = pplace(d)
        return remote(part(sm1, sh1, k).at[:, pp, :, lanes_of(yy, width(k))], part(rm2, rh2, k).at[d - 1],
                      gsend.at[k], g2r.at[k], ppeer(d))

    def g3(k, d):
        return remote(part(sm2, sh2, k).at[znear(d - 1)], part(rm3, rh3, k).at[z], gsend.at[k], g3r.at[k], zpeer(d))

    @named
    def sum1(k):
        g1(k).wait_recv()
        own = part(gm, gh, k)[:, :, :, lanes_of(core, Y * width(k))]
        part(sm1, sh1, k)[...] = (own.astype(F32) + part(rm1, rh1, k)[...].astype(F32)).astype(BF16)
        for d in range(PLANE - 1, 0, -1):
            g2(k, d).start()

    LAST = 3 + PAIRS

    def piece1(d):
        pp, yy = pplace(d)
        return remote(gh.at[PAIRS, :, pp, :, lanes_of((1 - core) * Y + yy, 128)],
                      rh1.at[PAIRS, :, pp, :, lanes_of(yy, 128)], gsend.at[LAST], glast.at[d], sibling)

    def piece_sum(d):
        pp, yy = pplace(d)
        piece1(d).wait_recv()
        own = gh[PAIRS, :, pp, :, lanes_of(core * Y + yy, 128)]
        got = rh1[PAIRS, :, pp, :, lanes_of(yy, 128)]
        sh1[PAIRS, :, pp, :, lanes_of(yy, 128)] = (own.astype(F32) + got.astype(F32)).astype(BF16)
        if d:
            g2(LAST, d).start()

    @named
    def sum1_last(_):
        for d in range(PLANE - 1, -1, -1):
            piece_sum(d)

    @named
    def sum2(k):
        arrived(g2r.at[k], span((PLANE - 1) * Z * (width(k) // 128)))
        total = part(sm1, sh1, k)[:, pd, :, lanes_of(y, width(k))].astype(F32)
        for d in range(1, PLANE):
            total += part(rm2, rh2, k)[d - 1].astype(F32)
        part(sm2, sh2, k)[...] = total.astype(BF16)
        for d in range(Z - 1, 0, -1):
            g3(k, d).start()

    @named
    def sum3(k):
        arrived(g3r.at[k], span((Z - 1) * (width(k) // 128)))
        total = part(sm2, sh2, k)[z].astype(F32)
        for d in range(1, Z):
            total += part(rm3, rh3, k)[znear(d - 1)].astype(F32)
        return total

    vec[...] = jnp.zeros(vec.shape, F32)
    spot = (
        ((to_sibling, 6), (to_sibling, 7)),
        ((to_sibling, 8), (to_sibling, 9), (sum1, 0)),
        ((sum1, 1),),
    )
    NH = FF // HC
    mlp_in = [((kcopy, 4 + 2 * j), (kcopy, 5 + 2 * j)) for j in range(NH)]

    def chunk(j, _):
        for n in range(NH):
            pl.when(j == n)(lambda n=n: (kcopy(4 + 2 * n).wait_recv(), kcopy(5 + 2 * n).wait_recv(), None)[2])
        if RV != RB:
            exc[...] = compact(exr[j])
            rtc[...] = compact(rtr[j])

        def ex_of():
            return exc[...] if RV != RB else exr[j].reshape(D, HC)

        def rt_of():
            return rtc[...] if RV != RB else rtr[j].reshape(D, HC)

        tile = lanes_of(j, 128)
        exb = jnp.concatenate([bias[p, 4:5, tile] for p in range(4)], axis=1)
        bsum = jnp.zeros((1, HC), F32)
        for i in range(nbig):
            s = rows_of(i, BIG)
            pre = nn(x[s, :], ex_of()) + exb
            ug = nn(up[s, :], rt_of())
            cdf = 0.5 + 0.5 * lax.erf(pre * ROOT_HALF)
            act[j, s, :] = (pre * cdf).astype(BF16)
            g = ug * (cdf + pre * (jnp.exp(pre * pre * -0.5) * INV_ROOT_TAU))
            hg[s, :] = g.astype(BF16)
            last = min(rows, (i + 1) * BIG)
            back = nt(hg[s, :], ex_of())
            o_grad[i * BIG:last, :] += back[:last - i * BIG]
            bsum += jnp.sum(g, axis=0, keepdims=True)
        for p in range(4):
            vec[9 + p:10 + p, tile] = bsum[:, p * 128:(p + 1) * 128]
        for n in range(NH):
            pl.when(j == n)(lambda n=n: do(spot[n]))
        for base, g in ((0, tn(x[0:RP, :], hg[...])), (128, tn(up[...], act[j]))):
            for p in range(4):
                gm[j, :, :, :, p * 256 + base:p * 256 + base + 128] = spread(g[:, p * 128:(p + 1) * 128])
        for n in range(NH):
            pl.when(j == n)(lambda n=n: (g1(n).start(), None)[1])
        return 0

    loop(0, NH, chunk, 0)

    def ln2b(i, carry):
        s = rows_of(i, SMALL)
        u = up[s, :].astype(F32)
        g = again(o_grad, i)
        normed = n2[s, :]
        inv = inv1[s, 64:65]
        scaled = g * ss
        d = u + inv * (scaled - mean(scaled) - normed * mean(scaled * normed))
        keep(o_grad, i, d)
        hg[s, 0:D] = d.astype(BF16)
        x[s, :] = nn(d.astype(BF16), pt[...]).astype(BF16)
        terms = (d, u, g * normed, g)
        return tuple(a + jnp.sum(t, axis=0, keepdims=True) for a, t in zip(carry, terms))

    zr1 = jnp.zeros((1, D), F32)
    sums = unrolled(0, nsm, ln2b, (zr1,) * 4)
    for r, t in zip((0, 1, 4, 5), sums):
        vec[r:r + 1, :] = t
    sum1(2)
    sum2(0)
    gj = tn(hg[:, 0:D], attn[0:RP, :]).astype(BF16)
    t0, t1, t2 = gj[:, 0:128], gj[:, 128:256], gj[:, 256:384]
    for c, t in enumerate((t0, jnp.where(lane_d < 64, t1, t0), jnp.where(lane_d < 64, t2, t1), t2)):
        gh[0, :, :, :, place(c) * 128:(place(c) + 1) * 128] = spread(t)
    g1(3).start()

    def finish_mlp(j):
        total = sum3(j)
        small[1, :, j * 128:(j + 1) * 128] = total[:, :128]
        small[2, :, j * 128:(j + 1) * 128] = total[:, 128:]

    def finish_projection(_):
        t = pltpu.roll(sum3(3), lax.rem(128 - lax.rem(96 * col_i, 128), 128), 1)
        small[3, :, 0:128] = t

    behind = (
        ((sum1, 3), (sum2, 1)),
        ((sum1, 4), (sum2, 2)),
        ((sum1, 5),),
    )

    for h in range(PAIRS):
        hl = pl.ds(h * 128, 128)

        def attend_back(i, _):
            off, base = window(i)
            qw = pl.ds(base, WIN)
            kk = pl.ds(base, KEYS)
            q = qkv[h, qw, 0:128]
            k = qkv[h, kk, 128:256]
            v = qkv[h, kk, 256:384]
            rid = lax.broadcasted_iota(jnp.int32, (WIN, 128), 0) - off
            mine = (rid >= 0) & (rid < SEQ)
            do = jnp.where(mine, x[qw, hl].astype(F32) * rinv[qw, hl], 0.0)
            dob = do.astype(BF16)
            xx = jnp.concatenate([dob, (do * attn[qw, hl].astype(F32)).astype(BF16)], axis=1)
            ev = even[:WIN]
            zw = zero[:WIN]
            e0 = est[h, i, 0]
            e1 = est[h, i, 1]
            d0 = (e0 * nt(xx, jnp.concatenate([jnp.where(even, v, zero), -ones_e], axis=1))).astype(BF16)
            d1 = (e1 * nt(xx, jnp.concatenate([jnp.where(even, zero, v), -ones_o], axis=1))).astype(BF16)
            dq = (nn(d0, jnp.where(even, k, zero)) + nn(d1, jnp.where(even, zero, k))) * 0.125
            dk = (tn(d0, jnp.where(ev, q, zw)) + tn(d1, jnp.where(ev, zw, q))) * 0.125
            dv = tn(e0, jnp.where(ev, dob, zw)) + tn(e1, jnp.where(ev, zw, dob))
            old = pgr[qw, h * D:(h + 1) * D].astype(F32)
            pgr[qw, h * D:h * D + 128] = jnp.where(mine, dq, old[:, 0:128]).astype(BF16)
            pgr[qw, h * D + 128:h * D + 256] = jnp.where(mine, dk[:WIN], old[:, 128:256]).astype(BF16)
            pgr[qw, h * D + 256:h * D + 384] = jnp.where(mine, dv[:WIN], old[:, 256:384]).astype(BF16)
            return 0

        unrolled(0, images, attend_back, 0)
        do(behind[h])
        gp = tn(rows1[...], pgr[0:RP, h * D:(h + 1) * D])
        for c, j in enumerate(SHARES[h]):
            gh[1 + h, :, :, :, place(c) * 128:(place(c) + 1) * 128] = spread(gp[:, j * 128:(j + 1) * 128])
        if h < PAIRS - 1:
            g1(4 + h).start()
        else:
            for d in range(PLANE - 1, -1, -1):
                piece1(d).start()
            do(((sum2, 3), (sum2, 4), (finish_mlp, 0), (finish_mlp, 1)))

    def bias_sum(i, carry):
        s = rows_of(i, SMALL)
        return carry + jnp.sum(pgr[s, :].astype(F32), axis=0, keepdims=True)

    bsum = unrolled(0, nsm, bias_sum, jnp.zeros((1, PAIRS * D), F32))
    for h in range(PAIRS):
        vec[6 + h:7 + h, :] = bsum[:, h * D:(h + 1) * D]
    vq[...] = jnp.zeros(vq.shape, F32)
    for q in range(4):
        for h in range(PAIRS):
            j = SHARES[h][q]
            vq[q, 6 + h:7 + h, :] = vec[6 + h:7 + h, j * 128:(j + 1) * 128]
            vq[q, 9 + h:10 + h, :] = vec[9 + place(q):10 + place(q), h * 128:(h + 1) * 128]

    gbuf = n2

    def ln1b(i, carry):
        s = rows_of(i, SMALL)
        g = nt(pgr[s, :], wp[...])
        gbuf[s, :] = g
        terms = (g * n1[s, :], g)
        hook(i, [(nsm // 2 - 2, lambda: sum1_last(0))])
        return tuple(a + jnp.sum(t, axis=0, keepdims=True) for a, t in zip(carry, terms))

    sums = unrolled(0, nsm, ln1b, (zr1,) * 2)

    for r, t in zip((2, 3), sums):
        vec[r:r + 1, :] = t
    wide_d = D // 4
    for q in range(4):
        vq[q, 0:6, 0:wide_d] = vec[0:6, q * wide_d:(q + 1) * wide_d]
    me = plane * 2 + core

    def v2(d):
        to = vpeer(d)
        return remote(vq.at[to[1]], vr2.at[me], vs.at[0], vs.at[1], to)

    def v3(d):
        return remote(vr3.at[z], vr3.at[z], vs.at[0], vs.at[2], zpeer(d))

    def vector2():
        arrived(vs.at[1], vspan(2 * PLANE - 1))
        total = vr2[0]
        for q in range(1, 2 * PLANE):
            total += vr2[q]
        vr3[z] = total
        for d in range(Z - 1, 0, -1):
            v3(d).start()

    for d in range(2 * PLANE - 1, 0, -1):
        v2(d).start()
    vr2[me] = vq[col_i]

    def ln1c(i, _):
        s = rows_of(i, SMALL)
        normed = n1[s, :]
        inv = inv1[s, 0:1]
        scaled = gbuf[s, :] * fs
        keep(o_grad, i, again(o_grad, i) + inv * (scaled - mean(scaled) - normed * mean(scaled * normed)))
        return 0

    unrolled(0, nsm, ln1c, 0)
    def emit(i):
        s = rows_of(i, BIG)
        last = min(rows, (i + 1) * BIG)
        value = acc1[s, :]
        for j in range(NH):
            value += nt(act[j, s, :], rtr[j].reshape(D, HC) if RV == RB else compact(rtr[j]))
        o_out[i * BIG:last, :] = value[:last - i * BIG].astype(BF16)

    do(((sum2, 5),))
    with jax.named_scope("emit"):
        for i in range(nbig):
            emit(i)
            if i == 0:
                do(((sum2, 6),))
            if i == min(1, nbig - 1):
                vector2()
        do(((finish_mlp, 2), (finish_projection, 3)))
    for h in range(PAIRS - 1):
        frame[:, turn(h)] = sum3(4 + h)
    frame[:, turn(PAIRS - 1)] = sum3(3 + PAIRS)
    back = lax.rem(D - 32 * col_i, D)
    small[0] = pltpu.roll(frame[...], back, 1)
    with jax.named_scope("vec3"):
        arrived(vs.at[2], vspan(Z - 1))
    total = vr3[0]
    for q in range(1, Z):
        total += vr3[q]
    small[3, 0:8, 128:256] = total[0:8]
    for h in range(PAIRS):
        frame[0:1, turn(h)] = total[6 + h:7 + h]
        small[4, 8:9, h * 128:(h + 1) * 128] = total[9 + h:10 + h]
    small[4, 0:8, :] = pltpu.roll(frame[0:8, :], back, 1)

    with jax.named_scope("ends"):
        for k in range(len(chunks)):
            left(asend.at[k], span(ALL))
        left(bs.at[0], n1.at[0:8 * (2 * Y - 1)])
        for k in range(7):
            left(gsend.at[k], span(ALL * (width(k) // 128)))
        left(vs.at[0], vspan(2 * PLANE + Z - 2))


def finish_kernel(*refs):
    out, grad, small = refs[:3]
    outs, stage, sem = refs[3:17], refs[17:29], refs[29]
    moves = [pltpu.make_async_copy(a, b, sem.at[k]) for k, (a, b) in enumerate(zip((grad, out) + stage, (outs[1], outs[0]) + outs[2:]))]
    moves[0].start()
    moves[1].start()
    rv, wide = stage[0].shape
    stage[0][...] = small[0, :rv, :wide]
    stage[1][...] = small[3, :rv, :stage[1].shape[1]]
    stage[2][...] = small[1, :rv, :]
    stage[3][...] = small[2, :rv, :]
    stage[4][...] = small[4, 0:1, :wide].reshape(wide)
    stage[6][...] = small[4, 8:9, :].reshape(D)
    for r, k in enumerate((5, 7, 8, 9, 10, 11)):
        n = stage[k].shape[0]
        stage[k][...] = small[3, r:r + 1, 128:128 + n].reshape(n)
    for move in moves[2:]:
        move.start()
    for move in moves:
        move.wait()


def body(dps, cols, tokens, packed, packed_bias, projection, projection_bias, expansion, expansion_bias, reduction,
         reduction_bias, first_scale, first_shift, second_scale, second_shift, upstream):
    args = (tokens, packed, packed_bias, projection.T, projection_bias, expansion, expansion_bias, reduction.T,
            reduction_bias, first_scale, first_shift, second_scale, second_shift, upstream)
    rows = tokens.shape[0]
    images = rows // SEQ
    Z = min(4, dps)
    PD = dps // Z
    Y = cols // 2
    RV = packed.shape[0]
    RB = -(-RV // 16) * 16
    PLANE = PD * Y
    RP = -(-rows // BIG) * BIG
    reach = ((images - 1) * SEQ) // 16 * 16
    XQ = max(RP + 16, reach + WIN)
    XP = max(RP + 16, reach + KEYS)
    cfg = (Z, PD, Y, RB, RV, rows)
    V = pl.BlockSpec(memory_space=pltpu.VMEM)
    A = pl.BlockSpec(memory_space=pl.ANY)
    S = jax.ShapeDtypeStruct
    vm = pltpu.VMEM
    dma = pltpu.SemaphoreType.DMA
    NH = FF // HC
    NC = PAIRS + 1 + 2 * NH
    small = RV != RB
    outs = (
        S((rows, D), BF16), S((rows, D), F32),
        S(packed.shape, F32), S(projection.shape[::-1], F32), S(expansion.shape, F32), S(reduction.shape[::-1], F32),
        S(packed_bias.shape, F32), S((D // cols,), F32), S(expansion_bias.shape, F32),
    ) + (S((D // cols,), F32),) * 5
    narrow = (args[1], args[2], args[3], args[4], args[5], args[6], args[7]) + args[8:13]
    scratch = [vm(a.shape, a.dtype) for a in narrow] + [
        vm((XQ, D), BF16), vm((RP, D), BF16),
        vm((RP, D), F32), vm((RP, D), BF16),
        vm((PAIRS, XP, D), BF16), vm((XQ, D), BF16),
        vm((PAIRS, images, 2, WIN, KEYS), BF16), vm((XQ, D), F32),
        vm((RP, D), F32), vm((RP, D), F32),
        vm((NH, RP, HC), BF16), vm((RP, HC), BF16),
        vm((XQ, PAIRS * D), BF16), vm((max(RP, (Z - 1 + (2 * PLANE - 1) * Z) * RB), 128), F32),
        vm((PAIRS, Z, PD, RB, 4 * 128), BF16), vm((Z, PD, RB, 4 * 128), BF16),
        vm((NH, Z, PD, RB, HC), BF16), vm((NH, Z, PD, RB, HC), BF16),
        vm((D, PAIRS * D), BF16), vm((D, D), BF16),
        vm((D, HC) if small else (16, 128), BF16), vm((D, HC) if small else (16, 128), BF16),
        vm((4, 8, D), F32),
        vm((NH, Z, PD, RB, 4 * 256), BF16), vm((4, Z, PD, RB, 4 * 128), BF16),
        vm((NH, Z, PD, RB, Y * 256), BF16), vm((NH, PLANE - 1, Z, RB, 256), BF16), vm((NH, Z, RB, 256), BF16),
        vm((4, Z, PD, RB, Y * 128), BF16), vm((4, PLANE - 1, Z, RB, 128), BF16), vm((4, Z, RB, 128), BF16),
        vm((NH, Z, PD, RB, Y * 256), BF16), vm((NH, Z, RB, 256), BF16),
        vm((4, Z, PD, RB, Y * 128), BF16), vm((4, Z, RB, 128), BF16),
        vm((RB, D), F32), vm((16, D), F32),
        vm((4, 16, 128), F32), vm((2 * PLANE, 16, 128), F32), vm((Z, 16, 128), F32),
        dma((NC,)), dma((Z,)), dma((PLANE - 1,)), dma((NC,)), dma((NC,)), dma((NC,)),
        dma((2,)), dma((7,)), dma((7,)), dma((7,)), dma((7,)), dma((PLANE,)), dma((3,)),
    ]
    got = pl.pallas_call(
        functools.partial(layer_kernel, cfg),
        out_shape=(vm((rows, D), BF16), vm((rows, D), F32), vm((5, RB, D), F32)),
        in_specs=[A] * 14,
        out_specs=(V,) * 3,
        scratch_shapes=scratch,
        compiler_params=pltpu.CompilerParams(vmem_limit_bytes=VMEM - rows * D * 6 - 5 * RB * D * 4 - 65536, collective_id=0, has_side_effects=True),
    )(*args)
    got = pl.pallas_call(
        finish_kernel,
        out_shape=outs,
        in_specs=[V] * 3,
        out_specs=(A,) * 14,
        scratch_shapes=[vm(o.shape, o.dtype) for o in outs[2:]] + [dma((14,))],
        compiler_params=pltpu.CompilerParams(vmem_limit_bytes=2 * 1024 * 1024),
    )(*(pltpu.with_memory_space_constraint(v, pltpu.VMEM) for v in got))
    return got[:3] + (got[3].T, got[4], got[5].T) + tuple(got[6:])


def solution(mesh):
    placed = (
        P(("dp", "col"), None), P("dp", "col"), P("col"), P("col", "dp"), P(), P("dp", "col"), P("col"),
        P("col", "dp"), P(), P(), P(), P(), P(), P(("dp", "col"), None),
    )
    return jax.shard_map(
        functools.partial(body, mesh.shape["dp"], mesh.shape["col"]),
        mesh=mesh,
        in_specs=placed,
        out_specs=(
            P(("dp", "col"), None), P(("dp", "col"), None),
            P("dp", "col"), P("col", "dp"), P("dp", "col"), P("col", "dp"),
        ) + (P("col"),) * 8,
        check_vma=False,
    )
```
